32 devices in a mesh: patch: 4 (over z), seq: 4 (over y, x), req: 2 (over core).
Axes of the slice: x: 2, y: 2, z: 4, core: 2. Of those that a mesh axis runs over, the one named last changes fastest.
Arguments:
- query: bfloat16 [4, 8, 3584], P(None, ('patch', 'req')), may hold values from -20 to 20
- text_cache: bfloat16 [4, 8, 3072, 1024], P(None, ('patch', 'req'), 'seq'), may hold values from -6 to 6
- text_len: int32 [8], P(('patch', 'req')), may hold values from 0 to 3072
- image_rows: bfloat16 [4, 8192, 1024], P(None, ('patch', 'seq', 'req')), may hold values from -6 to 6
- patch_map: int32 [8192], P(('patch', 'seq', 'req')), may hold values from 0 to 7, as said below
- image_places: int32 [8192], P(('patch', 'seq', 'req')), may hold values from 0 to 1023, as said below
Outputs:
- attended: bfloat16 [4, 8, 3584], P(None, ('patch', 'req'), 'seq')
- image_cache: bfloat16 [4, 8, 1024, 1024], P(None, ('patch', 'req'), 'seq')
The draws below stay inside these ranges and needn't reach their ends.
Inputs may be any that keep to these rules, and one draw needn't show every extreme that they name: `patch_map`: each aligned block of 256 rows (the rows of one prefill device) holds exactly 32 rows of every request. `image_places`: together with patch_map every pair of request and position occurs exactly once. The rows of a device whose seq index is s have positions from s * 256 to (s + 1) * 256 - 1.
All inputs are finite; a program needn't handle non-finite values.
Results may differ from the reference program's by a relative error of at most 0.0026.
Values may be sent and summed in bfloat16 or wider, within the bound.
A program may use at most 64 MiB of HBM per device.

```python
import math
import jax
import jax.numpy as jnp
from jax import lax

HEADS = 28
KV_HEADS = 4
HEAD_DIM = 128
LAYERS = 4
IMG = 1024
TXT = 3072
REQUESTS = 8
KVW = 512
N_PATCH = 4
N_SEQ = 4
N_REQ = 2


def layout_rows(key):
    groups = N_PATCH * N_REQ
    band_size = IMG // N_SEQ
    per_source = band_size // groups
    device_count = N_PATCH * N_SEQ * N_REQ
    pair_keys = jax.random.split(jax.random.fold_in(key, 7001), N_SEQ * REQUESTS)
    shuffled = jax.vmap(lambda piece: jax.random.permutation(piece, band_size))(pair_keys)
    shuffled = shuffled.astype(jnp.int32).reshape(N_SEQ, REQUESTS, N_PATCH, N_REQ, per_source)
    band_start = (jnp.arange(N_SEQ, dtype=jnp.int32) * band_size)[:, None, None, None, None]
    places = shuffled + band_start
    owners = jnp.broadcast_to(jnp.arange(REQUESTS, dtype=jnp.int32)[None, :, None, None, None], places.shape)
    places = jnp.transpose(places, (2, 0, 3, 1, 4)).reshape(device_count, REQUESTS * per_source)
    owners = jnp.transpose(owners, (2, 0, 3, 1, 4)).reshape(device_count, REQUESTS * per_source)
    row_keys = jax.random.split(jax.random.fold_in(key, 7002), device_count)
    mixing = jax.vmap(lambda piece: jax.random.permutation(piece, REQUESTS * per_source))(row_keys)
    mixing = mixing.astype(jnp.int32)
    places = jnp.take_along_axis(places, mixing, axis=1).reshape(-1)
    owners = jnp.take_along_axis(owners, mixing, axis=1).reshape(-1)
    return (owners, places)


def draw_patch_map(key, part):
    return layout_rows(key)[0]


def draw_image_places(key, part):
    return layout_rows(key)[1]


def draw_query(key, part):
    shape = (LAYERS, REQUESTS, HEADS * HEAD_DIM)
    noise_key = jax.random.fold_in(key, 7004)
    values = jnp.clip(2.5 * jax.random.normal(noise_key, shape, jnp.float32), -12.0, 12.0)
    return values.astype(jnp.bfloat16)


def draw_image_rows(key, part):
    shape = (LAYERS, REQUESTS * IMG, 2 * KV_HEADS * HEAD_DIM)
    noise_key = jax.random.fold_in(key, 7005)
    values = jnp.clip(jax.random.normal(noise_key, shape, jnp.float32), -6.0, 6.0)
    return values.astype(jnp.bfloat16)


def place_ends(values, own_key, least, top_value):
    index_at = [jax.random.randint(jax.random.fold_in(own_key, axis), (), 0, length) for axis, length in enumerate(values.shape)]
    longest = values.shape.index(max(values.shape))
    neighbour = index_at[:longest] + [(index_at[longest] + 1) % values.shape[longest]] + index_at[longest + 1:]
    return values.at[tuple(index_at)].set(least).at[tuple(neighbour)].set(top_value)


def block_levels(rng, shape, cuts, low, largest):
    loudness, own = 1.0, jax.random.fold_in(rng, 6)
    for position, shards_of in cuts:
        steps = jnp.exp(jax.random.uniform(jax.random.fold_in(own, position), (shards_of,), jnp.float32, low / len(cuts), largest / len(cuts)))
        loudness = loudness * jnp.repeat(steps, shape[position] // shards_of).reshape([-1 if axis == position else 1 for axis in range(len(shape))])
    return loudness


def bell_draw(rng, dims, deviation, most, cuts=(), kind=jnp.bfloat16):
    result = deviation * jax.random.normal(rng, dims, jnp.float32)
    if cuts:
        result = result * block_levels(rng, dims, cuts, -0.22, 0.18)
    return jnp.clip(result, -most, most).astype(kind)


def setup_inputs(seed: int = 0) -> dict:
    seeds = jax.random.split(jax.random.key(seed), 7)
    return {
        "query": draw_query(jax.random.fold_in(seeds[6], 71), 0),
        "text_cache": bell_draw(seeds[1], (LAYERS, REQUESTS, TXT, 2 * KVW), 1.0, 6.0, ((1, 8), (2, 4))),
        "text_len": place_ends(jax.random.randint(seeds[2], (REQUESTS,), 0, TXT + 1), jax.random.fold_in(seeds[2], 1), 0, TXT).astype(jnp.int32),
        "image_rows": draw_image_rows(jax.random.fold_in(seeds[6], 71), 0),
        "patch_map": draw_patch_map(jax.random.fold_in(seeds[6], 71), 0),
        "image_places": draw_image_places(jax.random.fold_in(seeds[6], 71), 0),
    }


def attend_one(query_row, image_block, text_block, length):
    kv_width = KV_HEADS * HEAD_DIM
    group = HEADS // KV_HEADS
    band_size = IMG // N_SEQ
    text_band = TXT // N_SEQ
    image_banded = image_block.reshape(N_SEQ, band_size, 2 * kv_width)
    text_banded = text_block.reshape(N_SEQ, text_band, 2 * kv_width)
    keys_all = jnp.concatenate([image_banded, text_banded], axis=1)
    width = band_size + text_band
    keys = keys_all[:, :, :kv_width].reshape(N_SEQ, width, KV_HEADS, HEAD_DIM).astype(jnp.float32)
    values = keys_all[:, :, kv_width:].reshape(N_SEQ, width, KV_HEADS, HEAD_DIM).astype(jnp.float32)
    queries = query_row.reshape(KV_HEADS, group, HEAD_DIM).astype(jnp.float32)
    scores = jnp.einsum('kgd,stkd->skgt', queries, keys) * (1.0 / math.sqrt(HEAD_DIM))
    inner = jnp.arange(width, dtype=jnp.int32)
    bands = jnp.arange(N_SEQ, dtype=jnp.int32)
    text_pos = bands[:, None] * text_band + inner[None, :] - band_size
    used = (inner[None, :] < band_size) | (text_pos < length)
    scores = jnp.where(used[:, None, None, :], scores, -jnp.inf)
    band_top = lax.optimization_barrier(jnp.max(scores, axis=-1, keepdims=True))
    weights = jnp.exp(scores - band_top)
    band_total = lax.optimization_barrier(jnp.sum(weights, axis=-1))
    rounded = lax.optimization_barrier(weights.astype(jnp.bfloat16)).astype(jnp.float32)
    band_sum = jnp.einsum('skgt,stkd->skgd', rounded, values)
    band_top = band_top[..., 0]
    top = lax.optimization_barrier(jnp.max(band_top, axis=0, keepdims=True))
    factor = jnp.exp(band_top - top)
    total = lax.optimization_barrier(jnp.sum(factor * band_total, axis=0))
    summed = lax.optimization_barrier(jnp.sum(factor[..., None] * band_sum, axis=0))
    return (summed / total[..., None]).reshape(HEADS * HEAD_DIM).astype(jnp.bfloat16)

def attend_packed(packed):
    return attend_one(packed[0], packed[1], packed[2], packed[3])

def reference(query, text_cache, text_len, image_rows, patch_map, image_places):
    order = jnp.argsort(patch_map * IMG + image_places)
    image_cache = jnp.take(image_rows, order, axis=1).reshape(LAYERS, REQUESTS, IMG, image_rows.shape[2])

    def per_layer(packed):
        return lax.map(attend_packed, (packed[0], packed[1], packed[2], text_len))
    attended = lax.map(per_layer, (query, image_cache, text_cache))
    return (attended, image_cache)
```

```python
import functools
import math

import jax
import jax.numpy as jnp
from jax import lax
from jax.experimental import pallas as pl
from jax.experimental.pallas import tpu as pltpu
from jax.sharding import PartitionSpec as P

HEADS = 28
KV_HEADS = 4
HEAD_DIM = 128
PAD = 8
MESH = pl.DeviceIdType.MESH
NT = (((1,), (1,)), ((), ()))


def near_hops(patch_count, req_count):
    half = patch_count // 2
    beside = [("near", i, c) for i in range(1, half) for c in range(req_count)]
    return beside + [("near", 0, c) for c in range(1, req_count)]


def far_hops(patch_count, req_count, k):
    return [("far", k, c) for c in range(req_count)]


def exchange(
    dims,
    query_hbm, len_hbm, map_hbm, place_hbm, rows_hbm, text_hbm,
    cache, put_out, values_out, weights_out, partial_out,
    query, length, maps, places, rows, text, main_out, main_in, own_out, own_in, place_out, place_in,
    heads, scores, part_out, part_in,
    small_sem, rows_sem, text_sem, main_send, main_recv, own_send, own_recv,
    place_send, place_recv, part_send, part_recv,
):
    patch_count, seq_count, req_count = dims
    layers, src_rows, full = rows.shape
    text_dev = text.shape[1]
    kvw = full // 2
    group = HEADS // KV_HEADS
    groups = patch_count * req_count
    per = src_rows // groups
    half = patch_count // 2
    side = (seq_count - 1) * HEAD_DIM
    main_width = 2 * side
    scale = 1.0 / math.sqrt(HEAD_DIM)
    patch, seq, req = (lax.axis_index(a) for a in ("patch", "seq", "req"))
    me = patch * req_count + req
    near = near_hops(patch_count, req_count)
    far = [far_hops(patch_count, req_count, k) for k in range(half)]
    hops = near + [hop for wave in far for hop in wave]
    f32, bf16 = jnp.float32, jnp.bfloat16
    upper = patch // half

    def partner(hop):
        kind, i, c = hop
        r = lax.rem(req + c, req_count)
        if kind == "near":
            return upper * half + lax.rem(lax.rem(patch, half) + i, half), r
        return (1 - upper) * (patch_count - 1 - i) + upper * i, r

    def rows_copy(l):
        return pltpu.make_async_copy(rows_hbm.at[l], rows.at[l], rows_sem.at[l])

    def text_copy(l):
        return pltpu.make_async_copy(text_hbm.at[l, 0], text.at[l], text_sem.at[l])

    small = [
        pltpu.make_async_copy(map_hbm, maps, small_sem.at[0]),
        pltpu.make_async_copy(place_hbm, places, small_sem.at[1]),
        pltpu.make_async_copy(query_hbm, query, small_sem.at[2]),
        pltpu.make_async_copy(len_hbm, length, small_sem.at[3]),
    ]
    small[0].start()
    rows_copy(0).start()
    barrier = pltpu.get_barrier_semaphore()
    for hop in hops:
        p, r = partner(hop)
        pl.semaphore_signal(barrier, inc=1, device_id=(p, seq, r), device_id_type=MESH)
    for d in range(1, seq_count):
        s = lax.rem(seq + d, seq_count)
        pl.semaphore_signal(barrier, inc=1, device_id=(patch, s, req), device_id_type=MESH)
    for copy in small[1:]:
        copy.start()

    def lanes_of(d, base=0):
        g = lax.rem(seq + d, seq_count)
        return pl.ds(pl.multiple_of(base + g * HEAD_DIM, HEAD_DIM), HEAD_DIM)

    owner = lax.broadcasted_iota(jnp.int32, (groups, src_rows), 0)
    row_i = lax.broadcasted_iota(jnp.int32, (src_rows, src_rows), 0)
    col_i = lax.broadcasted_iota(jnp.int32, (src_rows, src_rows), 1)
    before = (row_i < col_i).astype(f32).astype(bf16)
    small[0].wait()
    mine = maps[...] == owner
    rank = jnp.dot(mine.astype(f32).astype(bf16), before, preferred_element_type=f32)
    slot = jnp.sum(
        jnp.where(mine, rank + (owner * per).astype(f32), 0.0), axis=0, keepdims=True
    )
    pick = (row_i == slot.astype(jnp.int32)).astype(f32).astype(bf16)

    def place_copy(hop):
        p, r = partner(hop)
        q = p * req_count + r
        return pltpu.make_async_remote_copy(
            src_ref=place_out, dst_ref=place_in.at[me],
            send_sem=place_send.at[q], recv_sem=place_recv.at[me],
            device_id=(p, seq, r), device_id_type=MESH,
        )

    def place_wait(hop):
        p, r = partner(hop)
        q = p * req_count + r
        pltpu.make_async_remote_copy(
            src_ref=place_out, dst_ref=place_in.at[q],
            send_sem=place_send.at[q], recv_sem=place_recv.at[q],
            device_id=(p, seq, r), device_id_type=MESH,
        ).wait_recv()

    def main_copy(l, hop):
        p, r = partner(hop)
        q = p * req_count + r
        return pltpu.make_async_remote_copy(
            src_ref=main_out.at[l, q], dst_ref=main_in.at[l, me],
            send_sem=main_send.at[l, q], recv_sem=main_recv.at[l, me],
            device_id=(p, seq, r), device_id_type=MESH,
        )

    def main_wait(l, hop):
        p, r = partner(hop)
        q = p * req_count + r
        pltpu.make_async_remote_copy(
            src_ref=main_out.at[l, q], dst_ref=main_in.at[l, q],
            send_sem=main_send.at[l, q], recv_sem=main_recv.at[l, q],
            device_id=(p, seq, r), device_id_type=MESH,
        ).wait_recv()

    def own_copy(i, hop):
        p, r = partner(hop)
        q = p * req_count + r
        return pltpu.make_async_remote_copy(
            src_ref=own_out.at[i, q], dst_ref=own_in.at[i, me],
            send_sem=own_send.at[i, q], recv_sem=own_recv.at[i, me],
            device_id=(p, seq, r), device_id_type=MESH,
        )

    def own_wait(i, hop):
        p, r = partner(hop)
        q = p * req_count + r
        pltpu.make_async_remote_copy(
            src_ref=own_out.at[i, q], dst_ref=own_in.at[i, q],
            send_sem=own_send.at[i, q], recv_sem=own_recv.at[i, q],
            device_id=(p, seq, r), device_id_type=MESH,
        ).wait_recv()

    def part_copy(l, d):
        s = lax.rem(seq + d, seq_count)
        return pltpu.make_async_remote_copy(
            src_ref=part_out.at[l, d], dst_ref=part_in.at[l, d],
            send_sem=part_send.at[l, d], recv_sem=part_recv.at[l, d],
            device_id=(patch, s, req), device_id_type=MESH,
        )

    for l in range(layers):
        rows_copy(l).wait()
        if l == 0:
            for m in range(1, layers):
                rows_copy(m).start()
        turned = jnp.concatenate(
            [rows[l, :, lanes_of(d)] for d in range(1, seq_count)]
            + [rows[l, :, lanes_of(d, kvw)] for d in range(1, seq_count)],
            axis=1,
        )
        moved = jnp.dot(pick, turned, preferred_element_type=f32).astype(bf16)
        main_out[l] = moved.reshape(groups, per, main_width)
        if l == 0:
            pl.semaphore_wait(barrier, len(hops) + seq_count - 1)
        for hop in near:
            main_copy(l, hop).start()
        for wave in far[:-1]:
            for hop in wave:
                main_copy(l, hop).start()
        if l == 0:
            small[1].wait()
            local = (places[...] - seq * src_rows).astype(f32).astype(bf16)
            place_sorted = lax.dot_general(
                jnp.broadcast_to(local, (PAD, src_rows)), pick, NT,
                preferred_element_type=f32,
            )
            place_out[...] = place_sorted[0:1].astype(jnp.int32)
            place_in[me] = place_sorted[0:1].astype(jnp.int32)
            for hop in hops:
                place_copy(hop).start()
    for l in range(layers):
        turned = jnp.concatenate([rows[l, :, lanes_of(0)], rows[l, :, lanes_of(0, kvw)]], axis=1)
        moved = jnp.dot(pick, turned, preferred_element_type=f32).astype(bf16)
        own_out[0, :, l] = moved[:, :HEAD_DIM].reshape(groups, per, HEAD_DIM)
        own_out[1, :, l] = moved[:, HEAD_DIM:].reshape(groups, per, HEAD_DIM)
    for i in range(2):
        for hop in near:
            own_copy(i, hop).start()
    for l in range(layers):
        for hop in far[-1]:
            main_copy(l, hop).start()
    for wave in far:
        for i in range(2):
            for hop in wave:
                own_copy(i, hop).start()
    for l in range(layers):
        text_copy(l).start()
    for l in range(layers):
        main_in[l, me] = main_out[l, me]
    for i in range(2):
        own_in[i, me] = own_out[i, me]

    small[2].wait()
    lines = query[...].astype(f32)
    for l in range(layers):
        for g in range(KV_HEADS):
            heads[l, g * PAD:(g + 1) * PAD, :] = jnp.concatenate(
                [
                    lines[l:l + 1, (g * group + h) * HEAD_DIM:(g * group + h + 1) * HEAD_DIM]
                    for h in range(group)
                ] + [jnp.zeros((PAD - group, HEAD_DIM), f32)],
                axis=0,
            )

    def head_block(l, d):
        g = lax.rem(seq + d, seq_count)
        return heads[l, pl.ds(pl.multiple_of(g * PAD, PAD), PAD), :]

    small[3].wait()
    positions = seq * text_dev + lax.broadcasted_iota(
        jnp.int32, (KV_HEADS * PAD, text_dev), 1
    )
    used = positions < length[0]
    lane_group = lax.broadcasted_iota(jnp.int32, (PAD, kvw), 1) // HEAD_DIM
    for l in range(layers):
        spread = jnp.concatenate(
            [
                jnp.where(
                    lane_group == lax.rem(seq + d, seq_count),
                    jnp.concatenate([head_block(l, d)] * KV_HEADS, axis=1),
                    0.0,
                )
                for d in range(seq_count)
            ],
            axis=0,
        ).astype(bf16)
        text_copy(l).wait()
        raw = lax.dot_general(
            spread, text[l, :, :kvw], NT, preferred_element_type=f32
        ) * scale
        scores[l] = jnp.where(used, raw, -jnp.inf)

    for hop in hops:
        place_wait(hop)
    wanted = (row_i == me * per + lax.rem(col_i, per)).astype(f32).astype(bf16)
    lanes = jnp.dot(
        place_in[...].reshape(groups, src_rows).astype(f32).astype(bf16), wanted,
        preferred_element_type=f32,
    )
    source = lax.broadcasted_iota(jnp.int32, (groups, src_rows), 1) // per
    place = jnp.sum(jnp.where(source == owner, lanes, 0.0), axis=0, keepdims=True)
    put = (row_i == place.astype(jnp.int32)).astype(f32).astype(bf16)
    put_out[...] = put

    zeros = jnp.zeros((PAD, HEAD_DIM), f32)
    for l in range(layers):
        spread = jnp.concatenate(
            [
                jnp.concatenate(
                    [head_block(l, d) if c == d else zeros for c in range(1, seq_count)],
                    axis=1,
                )
                for d in range(1, seq_count)
            ],
            axis=0,
        ).astype(bf16)
        for hop in hops:
            main_wait(l, hop)
        block = main_in[l].reshape(src_rows, main_width)
        image_scores = lax.dot_general(
            spread, block[:, :side], NT, preferred_element_type=f32
        ) * scale
        text_scores = scores[l, PAD:, :]
        top = jnp.maximum(
            jnp.max(text_scores, axis=1, keepdims=True),
            jnp.max(image_scores, axis=1, keepdims=True),
        )
        text_w = jnp.exp(text_scores - top)
        image_w = jnp.exp(image_scores - top)
        total = jnp.sum(text_w, axis=1, keepdims=True) + jnp.sum(
            image_w, axis=1, keepdims=True
        )
        image_sums = jnp.dot(
            image_w.astype(bf16), block[:, side:], preferred_element_type=f32
        )
        for d in range(1, seq_count):
            at = slice((d - 1) * PAD, d * PAD)
            text_sums = jnp.dot(
                text_w[at].astype(bf16), text[l, :, lanes_of(d, kvw)],
                preferred_element_type=f32,
            )
            part_out[l, d, :, :HEAD_DIM] = (
                text_sums + image_sums[at, (d - 1) * HEAD_DIM:d * HEAD_DIM]
            )
            part_out[l, d, :, HEAD_DIM:2 * HEAD_DIM] = jnp.broadcast_to(
                top[at], (PAD, HEAD_DIM)
            )
            part_out[l, d, :, 2 * HEAD_DIM:] = jnp.broadcast_to(total[at], (PAD, HEAD_DIM))
            part_copy(l, d).start()
        moved = jnp.dot(put, block, preferred_element_type=f32).astype(bf16)
        for d in range(1, seq_count):
            cache[l, 0, :, lanes_of(d)] = moved[:, (d - 1) * HEAD_DIM:d * HEAD_DIM]
            cache[l, 0, :, lanes_of(d, kvw)] = moved[
                :, side + (d - 1) * HEAD_DIM:side + d * HEAD_DIM
            ]

    for hop in hops:
        own_wait(0, hop)
    own_keys = [own_in[0, :, l].reshape(src_rows, HEAD_DIM) for l in range(layers)]
    mine_now = []
    for l in range(layers):
        image_scores = lax.dot_general(
            head_block(l, 0).astype(bf16), own_keys[l], NT, preferred_element_type=f32
        ) * scale
        text_scores = scores[l, :PAD, :]
        top = jnp.maximum(
            jnp.max(text_scores, axis=1, keepdims=True),
            jnp.max(image_scores, axis=1, keepdims=True),
        )
        text_w = jnp.exp(text_scores - top)
        image_w = jnp.exp(image_scores - top)
        total = jnp.sum(text_w, axis=1, keepdims=True) + jnp.sum(
            image_w, axis=1, keepdims=True
        )
        value = jnp.dot(
            text_w.astype(bf16), text[l, :, lanes_of(0, kvw)], preferred_element_type=f32
        )
        weights_out[l * PAD:(l + 1) * PAD, :] = image_w
        mine_now.append(
            (value, jnp.broadcast_to(top, (PAD, HEAD_DIM)), jnp.broadcast_to(total, (PAD, HEAD_DIM)))
        )
    moved = jnp.dot(
        put, jnp.concatenate(own_keys, axis=1), preferred_element_type=f32
    ).astype(bf16)
    for l in range(layers):
        cache[l, 0, :, lanes_of(0)] = moved[:, l * HEAD_DIM:(l + 1) * HEAD_DIM]

    for l in range(layers):
        for d in range(1, seq_count):
            part_copy(l, d).wait_recv()
        cells = [mine_now[l]] + [
            tuple(part_in[l, d, :, i * HEAD_DIM:(i + 1) * HEAD_DIM] for i in range(3))
            for d in range(1, seq_count)
        ]
        top = functools.reduce(jnp.maximum, [c[1] for c in cells])
        factors = [jnp.exp(c[1] - top) for c in cells]
        partial_out[l, :, :HEAD_DIM] = factors[0]
        partial_out[l, :, HEAD_DIM:2 * HEAD_DIM] = sum(
            f * c[0] for f, c in zip(factors, cells)
        )
        partial_out[l, :, 2 * HEAD_DIM:] = sum(f * c[2] for f, c in zip(factors, cells))

    for l in range(layers):
        for hop in hops:
            main_copy(l, hop).wait_send()
        for d in range(1, seq_count):
            part_copy(l, d).wait_send()
    for hop in hops:
        place_copy(hop).wait_send()
        own_copy(0, hop).wait_send()
    for hop in hops:
        own_wait(1, hop)
    for l in range(layers):
        values_out[:, l * HEAD_DIM:(l + 1) * HEAD_DIM] = own_in[1, :, l].reshape(
            src_rows, HEAD_DIM
        )
    for hop in hops:
        own_copy(1, hop).wait_send()


def finish(
    dims, cache, put, values, weights, partial, att_out, cache_out, att, last, sem, last_sem
):
    _, seq_count, _ = dims
    layers, _, src_rows, full = cache.shape
    kvw = full // 2
    group = HEADS // KV_HEADS
    seq = lax.axis_index("seq")
    f32, bf16 = jnp.float32, jnp.bfloat16

    def lanes_of(d):
        g = lax.rem(seq + d, seq_count)
        return pl.ds(pl.multiple_of(kvw + g * HEAD_DIM, HEAD_DIM), HEAD_DIM)

    early = []
    for l in range(layers):
        early.append(
            pltpu.make_async_copy(
                cache.at[l, 0, :, pl.ds(0, kvw)], cache_out.at[l, 0, :, pl.ds(0, kvw)],
                sem.at[l, 0],
            )
        )
        for d in range(1, seq_count):
            early.append(
                pltpu.make_async_copy(
                    cache.at[l, 0, :, lanes_of(d)], cache_out.at[l, 0, :, lanes_of(d)],
                    sem.at[l, d],
                )
            )
    for copy in early:
        copy.start()
    late = []
    both = jnp.concatenate([put[...], weights[...].astype(bf16)], axis=0)
    moved = jnp.dot(both, values[...], preferred_element_type=f32)
    for l in range(layers):
        at = slice(l * HEAD_DIM, (l + 1) * HEAD_DIM)
        last[l] = moved[:src_rows, at].astype(bf16)
        late.append(
            pltpu.make_async_copy(
                last.at[l], cache_out.at[l, 0, :, lanes_of(0)], last_sem.at[l]
            )
        )
        late[-1].start()
    lines = []
    for l in range(layers):
        value = moved[
            src_rows + l * PAD:src_rows + (l + 1) * PAD, l * HEAD_DIM:(l + 1) * HEAD_DIM
        ]
        factor = partial[l, :, :HEAD_DIM]
        summed = partial[l, :, HEAD_DIM:2 * HEAD_DIM]
        result = (summed + factor * value) / partial[l, :, 2 * HEAD_DIM:]
        lines.append(jnp.concatenate([result[h:h + 1] for h in range(group)], axis=1))
    att[...] = jnp.concatenate(lines, axis=0).astype(bf16)
    late.append(pltpu.make_async_copy(att, att_out, last_sem.at[layers]))
    late[-1].start()
    for copy in early + late:
        copy.wait()


def body(dims, query, text_cache, text_len, image_rows, patch_map, image_places):
    patch_count, seq_count, req_count = dims
    layers, req_dev, query_width = query.shape
    text_dev, full = text_cache.shape[2:]
    src_rows = image_rows.shape[1]
    groups = patch_count * req_count
    assert req_dev == 1 and seq_count == KV_HEADS and full == 2 * KV_HEADS * HEAD_DIM
    assert patch_count % 2 == 0
    per = src_rows // groups
    main_width = full - 2 * HEAD_DIM
    rows_padded = KV_HEADS * PAD
    bf16, f32, i32 = jnp.bfloat16, jnp.float32, jnp.int32
    dma = pltpu.SemaphoreType.DMA
    vmem = pl.BlockSpec(memory_space=pltpu.VMEM)
    hbm = pl.BlockSpec(memory_space=pltpu.HBM)
    att_shape = jax.ShapeDtypeStruct((layers, query_width // seq_count), bf16)
    cache_shape = jax.ShapeDtypeStruct((layers, 1, src_rows, full), bf16)
    in_hbm = lambda x: pltpu.with_memory_space_constraint(x, pltpu.HBM)
    in_vmem = lambda x: pltpu.with_memory_space_constraint(x, pltpu.VMEM)
    state = pl.pallas_call(
        functools.partial(exchange, dims),
        out_shape=(
            pltpu.VMEM(cache_shape.shape, bf16),
            pltpu.VMEM((src_rows, src_rows), bf16),
            pltpu.VMEM((src_rows, layers * HEAD_DIM), bf16),
            pltpu.VMEM((layers * PAD, src_rows), f32),
            pltpu.VMEM((layers, PAD, 3 * HEAD_DIM), f32),
        ),
        in_specs=[hbm, pl.BlockSpec(memory_space=pl.ANY), hbm, hbm, hbm, hbm],
        out_specs=(vmem,) * 5,
        scratch_shapes=[
            pltpu.VMEM((layers, query_width), bf16),
            pltpu.SMEM((1,), i32),
            pltpu.VMEM((1, src_rows), i32),
            pltpu.VMEM((1, src_rows), i32),
            pltpu.VMEM((layers, src_rows, full), bf16),
            pltpu.VMEM((layers, text_dev, full), bf16),
            pltpu.VMEM((layers, groups, per, main_width), bf16),
            pltpu.VMEM((layers, groups, per, main_width), bf16),
            pltpu.VMEM((2, groups, layers, per, HEAD_DIM), bf16),
            pltpu.VMEM((2, groups, layers, per, HEAD_DIM), bf16),
            pltpu.VMEM((1, src_rows), i32),
            pltpu.VMEM((groups, 1, src_rows), i32),
            pltpu.VMEM((layers, rows_padded, HEAD_DIM), f32),
            pltpu.VMEM((layers, rows_padded, text_dev), f32),
            pltpu.VMEM((layers, seq_count, PAD, 3 * HEAD_DIM), f32),
            pltpu.VMEM((layers, seq_count, PAD, 3 * HEAD_DIM), f32),
            dma((4,)), dma((layers,)), dma((layers,)),
            dma((layers, groups)), dma((layers, groups)), dma((2, groups)), dma((2, groups)),
            dma((groups,)), dma((groups,)), dma((layers, seq_count)), dma((layers, seq_count)),
        ],
        compiler_params=pltpu.CompilerParams(
            collective_id=0, has_side_effects=True, vmem_limit_bytes=32 * 1024 * 1024
        ),
    )(
        in_hbm(query.reshape(layers, query_width)), text_len,
        in_hbm(patch_map.reshape(1, src_rows)), in_hbm(image_places.reshape(1, src_rows)),
        in_hbm(image_rows), in_hbm(text_cache),
    )
    attended, cache = pl.pallas_call(
        functools.partial(finish, dims),
        out_shape=(att_shape, cache_shape),
        in_specs=[vmem] * 5,
        out_specs=(hbm, hbm),
        scratch_shapes=[
            pltpu.VMEM(att_shape.shape, bf16),
            pltpu.VMEM((layers, src_rows, HEAD_DIM), bf16),
            dma((layers, seq_count)), dma((layers + 1,)),
        ],
    )(*(in_vmem(x) for x in state))
    return attended.reshape(layers, 1, query_width // seq_count), cache


def solution(mesh):
    dims = tuple(mesh.shape[a] for a in ("patch", "seq", "req"))
    return jax.shard_map(
        functools.partial(body, dims),
        mesh=mesh,
        in_specs=(
            P(None, ("patch", "req"), None),
            P(None, ("patch", "req"), "seq", None),
            P(("patch", "req")),
            P(None, ("patch", "seq", "req"), None),
            P(("patch", "seq", "req")),
            P(("patch", "seq", "req")),
        ),
        out_specs=(P(None, ("patch", "req"), "seq"), P(None, ("patch", "req"), "seq", None)),
        check_vma=False,
    )
```

```python
import functools
import math

import jax
import jax.numpy as jnp
from jax import lax
from jax.experimental import pallas as pl
from jax.experimental.pallas import tpu as pltpu
from jax.sharding import PartitionSpec as P

HEADS = 28
KV_HEADS = 4
HEAD_DIM = 128
PAD = 8
MESH = pl.DeviceIdType.MESH
NT = (((1,), (1,)), ((), ()))


def near_hops(patch_count, req_count):
    half = patch_count // 2
    beside = [("near", i, c) for i in range(1, half) for c in range(req_count)]
    return beside + [("near", 0, c) for c in range(1, req_count)]


def far_hops(patch_count, req_count, k):
    return [("far", k, c) for c in range(req_count)]


def exchange(
    dims,
    query_hbm, len_hbm, map_hbm, place_hbm, rows_hbm, text_hbm,
    cache, put_out, values_in, weights_out, partial_out,
    query, length, maps, places, rows, text, main_out, main_in, own_out, keys_in, place_out, place_in,
    heads, scores, part_out, part_in,
    small_sem, rows_sem, text_sem, main_send, main_recv, own_send, own_recv, place_sem, part_sem,
):
    patch_count, seq_count, req_count = dims
    layers, src_rows, full = rows.shape
    text_dev = text.shape[1]
    kvw = full // 2
    group = HEADS // KV_HEADS
    groups = patch_count * req_count
    per = src_rows // groups
    half = patch_count // 2
    side = (seq_count - 1) * HEAD_DIM
    main_width = 2 * side
    scale = 1.0 / math.sqrt(HEAD_DIM)
    patch, seq, req = (lax.axis_index(a) for a in ("patch", "seq", "req"))
    me = patch * req_count + req
    near = near_hops(patch_count, req_count)
    far = [far_hops(patch_count, req_count, k) for k in range(half)]
    hops = near + [hop for wave in far for hop in wave]
    f32, bf16 = jnp.float32, jnp.bfloat16
    upper = patch // half

    def partner(hop):
        kind, i, c = hop
        r = lax.rem(req + c, req_count)
        if kind == "near":
            return upper * half + lax.rem(lax.rem(patch, half) + i, half), r
        return (1 - upper) * (patch_count - 1 - i) + upper * i, r

    others = pl.ds(0, groups - 1)
    own_in = (keys_in, values_in)
    first_rows = pltpu.make_async_copy(rows_hbm.at[0], rows.at[0], rows_sem.at[0])
    later = pl.ds(1, layers - 1)
    later_rows = pltpu.make_async_copy(rows_hbm.at[later], rows.at[later], rows_sem.at[1])
    text_copy = pltpu.make_async_copy(text_hbm.at[:, 0], text, text_sem.at[0])

    def settle(ref, sem):
        pltpu.make_async_copy(ref, ref, sem).wait()

    small = [
        pltpu.make_async_copy(map_hbm, maps, small_sem.at[0]),
        pltpu.make_async_copy(place_hbm, places, small_sem.at[1]),
        pltpu.make_async_copy(query_hbm, query, small_sem.at[2]),
        pltpu.make_async_copy(len_hbm, length, small_sem.at[3]),
    ]
    small[0].start()
    first_rows.start()
    barrier = pltpu.get_barrier_semaphore()
    for hop in hops:
        p, r = partner(hop)
        pl.semaphore_signal(barrier, inc=1, device_id=(p, seq, r), device_id_type=MESH)
    for d in range(1, seq_count):
        s = lax.rem(seq + d, seq_count)
        pl.semaphore_signal(barrier, inc=1, device_id=(patch, s, req), device_id_type=MESH)
    for copy in small[1:]:
        copy.start()

    def lanes_of(d, base=0):
        g = lax.rem(seq + d, seq_count)
        return pl.ds(pl.multiple_of(base + g * HEAD_DIM, HEAD_DIM), HEAD_DIM)

    owner = lax.broadcasted_iota(jnp.int32, (groups, src_rows), 0)
    row_i = lax.broadcasted_iota(jnp.int32, (src_rows, src_rows), 0)
    col_i = lax.broadcasted_iota(jnp.int32, (src_rows, src_rows), 1)
    before = (row_i < col_i).astype(f32).astype(bf16)
    small[0].wait()
    mine = maps[...] == owner
    rank = jnp.dot(mine.astype(f32).astype(bf16), before, preferred_element_type=f32)
    slot = jnp.sum(
        jnp.where(mine, rank + (owner * per).astype(f32), 0.0), axis=0, keepdims=True
    )
    pick = (row_i == slot.astype(jnp.int32)).astype(f32).astype(bf16)

    def place_copy(hop):
        p, r = partner(hop)
        return pltpu.make_async_remote_copy(
            src_ref=place_out, dst_ref=place_in.at[me],
            send_sem=place_sem.at[0], recv_sem=place_sem.at[1],
            device_id=(p, seq, r), device_id_type=MESH,
        )

    def main_copy(l, hop):
        p, r = partner(hop)
        return pltpu.make_async_remote_copy(
            src_ref=main_out.at[l, p * req_count + r], dst_ref=main_in.at[l, me],
            send_sem=main_send.at[0], recv_sem=main_recv.at[l],
            device_id=(p, seq, r), device_id_type=MESH,
        )

    def own_copy(i, hop):
        p, r = partner(hop)
        return pltpu.make_async_remote_copy(
            src_ref=own_out.at[i, p * req_count + r], dst_ref=own_in[i].at[me],
            send_sem=own_send.at[0], recv_sem=own_recv.at[i],
            device_id=(p, seq, r), device_id_type=MESH,
        )

    def part_copy(l, d):
        s = lax.rem(seq + d, seq_count)
        return pltpu.make_async_remote_copy(
            src_ref=part_out.at[l, d], dst_ref=part_in.at[l, d],
            send_sem=part_sem.at[0], recv_sem=part_sem.at[1],
            device_id=(patch, s, req), device_id_type=MESH,
        )

    for l in range(layers):
        if l == 0:
            first_rows.wait()
            later_rows.start()
        if l == 1:
            later_rows.wait()
        turned = jnp.concatenate(
            [rows[l, :, lanes_of(d)] for d in range(1, seq_count)]
            + [rows[l, :, lanes_of(d, kvw)] for d in range(1, seq_count)],
            axis=1,
        )
        moved = jnp.dot(pick, turned, preferred_element_type=f32).astype(bf16)
        main_out[l] = moved.reshape(groups, per, main_width)
        if l == 0:
            pl.semaphore_wait(barrier, len(hops) + seq_count - 1)
        for hop in near:
            main_copy(l, hop).start()
        for wave in far[:-1]:
            for hop in wave:
                main_copy(l, hop).start()
        if l == 0:
            small[1].wait()
            local = (places[...] - seq * src_rows).astype(f32).astype(bf16)
            place_sorted = lax.dot_general(
                jnp.broadcast_to(local, (PAD, src_rows)), pick, NT,
                preferred_element_type=f32,
            )
            place_out[...] = place_sorted[0:1].astype(jnp.int32)
            place_in[me] = place_sorted[0:1].astype(jnp.int32)
            for hop in hops:
                place_copy(hop).start()
    for l in range(layers):
        turned = jnp.concatenate([rows[l, :, lanes_of(0)], rows[l, :, lanes_of(0, kvw)]], axis=1)
        moved = jnp.dot(pick, turned, preferred_element_type=f32).astype(bf16)
        own_out[0, :, l] = moved[:, :HEAD_DIM].reshape(groups, per, HEAD_DIM)
        own_out[1, :, l] = moved[:, HEAD_DIM:].reshape(groups, per, HEAD_DIM)
    for i in range(2):
        for hop in near:
            own_copy(i, hop).start()
    for l in range(layers):
        for hop in far[-1]:
            main_copy(l, hop).start()
    for wave in far:
        for i in range(2):
            for hop in wave:
                own_copy(i, hop).start()
    text_copy.start()
    for l in range(layers):
        main_in[l, me] = main_out[l, me]
    for i in range(2):
        own_in[i][me] = own_out[i, me]

    small[2].wait()
    lines = query[...].astype(f32)
    for l in range(layers):
        for g in range(KV_HEADS):
            heads[l, g * PAD:(g + 1) * PAD, :] = jnp.concatenate(
                [
                    lines[l:l + 1, (g * group + h) * HEAD_DIM:(g * group + h + 1) * HEAD_DIM]
                    for h in range(group)
                ] + [jnp.zeros((PAD - group, HEAD_DIM), f32)],
                axis=0,
            )

    def head_block(l, d):
        g = lax.rem(seq + d, seq_count)
        return heads[l, pl.ds(pl.multiple_of(g * PAD, PAD), PAD), :]

    small[3].wait()
    positions = seq * text_dev + lax.broadcasted_iota(
        jnp.int32, (KV_HEADS * PAD, text_dev), 1
    )
    used = positions < length[0]
    lane_group = lax.broadcasted_iota(jnp.int32, (PAD, kvw), 1) // HEAD_DIM
    for l in range(layers):
        spread = jnp.concatenate(
            [
                jnp.where(
                    lane_group == lax.rem(seq + d, seq_count),
                    jnp.concatenate([head_block(l, d)] * KV_HEADS, axis=1),
                    0.0,
                )
                for d in range(seq_count)
            ],
            axis=0,
        ).astype(bf16)
        if l == 0:
            text_copy.wait()
        raw = lax.dot_general(
            spread, text[l, :, :kvw], NT, preferred_element_type=f32
        ) * scale
        scores[l] = jnp.where(used, raw, -jnp.inf)

    settle(place_in.at[others], place_sem.at[1])
    wanted = (row_i == me * per + lax.rem(col_i, per)).astype(f32).astype(bf16)
    lanes = jnp.dot(
        place_in[...].reshape(groups, src_rows).astype(f32).astype(bf16), wanted,
        preferred_element_type=f32,
    )
    source = lax.broadcasted_iota(jnp.int32, (groups, src_rows), 1) // per
    place = jnp.sum(jnp.where(source == owner, lanes, 0.0), axis=0, keepdims=True)
    put = (row_i == place.astype(jnp.int32)).astype(f32).astype(bf16)
    put_out[...] = put

    zeros = jnp.zeros((PAD, HEAD_DIM), f32)
    for l in range(layers):
        spread = jnp.concatenate(
            [
                jnp.concatenate(
                    [head_block(l, d) if c == d else zeros for c in range(1, seq_count)],
                    axis=1,
                )
                for d in range(1, seq_count)
            ],
            axis=0,
        ).astype(bf16)
        settle(main_in.at[l, others], main_recv.at[l])
        block = main_in[l].reshape(src_rows, main_width)
        image_scores = lax.dot_general(
            spread, block[:, :side], NT, preferred_element_type=f32
        ) * scale
        text_scores = scores[l, PAD:, :]
        top = jnp.maximum(
            jnp.max(text_scores, axis=1, keepdims=True),
            jnp.max(image_scores, axis=1, keepdims=True),
        )
        text_w = jnp.exp(text_scores - top)
        image_w = jnp.exp(image_scores - top)
        total = jnp.sum(text_w, axis=1, keepdims=True) + jnp.sum(
            image_w, axis=1, keepdims=True
        )
        image_sums = jnp.dot(
            image_w.astype(bf16), block[:, side:], preferred_element_type=f32
        )
        for d in range(1, seq_count):
            at = slice((d - 1) * PAD, d * PAD)
            text_sums = jnp.dot(
                text_w[at].astype(bf16), text[l, :, lanes_of(d, kvw)],
                preferred_element_type=f32,
            )
            part_out[l, d, :, :HEAD_DIM] = (
                text_sums + image_sums[at, (d - 1) * HEAD_DIM:d * HEAD_DIM]
            )
            part_out[l, d, :, HEAD_DIM:2 * HEAD_DIM] = jnp.broadcast_to(
                top[at], (PAD, HEAD_DIM)
            )
            part_out[l, d, :, 2 * HEAD_DIM:] = jnp.broadcast_to(total[at], (PAD, HEAD_DIM))
            part_copy(l, d).start()
        moved = jnp.dot(put, block, preferred_element_type=f32).astype(bf16)
        for d in range(1, seq_count):
            cache[l, 0, :, lanes_of(d)] = moved[:, (d - 1) * HEAD_DIM:d * HEAD_DIM]
            cache[l, 0, :, lanes_of(d, kvw)] = moved[
                :, side + (d - 1) * HEAD_DIM:side + d * HEAD_DIM
            ]

    settle(keys_in.at[others], own_recv.at[0])
    own_keys = [keys_in[:, l].reshape(src_rows, HEAD_DIM) for l in range(layers)]
    mine_now = []
    for l in range(layers):
        image_scores = lax.dot_general(
            head_block(l, 0).astype(bf16), own_keys[l], NT, preferred_element_type=f32
        ) * scale
        text_scores = scores[l, :PAD, :]
        top = jnp.maximum(
            jnp.max(text_scores, axis=1, keepdims=True),
            jnp.max(image_scores, axis=1, keepdims=True),
        )
        text_w = jnp.exp(text_scores - top)
        image_w = jnp.exp(image_scores - top)
        total = jnp.sum(text_w, axis=1, keepdims=True) + jnp.sum(
            image_w, axis=1, keepdims=True
        )
        value = jnp.dot(
            text_w.astype(bf16), text[l, :, lanes_of(0, kvw)], preferred_element_type=f32
        )
        weights_out[l * PAD:(l + 1) * PAD, :] = image_w
        mine_now.append(
            (value, jnp.broadcast_to(top, (PAD, HEAD_DIM)), jnp.broadcast_to(total, (PAD, HEAD_DIM)))
        )
    moved = jnp.dot(
        put, jnp.concatenate(own_keys, axis=1), preferred_element_type=f32
    ).astype(bf16)
    for l in range(layers):
        cache[l, 0, :, lanes_of(0)] = moved[:, l * HEAD_DIM:(l + 1) * HEAD_DIM]

    beside = pl.ds(1, seq_count - 1)
    settle(part_in.at[:, beside], part_sem.at[1])
    for l in range(layers):
        cells = [mine_now[l]] + [
            tuple(part_in[l, d, :, i * HEAD_DIM:(i + 1) * HEAD_DIM] for i in range(3))
            for d in range(1, seq_count)
        ]
        top = functools.reduce(jnp.maximum, [c[1] for c in cells])
        factors = [jnp.exp(c[1] - top) for c in cells]
        partial_out[l, :, :HEAD_DIM] = factors[0]
        partial_out[l, :, HEAD_DIM:2 * HEAD_DIM] = sum(
            f * c[0] for f, c in zip(factors, cells)
        )
        partial_out[l, :, 2 * HEAD_DIM:] = sum(f * c[2] for f, c in zip(factors, cells))

    settle(main_out.at[:, others], main_send.at[0])
    settle(place_in.at[others], place_sem.at[0])
    settle(part_out.at[:, beside], part_sem.at[0])
    settle(own_out.at[:, others], own_send.at[0])
    settle(values_in.at[others], own_recv.at[1])


def finish(
    dims, cache, put, values, weights, partial, att_out, cache_out, att, last, sem
):
    _, seq_count, _ = dims
    layers, _, src_rows, full = cache.shape
    kvw = full // 2
    group = HEADS // KV_HEADS
    seq = lax.axis_index("seq")
    f32, bf16 = jnp.float32, jnp.bfloat16

    def lanes_of(d):
        g = lax.rem(seq + d, seq_count)
        return pl.ds(pl.multiple_of(kvw + g * HEAD_DIM, HEAD_DIM), HEAD_DIM)

    for l in range(layers):
        pltpu.make_async_copy(
            cache.at[l, 0, :, pl.ds(0, kvw)], cache_out.at[l, 0, :, pl.ds(0, kvw)], sem.at[0]
        ).start()
        for d in range(1, seq_count):
            pltpu.make_async_copy(
                cache.at[l, 0, :, lanes_of(d)], cache_out.at[l, 0, :, lanes_of(d)], sem.at[0]
            ).start()
    own = [values[:, l].reshape(src_rows, HEAD_DIM) for l in range(layers)]
    both = jnp.concatenate([put[...], weights[...].astype(bf16)], axis=0)
    moved = jnp.dot(both, jnp.concatenate(own, axis=1), preferred_element_type=f32)
    for l in range(layers):
        at = slice(l * HEAD_DIM, (l + 1) * HEAD_DIM)
        last[l] = moved[:src_rows, at].astype(bf16)
        pltpu.make_async_copy(
            last.at[l], cache_out.at[l, 0, :, lanes_of(0)], sem.at[0]
        ).start()
    lines = []
    for l in range(layers):
        value = moved[
            src_rows + l * PAD:src_rows + (l + 1) * PAD, l * HEAD_DIM:(l + 1) * HEAD_DIM
        ]
        factor = partial[l, :, :HEAD_DIM]
        summed = partial[l, :, HEAD_DIM:2 * HEAD_DIM]
        result = (summed + factor * value) / partial[l, :, 2 * HEAD_DIM:]
        lines.append(jnp.concatenate([result[h:h + 1] for h in range(group)], axis=1))
    att[...] = jnp.concatenate(lines, axis=0).astype(bf16)
    att_copy = pltpu.make_async_copy(att, att_out, sem.at[1])
    att_copy.start()
    pltpu.make_async_copy(cache, cache_out, sem.at[0]).wait()
    att_copy.wait()


def body(dims, query, text_cache, text_len, image_rows, patch_map, image_places):
    patch_count, seq_count, req_count = dims
    layers, req_dev, query_width = query.shape
    text_dev, full = text_cache.shape[2:]
    src_rows = image_rows.shape[1]
    groups = patch_count * req_count
    assert req_dev == 1 and seq_count == KV_HEADS and full == 2 * KV_HEADS * HEAD_DIM
    assert patch_count % 2 == 0
    per = src_rows // groups
    main_width = full - 2 * HEAD_DIM
    rows_padded = KV_HEADS * PAD
    bf16, f32, i32 = jnp.bfloat16, jnp.float32, jnp.int32
    dma = pltpu.SemaphoreType.DMA
    vmem = pl.BlockSpec(memory_space=pltpu.VMEM)
    hbm = pl.BlockSpec(memory_space=pltpu.HBM)
    att_shape = jax.ShapeDtypeStruct((layers, query_width // seq_count), bf16)
    cache_shape = jax.ShapeDtypeStruct((layers, 1, src_rows, full), bf16)
    in_hbm = lambda x: pltpu.with_memory_space_constraint(x, pltpu.HBM)
    in_vmem = lambda x: pltpu.with_memory_space_constraint(x, pltpu.VMEM)
    state = pl.pallas_call(
        functools.partial(exchange, dims),
        out_shape=(
            pltpu.VMEM(cache_shape.shape, bf16),
            pltpu.VMEM((src_rows, src_rows), bf16),
            pltpu.VMEM((groups, layers, per, HEAD_DIM), bf16),
            pltpu.VMEM((layers * PAD, src_rows), f32),
            pltpu.VMEM((layers, PAD, 3 * HEAD_DIM), f32),
        ),
        in_specs=[hbm, pl.BlockSpec(memory_space=pl.ANY), hbm, hbm, hbm, hbm],
        out_specs=(vmem,) * 5,
        scratch_shapes=[
            pltpu.VMEM((layers, query_width), bf16),
            pltpu.SMEM((1,), i32),
            pltpu.VMEM((1, src_rows), i32),
            pltpu.VMEM((1, src_rows), i32),
            pltpu.VMEM((layers, src_rows, full), bf16),
            pltpu.VMEM((layers, text_dev, full), bf16),
            pltpu.VMEM((layers, groups, per, main_width), bf16),
            pltpu.VMEM((layers, groups, per, main_width), bf16),
            pltpu.VMEM((2, groups, layers, per, HEAD_DIM), bf16),
            pltpu.VMEM((groups, layers, per, HEAD_DIM), bf16),
            pltpu.VMEM((1, src_rows), i32),
            pltpu.VMEM((groups, 1, src_rows), i32),
            pltpu.VMEM((layers, rows_padded, HEAD_DIM), f32),
            pltpu.VMEM((layers, rows_padded, text_dev), f32),
            pltpu.VMEM((layers, seq_count, PAD, 3 * HEAD_DIM), f32),
            pltpu.VMEM((layers, seq_count, PAD, 3 * HEAD_DIM), f32),
            dma((4,)), dma((2,)), dma((1,)), dma((1,)), dma((layers,)), dma((1,)), dma((2,)),
            dma((2,)), dma((2,)),
        ],
        compiler_params=pltpu.CompilerParams(
            collective_id=0, has_side_effects=True, vmem_limit_bytes=32 * 1024 * 1024
        ),
    )(
        in_hbm(query.reshape(layers, query_width)), text_len,
        in_hbm(patch_map.reshape(1, src_rows)), in_hbm(image_places.reshape(1, src_rows)),
        in_hbm(image_rows), in_hbm(text_cache),
    )
    attended, cache = pl.pallas_call(
        functools.partial(finish, dims),
        out_shape=(att_shape, cache_shape),
        in_specs=[vmem] * 5,
        out_specs=(hbm, hbm),
        scratch_shapes=[
            pltpu.VMEM(att_shape.shape, bf16),
            pltpu.VMEM((layers, src_rows, HEAD_DIM), bf16),
            dma((2,)),
        ],
    )(*(in_vmem(x) for x in state))
    return attended.reshape(layers, 1, query_width // seq_count), cache


def solution(mesh):
    dims = tuple(mesh.shape[a] for a in ("patch", "seq", "req"))
    return jax.shard_map(
        functools.partial(body, dims),
        mesh=mesh,
        in_specs=(
            P(None, ("patch", "req"), None),
            P(None, ("patch", "req"), "seq", None),
            P(("patch", "req")),
            P(None, ("patch", "seq", "req"), None),
            P(("patch", "seq", "req")),
            P(("patch", "seq", "req")),
        ),
        out_specs=(P(None, ("patch", "req"), "seq"), P(None, ("patch", "req"), "seq", None)),
        check_vma=False,
    )
```

```python
import functools
import math

import jax
import jax.numpy as jnp
from jax import lax
from jax.experimental import pallas as pl
from jax.experimental.pallas import tpu as pltpu
from jax.sharding import PartitionSpec as P

HEADS = 28
KV_HEADS = 4
HEAD_DIM = 128
PAD = 8
MESH = pl.DeviceIdType.MESH
NT = (((1,), (1,)), ((), ()))


def near_hops(patch_count, req_count):
    half = patch_count // 2
    beside = [("near", i, c) for i in range(1, half) for c in range(req_count)]
    return beside + [("near", 0, c) for c in range(1, req_count)]


def far_hops(patch_count, req_count, k):
    return [("far", k, c) for c in range(req_count)]


def exchange(
    dims,
    query_hbm, len_hbm, map_hbm, place_hbm, rows_hbm, text_hbm,
    cache, put_out, values_in, weights_out, partial_out,
    query, length, maps, places, rows, text, main_out, main_in, own_out, keys_in, place_out, place_in,
    heads, scores, part_out, part_in,
    small_sem, rows_sem, text_sem, main_send, main_recv, own_send, own_recv, place_sem, part_sem,
    info,
):
    patch_count, seq_count, req_count = dims
    layers, src_rows, full = rows.shape
    text_dev = text.shape[1]
    kvw = full // 2
    group = HEADS // KV_HEADS
    groups = patch_count * req_count
    per = src_rows // groups
    half = patch_count // 2
    side = (seq_count - 1) * HEAD_DIM
    main_width = 2 * side
    scale = 1.0 / math.sqrt(HEAD_DIM)
    patch, seq, req = (lax.axis_index(a) for a in ("patch", "seq", "req"))
    me = patch * req_count + req
    near = near_hops(patch_count, req_count)
    far = [far_hops(patch_count, req_count, k) for k in range(half)]
    early = near if half <= 2 else [hop for hop in near if hop[1] == 0]
    late = [hop for hop in near if hop not in early]
    ahead = min(2, layers)
    f32, bf16 = jnp.float32, jnp.bfloat16
    upper = patch // half
    inner = jnp.logical_or(patch == half - 1, patch == half)

    def partner(hop):
        kind, i, c = hop
        r = lax.rem(req + c, req_count)
        if kind == "near":
            return upper * half + lax.rem(lax.rem(patch, half) + i, half), r
        return (1 - upper) * (patch_count - 1 - i) + upper * i, r

    others = pl.ds(0, groups - 1)
    own_in = (keys_in, values_in)
    first_rows = pltpu.make_async_copy(rows_hbm.at[0], rows.at[0], rows_sem.at[0])
    later = pl.ds(1, layers - 1)
    later_rows = pltpu.make_async_copy(rows_hbm.at[later], rows.at[later], rows_sem.at[1])
    text_copy = pltpu.make_async_copy(text_hbm.at[:, 0], text, text_sem.at[0])

    def settle(ref, sem):
        pltpu.make_async_copy(ref, ref, sem).wait()

    small = [
        pltpu.make_async_copy(map_hbm, maps, small_sem.at[0]),
        pltpu.make_async_copy(place_hbm, places, small_sem.at[1]),
        pltpu.make_async_copy(query_hbm, query, small_sem.at[2]),
        pltpu.make_async_copy(len_hbm, length, small_sem.at[3]),
    ]
    small[0].start()
    first_rows.start()
    barrier = pltpu.get_barrier_semaphore()

    def tell(sem, p, s, r):
        pl.semaphore_signal(sem, inc=1, device_id=(p, s, r), device_id_type=MESH)

    above, below = patch < patch_count - 1, patch > 0

    @pl.when(above)
    def _():
        for c in range(req_count):
            tell(barrier, patch + 1, seq, lax.rem(req + c, req_count))

    @pl.when(below)
    def _():
        for c in range(req_count):
            tell(barrier, patch - 1, seq, lax.rem(req + c, req_count))

    for c in range(1, req_count):
        tell(barrier, patch, seq, lax.rem(req + c, req_count))

    @pl.when(patch == 0)
    def _():
        for d in range(1, seq_count):
            tell(barrier, patch, lax.rem(seq + d, seq_count), req)

    has_above = 1 - patch // (patch_count - 1)
    has_below = 1 - (patch_count - 1 - patch) // (patch_count - 1)
    arrivals = (
        req_count - 1 + req_count * (has_above + has_below)
        + (seq_count - 1) * (1 - has_below)
    )

    for copy in small[1:]:
        copy.start()

    def lanes_of(d, base=0):
        g = lax.rem(seq + d, seq_count)
        return pl.ds(pl.multiple_of(base + g * HEAD_DIM, HEAD_DIM), HEAD_DIM)

    owner = lax.broadcasted_iota(jnp.int32, (groups, src_rows), 0)
    row_i = lax.broadcasted_iota(jnp.int32, (src_rows, src_rows), 0)
    col_i = lax.broadcasted_iota(jnp.int32, (src_rows, src_rows), 1)
    before = (row_i < col_i).astype(f32).astype(bf16)
    small[0].wait()
    mine = maps[...] == owner
    rank = jnp.dot(mine.astype(f32).astype(bf16), before, preferred_element_type=f32)
    slot = jnp.sum(
        jnp.where(mine, rank + (owner * per).astype(f32), 0.0), axis=0, keepdims=True
    )
    pick = (row_i == slot.astype(jnp.int32)).astype(f32).astype(bf16)

    def place_copy(hop):
        p, r = partner(hop)
        return pltpu.make_async_remote_copy(
            src_ref=place_out, dst_ref=place_in.at[me],
            send_sem=place_sem.at[0], recv_sem=place_sem.at[1],
            device_id=(p, seq, r), device_id_type=MESH,
        )

    def main_copy(l, hop):
        p, r = partner(hop)
        return pltpu.make_async_remote_copy(
            src_ref=main_out.at[l, p * req_count + r], dst_ref=main_in.at[l, me],
            send_sem=main_send.at[0], recv_sem=main_recv.at[l],
            device_id=(p, seq, r), device_id_type=MESH,
        )

    def own_copy(i, hop):
        p, r = partner(hop)
        return pltpu.make_async_remote_copy(
            src_ref=own_out.at[i, p * req_count + r], dst_ref=own_in[i].at[me],
            send_sem=own_send.at[0], recv_sem=own_recv.at[i],
            device_id=(p, seq, r), device_id_type=MESH,
        )

    def part_copy(l, d):
        s = lax.rem(seq + d, seq_count)
        return pltpu.make_async_remote_copy(
            src_ref=part_out.at[l, d], dst_ref=part_in.at[l, d],
            send_sem=part_sem.at[0], recv_sem=part_sem.at[1],
            device_id=(patch, s, req), device_id_type=MESH,
        )

    for l in range(layers):
        if l == 0:
            first_rows.wait()
            later_rows.start()
        if l == 1:
            later_rows.wait()
        turned = jnp.concatenate(
            [rows[l, :, lanes_of(d)] for d in range(1, seq_count)]
            + [rows[l, :, lanes_of(d, kvw)] for d in range(1, seq_count)],
            axis=1,
        )
        moved = jnp.dot(pick, turned, preferred_element_type=f32).astype(bf16)
        main_out[l] = moved.reshape(groups, per, main_width)
        if l == 0:
            pl.semaphore_wait(barrier, arrivals)

            @pl.when(jnp.logical_and(patch == 1, above))
            def _():
                tell(info.at[1], patch + 1, seq, req)

            @pl.when(jnp.logical_and(patch == patch_count - 2, below))
            def _():
                tell(info.at[0], patch - 1, seq, req)

        for hop in early:
            main_copy(l, hop).start()
        if l < ahead:

            @pl.when(inner)
            def _():
                for hop in far[-1]:
                    main_copy(l, hop).start()

        if l == 0:
            small[1].wait()
            local = (places[...] - seq * src_rows).astype(f32).astype(bf16)
            place_sorted = lax.dot_general(
                jnp.broadcast_to(local, (PAD, src_rows)), pick, NT,
                preferred_element_type=f32,
            )
            place_out[...] = place_sorted[0:1].astype(jnp.int32)
            place_in[me] = place_sorted[0:1].astype(jnp.int32)
            for hop in early:
                place_copy(hop).start()
    for l in range(layers):
        turned = jnp.concatenate([rows[l, :, lanes_of(0)], rows[l, :, lanes_of(0, kvw)]], axis=1)
        moved = jnp.dot(pick, turned, preferred_element_type=f32).astype(bf16)
        own_out[0, :, l] = moved[:, :HEAD_DIM].reshape(groups, per, HEAD_DIM)
        own_out[1, :, l] = moved[:, HEAD_DIM:].reshape(groups, per, HEAD_DIM)
    for i in range(2):
        for hop in early:
            own_copy(i, hop).start()

    @pl.when(patch < patch_count - 2)
    def _():
        pl.semaphore_wait(info.at[0], 1)

    @pl.when(jnp.logical_and(patch < patch_count - 2, below))
    def _():
        tell(info.at[0], patch - 1, seq, req)

    @pl.when(patch > 1)
    def _():
        pl.semaphore_wait(info.at[1], 1)

    @pl.when(jnp.logical_and(patch > 1, above))
    def _():
        tell(info.at[1], patch + 1, seq, req)

    for hop in late:
        place_copy(hop).start()
        for l in range(layers):
            main_copy(l, hop).start()
        for i in range(2):
            own_copy(i, hop).start()
    for wave in far:
        for hop in wave:
            place_copy(hop).start()
    for l in range(layers):
        for wave in far[:-1]:
            for hop in wave:
                main_copy(l, hop).start()

    @pl.when(jnp.logical_not(inner))
    def _():
        for l in range(ahead):
            for hop in far[-1]:
                main_copy(l, hop).start()

    for l in range(ahead, layers):
        for hop in far[-1]:
            main_copy(l, hop).start()
    for wave in far:
        for i in range(2):
            for hop in wave:
                own_copy(i, hop).start()
    text_copy.start()
    for l in range(layers):
        main_in[l, me] = main_out[l, me]
    for i in range(2):
        own_in[i][me] = own_out[i, me]

    small[2].wait()
    lines = query[...].astype(f32)
    for l in range(layers):
        for g in range(KV_HEADS):
            heads[l, g * PAD:(g + 1) * PAD, :] = jnp.concatenate(
                [
                    lines[l:l + 1, (g * group + h) * HEAD_DIM:(g * group + h + 1) * HEAD_DIM]
                    for h in range(group)
                ] + [jnp.zeros((PAD - group, HEAD_DIM), f32)],
                axis=0,
            )

    def head_block(l, d):
        g = lax.rem(seq + d, seq_count)
        return heads[l, pl.ds(pl.multiple_of(g * PAD, PAD), PAD), :]

    small[3].wait()
    positions = seq * text_dev + lax.broadcasted_iota(
        jnp.int32, (KV_HEADS * PAD, text_dev), 1
    )
    used = positions < length[0]
    lane_group = lax.broadcasted_iota(jnp.int32, (PAD, kvw), 1) // HEAD_DIM
    for l in range(layers):
        spread = jnp.concatenate(
            [
                jnp.where(
                    lane_group == lax.rem(seq + d, seq_count),
                    jnp.concatenate([head_block(l, d)] * KV_HEADS, axis=1),
                    0.0,
                )
                for d in range(seq_count)
            ],
            axis=0,
        ).astype(bf16)
        if l == 0:
            text_copy.wait()
        raw = lax.dot_general(
            spread, text[l, :, :kvw], NT, preferred_element_type=f32
        ) * scale
        scores[l] = jnp.where(used, raw, -jnp.inf)

    settle(place_in.at[others], place_sem.at[1])
    wanted = (row_i == me * per + lax.rem(col_i, per)).astype(f32).astype(bf16)
    lanes = jnp.dot(
        place_in[...].reshape(groups, src_rows).astype(f32).astype(bf16), wanted,
        preferred_element_type=f32,
    )
    source = lax.broadcasted_iota(jnp.int32, (groups, src_rows), 1) // per
    place = jnp.sum(jnp.where(source == owner, lanes, 0.0), axis=0, keepdims=True)
    put = (row_i == place.astype(jnp.int32)).astype(f32).astype(bf16)
    put_out[...] = put

    @pl.when(patch == 0)
    def _():
        for d in range(1, seq_count):
            tell(info.at[2], patch, lax.rem(seq + d, seq_count), req)
        pl.semaphore_wait(info.at[2], seq_count - 1)
        for p in range(1, patch_count):
            tell(info.at[3], p, seq, req)

    @pl.when(below)
    def _():
        pl.semaphore_wait(info.at[3], 1)

    zeros = jnp.zeros((PAD, HEAD_DIM), f32)
    for l in range(layers):
        spread = jnp.concatenate(
            [
                jnp.concatenate(
                    [head_block(l, d) if c == d else zeros for c in range(1, seq_count)],
                    axis=1,
                )
                for d in range(1, seq_count)
            ],
            axis=0,
        ).astype(bf16)
        settle(main_in.at[l, others], main_recv.at[l])
        block = main_in[l].reshape(src_rows, main_width)
        image_scores = lax.dot_general(
            spread, block[:, :side], NT, preferred_element_type=f32
        ) * scale
        text_scores = scores[l, PAD:, :]
        top = jnp.maximum(
            jnp.max(text_scores, axis=1, keepdims=True),
            jnp.max(image_scores, axis=1, keepdims=True),
        )
        text_w = jnp.exp(text_scores - top)
        image_w = jnp.exp(image_scores - top)
        total = jnp.sum(text_w, axis=1, keepdims=True) + jnp.sum(
            image_w, axis=1, keepdims=True
        )
        image_sums = jnp.dot(
            image_w.astype(bf16), block[:, side:], preferred_element_type=f32
        )
        for d in range(1, seq_count):
            at = slice((d - 1) * PAD, d * PAD)
            text_sums = jnp.dot(
                text_w[at].astype(bf16), text[l, :, lanes_of(d, kvw)],
                preferred_element_type=f32,
            )
            part_out[l, d, :, :HEAD_DIM] = (
                text_sums + image_sums[at, (d - 1) * HEAD_DIM:d * HEAD_DIM]
            )
            part_out[l, d, :, HEAD_DIM:2 * HEAD_DIM] = jnp.broadcast_to(
                top[at], (PAD, HEAD_DIM)
            )
            part_out[l, d, :, 2 * HEAD_DIM:] = jnp.broadcast_to(total[at], (PAD, HEAD_DIM))
            part_copy(l, d).start()
        moved = jnp.dot(put, block, preferred_element_type=f32).astype(bf16)
        for d in range(1, seq_count):
            cache[l, 0, :, lanes_of(d)] = moved[:, (d - 1) * HEAD_DIM:d * HEAD_DIM]
            cache[l, 0, :, lanes_of(d, kvw)] = moved[
                :, side + (d - 1) * HEAD_DIM:side + d * HEAD_DIM
            ]

    settle(keys_in.at[others], own_recv.at[0])
    own_keys = [keys_in[:, l].reshape(src_rows, HEAD_DIM) for l in range(layers)]
    mine_now = []
    for l in range(layers):
        image_scores = lax.dot_general(
            head_block(l, 0).astype(bf16), own_keys[l], NT, preferred_element_type=f32
        ) * scale
        text_scores = scores[l, :PAD, :]
        top = jnp.maximum(
            jnp.max(text_scores, axis=1, keepdims=True),
            jnp.max(image_scores, axis=1, keepdims=True),
        )
        text_w = jnp.exp(text_scores - top)
        image_w = jnp.exp(image_scores - top)
        total = jnp.sum(text_w, axis=1, keepdims=True) + jnp.sum(
            image_w, axis=1, keepdims=True
        )
        value = jnp.dot(
            text_w.astype(bf16), text[l, :, lanes_of(0, kvw)], preferred_element_type=f32
        )
        weights_out[l * PAD:(l + 1) * PAD, :] = image_w
        mine_now.append(
            (value, jnp.broadcast_to(top, (PAD, HEAD_DIM)), jnp.broadcast_to(total, (PAD, HEAD_DIM)))
        )
    moved = jnp.dot(
        put, jnp.concatenate(own_keys, axis=1), preferred_element_type=f32
    ).astype(bf16)
    for l in range(layers):
        cache[l, 0, :, lanes_of(0)] = moved[:, l * HEAD_DIM:(l + 1) * HEAD_DIM]

    beside = pl.ds(1, seq_count - 1)
    settle(part_in.at[:, beside], part_sem.at[1])
    for l in range(layers):
        cells = [mine_now[l]] + [
            tuple(part_in[l, d, :, i * HEAD_DIM:(i + 1) * HEAD_DIM] for i in range(3))
            for d in range(1, seq_count)
        ]
        top = functools.reduce(jnp.maximum, [c[1] for c in cells])
        factors = [jnp.exp(c[1] - top) for c in cells]
        partial_out[l, :, :HEAD_DIM] = factors[0]
        partial_out[l, :, HEAD_DIM:2 * HEAD_DIM] = sum(
            f * c[0] for f, c in zip(factors, cells)
        )
        partial_out[l, :, 2 * HEAD_DIM:] = sum(f * c[2] for f, c in zip(factors, cells))

    settle(main_out.at[:, others], main_send.at[0])
    settle(place_in.at[others], place_sem.at[0])
    settle(part_out.at[:, beside], part_sem.at[0])
    settle(own_out.at[:, others], own_send.at[0])
    settle(values_in.at[others], own_recv.at[1])


def finish(
    dims, cache, put, values, weights, partial, att_out, cache_out, att, last, sem
):
    _, seq_count, _ = dims
    layers, _, src_rows, full = cache.shape
    kvw = full // 2
    group = HEADS // KV_HEADS
    seq = lax.axis_index("seq")
    f32, bf16 = jnp.float32, jnp.bfloat16

    def lanes_of(d):
        g = lax.rem(seq + d, seq_count)
        return pl.ds(pl.multiple_of(kvw + g * HEAD_DIM, HEAD_DIM), HEAD_DIM)

    for l in range(layers):
        pltpu.make_async_copy(
            cache.at[l, 0, :, pl.ds(0, kvw)], cache_out.at[l, 0, :, pl.ds(0, kvw)], sem.at[0]
        ).start()
        for d in range(1, seq_count):
            pltpu.make_async_copy(
                cache.at[l, 0, :, lanes_of(d)], cache_out.at[l, 0, :, lanes_of(d)], sem.at[0]
            ).start()
    own = [values[:, l].reshape(src_rows, HEAD_DIM) for l in range(layers)]
    both = jnp.concatenate([put[...], weights[...].astype(bf16)], axis=0)
    moved = jnp.dot(both, jnp.concatenate(own, axis=1), preferred_element_type=f32)
    for l in range(layers):
        at = slice(l * HEAD_DIM, (l + 1) * HEAD_DIM)
        last[l] = moved[:src_rows, at].astype(bf16)
        pltpu.make_async_copy(
            last.at[l], cache_out.at[l, 0, :, lanes_of(0)], sem.at[0]
        ).start()
    lines = []
    for l in range(layers):
        value = moved[
            src_rows + l * PAD:src_rows + (l + 1) * PAD, l * HEAD_DIM:(l + 1) * HEAD_DIM
        ]
        factor = partial[l, :, :HEAD_DIM]
        summed = partial[l, :, HEAD_DIM:2 * HEAD_DIM]
        result = (summed + factor * value) / partial[l, :, 2 * HEAD_DIM:]
        lines.append(jnp.concatenate([result[h:h + 1] for h in range(group)], axis=1))
    att[...] = jnp.concatenate(lines, axis=0).astype(bf16)
    att_copy = pltpu.make_async_copy(att, att_out, sem.at[1])
    att_copy.start()
    pltpu.make_async_copy(cache, cache_out, sem.at[0]).wait()
    att_copy.wait()


def body(dims, query, text_cache, text_len, image_rows, patch_map, image_places):
    patch_count, seq_count, req_count = dims
    layers, req_dev, query_width = query.shape
    text_dev, full = text_cache.shape[2:]
    src_rows = image_rows.shape[1]
    groups = patch_count * req_count
    assert req_dev == 1 and seq_count == KV_HEADS and full == 2 * KV_HEADS * HEAD_DIM
    assert patch_count % 2 == 0
    per = src_rows // groups
    main_width = full - 2 * HEAD_DIM
    rows_padded = KV_HEADS * PAD
    bf16, f32, i32 = jnp.bfloat16, jnp.float32, jnp.int32
    dma = pltpu.SemaphoreType.DMA
    vmem = pl.BlockSpec(memory_space=pltpu.VMEM)
    hbm = pl.BlockSpec(memory_space=pltpu.HBM)
    att_shape = jax.ShapeDtypeStruct((layers, query_width // seq_count), bf16)
    cache_shape = jax.ShapeDtypeStruct((layers, 1, src_rows, full), bf16)
    in_hbm = lambda x: pltpu.with_memory_space_constraint(x, pltpu.HBM)
    in_vmem = lambda x: pltpu.with_memory_space_constraint(x, pltpu.VMEM)
    state = pl.pallas_call(
        functools.partial(exchange, dims),
        out_shape=(
            pltpu.VMEM(cache_shape.shape, bf16),
            pltpu.VMEM((src_rows, src_rows), bf16),
            pltpu.VMEM((groups, layers, per, HEAD_DIM), bf16),
            pltpu.VMEM((layers * PAD, src_rows), f32),
            pltpu.VMEM((layers, PAD, 3 * HEAD_DIM), f32),
        ),
        in_specs=[hbm, pl.BlockSpec(memory_space=pl.ANY), hbm, hbm, hbm, hbm],
        out_specs=(vmem,) * 5,
        scratch_shapes=[
            pltpu.VMEM((layers, query_width), bf16),
            pltpu.SMEM((1,), i32),
            pltpu.VMEM((1, src_rows), i32),
            pltpu.VMEM((1, src_rows), i32),
            pltpu.VMEM((layers, src_rows, full), bf16),
            pltpu.VMEM((layers, text_dev, full), bf16),
            pltpu.VMEM((layers, groups, per, main_width), bf16),
            pltpu.VMEM((layers, groups, per, main_width), bf16),
            pltpu.VMEM((2, groups, layers, per, HEAD_DIM), bf16),
            pltpu.VMEM((groups, layers, per, HEAD_DIM), bf16),
            pltpu.VMEM((1, src_rows), i32),
            pltpu.VMEM((groups, 1, src_rows), i32),
            pltpu.VMEM((layers, rows_padded, HEAD_DIM), f32),
            pltpu.VMEM((layers, rows_padded, text_dev), f32),
            pltpu.VMEM((layers, seq_count, PAD, 3 * HEAD_DIM), f32),
            pltpu.VMEM((layers, seq_count, PAD, 3 * HEAD_DIM), f32),
            dma((4,)), dma((2,)), dma((1,)), dma((1,)), dma((layers,)), dma((1,)), dma((2,)),
            dma((2,)), dma((2,)), pltpu.SemaphoreType.REGULAR((4,)),
        ],
        compiler_params=pltpu.CompilerParams(
            collective_id=0, has_side_effects=True, vmem_limit_bytes=32 * 1024 * 1024
        ),
    )(
        in_hbm(query.reshape(layers, query_width)), text_len,
        in_hbm(patch_map.reshape(1, src_rows)), in_hbm(image_places.reshape(1, src_rows)),
        in_hbm(image_rows), in_hbm(text_cache),
    )
    attended, cache = pl.pallas_call(
        functools.partial(finish, dims),
        out_shape=(att_shape, cache_shape),
        in_specs=[vmem] * 5,
        out_specs=(hbm, hbm),
        scratch_shapes=[
            pltpu.VMEM(att_shape.shape, bf16),
            pltpu.VMEM((layers, src_rows, HEAD_DIM), bf16),
            dma((2,)),
        ],
    )(*(in_vmem(x) for x in state))
    return attended.reshape(layers, 1, query_width // seq_count), cache


def solution(mesh):
    dims = tuple(mesh.shape[a] for a in ("patch", "seq", "req"))
    return jax.shard_map(
        functools.partial(body, dims),
        mesh=mesh,
        in_specs=(
            P(None, ("patch", "req"), None),
            P(None, ("patch", "req"), "seq", None),
            P(("patch", "req")),
            P(None, ("patch", "seq", "req"), None),
            P(("patch", "seq", "req")),
            P(("patch", "seq", "req")),
        ),
        out_specs=(P(None, ("patch", "req"), "seq"), P(None, ("patch", "req"), "seq", None)),
        check_vma=False,
    )
```

```python
import functools
import math

import jax
import jax.numpy as jnp
from jax import lax
from jax.experimental import pallas as pl
from jax.experimental.pallas import tpu as pltpu
from jax.sharding import PartitionSpec as P

HEADS = 28
KV_HEADS = 4
HEAD_DIM = 128
PAD = 8
MESH = pl.DeviceIdType.MESH
NT = (((1,), (1,)), ((), ()))


def all_hops(patch_count, req_count):
    half = patch_count // 2
    cores = range(req_count)
    mates = [("mate", 0, c) for c in cores if c]
    near = [("near", i, c) for i in range(1, half) for c in cores]
    far = [[("far", k, c) for c in cores] for k in range(half)]
    return mates, near, far


def exchange(
    dims,
    query_hbm, len_hbm, map_hbm, place_hbm, rows_hbm, text_hbm,
    cache, put_out, values_in, weights_out, partial_out,
    query, length, maps, places, rows, text, main_out, main_in, own_out, keys_in, place_out, place_in,
    heads, scores, part_out, part_in,
    small_sem, rows_sem, text_sem, main_send, main_recv, own_send, own_recv, place_sem, part_sem,
    info,
):
    patch_count, seq_count, req_count = dims
    layers, src_rows, full = rows.shape
    text_dev = text.shape[1]
    kvw = full // 2
    group = HEADS // KV_HEADS
    groups = patch_count * req_count
    per = src_rows // groups
    half = patch_count // 2
    side = (seq_count - 1) * HEAD_DIM
    main_width = 2 * side
    scale = 1.0 / math.sqrt(HEAD_DIM)
    patch, seq, req = (lax.axis_index(a) for a in ("patch", "seq", "req"))
    me = patch * req_count + req
    mates, near, far = all_hops(patch_count, req_count)
    beside = near if half == 2 else []
    late = [hop for hop in near if hop not in beside]
    ahead = min(2, layers)
    f32, bf16 = jnp.float32, jnp.bfloat16
    upper = patch // half
    inner = jnp.logical_or(patch == half - 1, patch == half)

    def partner(hop):
        kind, i, c = hop
        r = req_count - 1 - c
        if kind == "mate":
            return patch, lax.rem(req + c, req_count)
        if kind == "near":
            return upper * half + lax.rem(lax.rem(patch, half) + i, half), r
        return (1 - upper) * (patch_count - 1 - i) + upper * i, r

    others = pl.ds(0, groups - 1)
    own_in = (keys_in, values_in)
    halves = (pl.ds(0, kvw), pl.ds(kvw, kvw))
    first_rows = [
        pltpu.make_async_copy(rows_hbm.at[0, :, at], rows.at[0, :, at], rows_sem.at[1 + i])
        for i, at in enumerate(halves)
    ]
    later = pl.ds(1, layers - 1)
    later_rows = pltpu.make_async_copy(rows_hbm.at[later], rows.at[later], rows_sem.at[0])
    text_copy = pltpu.make_async_copy(text_hbm.at[:, 0], text, text_sem.at[0])

    def settle(ref, sem):
        pltpu.make_async_copy(ref, ref, sem).wait()

    small = [
        pltpu.make_async_copy(map_hbm, maps, small_sem.at[0]),
        pltpu.make_async_copy(place_hbm, places, small_sem.at[1]),
        pltpu.make_async_copy(query_hbm, query, small_sem.at[2]),
        pltpu.make_async_copy(len_hbm, length, small_sem.at[3]),
    ]
    small[0].start()
    for copy in first_rows:
        copy.start()
    barrier = pltpu.get_barrier_semaphore()

    def tell(sem, p, s, r):
        pl.semaphore_signal(sem, inc=1, device_id=(p, s, r), device_id_type=MESH)

    above, below = patch < patch_count - 1, patch > 0

    @pl.when(above)
    def _():
        for c in range(req_count):
            tell(barrier, patch + 1, seq, lax.rem(req + c, req_count))

    @pl.when(jnp.logical_and(below, patch <= half))
    def _():
        for c in range(req_count):
            tell(barrier, patch - 1, seq, lax.rem(req + c, req_count))

    for c in range(1, req_count):
        tell(barrier, patch, seq, lax.rem(req + c, req_count))

    @pl.when(patch == 0)
    def _():
        for d in range(1, seq_count):
            tell(barrier, patch, lax.rem(seq + d, seq_count), req)

    has_below = 1 - (patch_count - 1 - patch) // (patch_count - 1)
    arrivals = (
        req_count - 1 + req_count * (has_below + 1 - upper) + (seq_count - 1) * (1 - has_below)
    )
    answers = jnp.logical_and(patch == patch_count - 1, patch > half)

    for copy in small[1:]:
        copy.start()

    @pl.when(answers)
    def _():
        pl.semaphore_wait(barrier, arrivals)
        tell(info.at[0], patch - 1, seq, req)


    def lanes_of(d, base=0):
        g = lax.rem(seq + d, seq_count)
        return pl.ds(pl.multiple_of(base + g * HEAD_DIM, HEAD_DIM), HEAD_DIM)

    owner = lax.broadcasted_iota(jnp.int32, (groups, src_rows), 0)
    row_i = lax.broadcasted_iota(jnp.int32, (src_rows, src_rows), 0)
    col_i = lax.broadcasted_iota(jnp.int32, (src_rows, src_rows), 1)
    before = (row_i < col_i).astype(f32).astype(bf16)
    small[0].wait()
    mine = maps[...] == owner
    rank = jnp.dot(mine.astype(f32).astype(bf16), before, preferred_element_type=f32)
    slot = jnp.sum(
        jnp.where(mine, rank + (owner * per).astype(f32), 0.0), axis=0, keepdims=True
    )
    pick = (row_i == slot.astype(jnp.int32)).astype(f32).astype(bf16)

    def place_copy(hop):
        p, r = partner(hop)
        return pltpu.make_async_remote_copy(
            src_ref=place_out, dst_ref=place_in.at[me],
            send_sem=place_sem.at[0], recv_sem=place_sem.at[1],
            device_id=(p, seq, r), device_id_type=MESH,
        )

    def main_copy(l, hop, at=pl.ds(0, main_width)):
        p, r = partner(hop)
        return pltpu.make_async_remote_copy(
            src_ref=main_out.at[l, p * req_count + r, :, at], dst_ref=main_in.at[l, me, :, at],
            send_sem=main_send.at[0], recv_sem=main_recv.at[l],
            device_id=(p, seq, r), device_id_type=MESH,
        )

    def own_copy(i, hop):
        p, r = partner(hop)
        return pltpu.make_async_remote_copy(
            src_ref=own_out.at[i, p * req_count + r], dst_ref=own_in[i].at[me],
            send_sem=own_send.at[0], recv_sem=own_recv.at[i],
            device_id=(p, seq, r), device_id_type=MESH,
        )

    def part_copy(l, d):
        s = lax.rem(seq + d, seq_count)
        return pltpu.make_async_remote_copy(
            src_ref=part_out.at[l, d], dst_ref=part_in.at[l, d],
            send_sem=part_sem.at[0], recv_sem=part_sem.at[1],
            device_id=(patch, s, req), device_id_type=MESH,
        )

    def sort(l, base):
        turned = jnp.concatenate(
            [rows[l, :, lanes_of(d, base)] for d in range(1, seq_count)], axis=1
        )
        moved = jnp.dot(pick, turned, preferred_element_type=f32).astype(bf16)
        at = slice(0, side) if base == 0 else slice(side, main_width)
        main_out[l, :, :, at] = moved.reshape(groups, per, side)

    def send_first(l, at):
        for hop in mates:
            main_copy(l, hop, at).start()

        @pl.when(patch != half)
        def _():
            for hop in beside:
                main_copy(l, hop, at).start()

        if l < ahead:

            @pl.when(inner)
            def _():
                for hop in far[-1]:
                    main_copy(l, hop, at).start()

    for l in range(layers):
        if l == 0:
            first_rows[0].wait()
            sort(l, 0)

            @pl.when(jnp.logical_not(answers))
            def _():
                pl.semaphore_wait(barrier, arrivals)

            send_first(l, pl.ds(0, side))
            first_rows[1].wait()
            later_rows.start()
            sort(l, kvw)
            send_first(l, pl.ds(side, side))

            @pl.when(jnp.logical_and(patch == 1, above))
            def _():
                tell(info.at[1], patch + 1, seq, req)

        else:
            if l == 1:
                later_rows.wait()
            sort(l, 0)
            sort(l, kvw)
            send_first(l, pl.ds(0, main_width))
        if l == 0:
            small[1].wait()
            local = (places[...] - seq * src_rows).astype(f32).astype(bf16)
            place_sorted = lax.dot_general(
                jnp.broadcast_to(local, (PAD, src_rows)), pick, NT,
                preferred_element_type=f32,
            )
            place_out[...] = place_sorted[0:1].astype(jnp.int32)
            place_in[me] = place_sorted[0:1].astype(jnp.int32)
            for hop in mates:
                place_copy(hop).start()
    for l in range(layers):
        turned = jnp.concatenate([rows[l, :, lanes_of(0)], rows[l, :, lanes_of(0, kvw)]], axis=1)
        moved = jnp.dot(pick, turned, preferred_element_type=f32).astype(bf16)
        own_out[0, :, l] = moved[:, :HEAD_DIM].reshape(groups, per, HEAD_DIM)
        own_out[1, :, l] = moved[:, HEAD_DIM:].reshape(groups, per, HEAD_DIM)
    def own_near():
        for i in range(2):
            for hop in beside:
                own_copy(i, hop).start()

    for i in range(2):
        for hop in mates:
            own_copy(i, hop).start()
    pl.when(patch != half)(own_near)
    listens = jnp.logical_or(
        patch < patch_count - 2, jnp.logical_and(patch >= half, above)
    )

    @pl.when(listens)
    def _():
        pl.semaphore_wait(info.at[0], 1)

    @pl.when(jnp.logical_and(listens, below))
    def _():
        tell(info.at[0], patch - 1, seq, req)

    @pl.when(patch > 1)
    def _():
        pl.semaphore_wait(info.at[1], 1)

    @pl.when(jnp.logical_and(patch > 1, above))
    def _():
        tell(info.at[1], patch + 1, seq, req)

    @pl.when(patch == half)
    def _():
        for l in range(layers):
            for hop in beside:
                main_copy(l, hop).start()
        own_near()

    for hop in beside:
        place_copy(hop).start()
    for hop in late:
        place_copy(hop).start()
        for l in range(layers):
            main_copy(l, hop).start()
        for i in range(2):
            own_copy(i, hop).start()
    for wave in far:
        for hop in wave:
            place_copy(hop).start()
    for l in range(layers):
        for wave in far[:-1]:
            for hop in wave:
                main_copy(l, hop).start()

    @pl.when(jnp.logical_not(inner))
    def _():
        for l in range(ahead):
            for hop in far[-1]:
                main_copy(l, hop).start()

    for l in range(ahead, layers):
        for hop in far[-1]:
            main_copy(l, hop).start()
    for wave in far:
        for i in range(2):
            for hop in wave:
                own_copy(i, hop).start()
    text_copy.start()
    for l in range(layers):
        main_in[l, me] = main_out[l, me]
    for i in range(2):
        own_in[i][me] = own_out[i, me]

    small[2].wait()
    lines = query[...].astype(f32)
    for l in range(layers):
        for g in range(KV_HEADS):
            heads[l, g * PAD:(g + 1) * PAD, :] = jnp.concatenate(
                [
                    lines[l:l + 1, (g * group + h) * HEAD_DIM:(g * group + h + 1) * HEAD_DIM]
                    for h in range(group)
                ] + [jnp.zeros((PAD - group, HEAD_DIM), f32)],
                axis=0,
            )

    def head_block(l, d):
        g = lax.rem(seq + d, seq_count)
        return heads[l, pl.ds(pl.multiple_of(g * PAD, PAD), PAD), :]

    small[3].wait()
    positions = seq * text_dev + lax.broadcasted_iota(
        jnp.int32, (KV_HEADS * PAD, text_dev), 1
    )
    used = positions < length[0]
    lane_group = lax.broadcasted_iota(jnp.int32, (PAD, kvw), 1) // HEAD_DIM
    for l in range(layers):
        spread = jnp.concatenate(
            [
                jnp.where(
                    lane_group == lax.rem(seq + d, seq_count),
                    jnp.concatenate([head_block(l, d)] * KV_HEADS, axis=1),
                    0.0,
                )
                for d in range(seq_count)
            ],
            axis=0,
        ).astype(bf16)
        if l == 0:
            text_copy.wait()
        raw = lax.dot_general(
            spread, text[l, :, :kvw], NT, preferred_element_type=f32
        ) * scale
        scores[l] = jnp.where(used, raw, -jnp.inf)

    settle(place_in.at[others], place_sem.at[1])
    wanted = (row_i == me * per + lax.rem(col_i, per)).astype(f32).astype(bf16)
    lanes = jnp.dot(
        place_in[...].reshape(groups, src_rows).astype(f32).astype(bf16), wanted,
        preferred_element_type=f32,
    )
    source = lax.broadcasted_iota(jnp.int32, (groups, src_rows), 1) // per
    place = jnp.sum(jnp.where(source == owner, lanes, 0.0), axis=0, keepdims=True)
    put = (row_i == place.astype(jnp.int32)).astype(f32).astype(bf16)
    put_out[...] = put

    @pl.when(patch == 0)
    def _():
        for d in range(1, seq_count):
            tell(info.at[2], patch, lax.rem(seq + d, seq_count), req)
        pl.semaphore_wait(info.at[2], seq_count - 1)
        for p in range(1, patch_count):
            tell(info.at[3], p, seq, req)

    @pl.when(below)
    def _():
        pl.semaphore_wait(info.at[3], 1)

    zeros = jnp.zeros((PAD, HEAD_DIM), f32)
    for l in range(layers):
        spread = jnp.concatenate(
            [
                jnp.concatenate(
                    [head_block(l, d) if c == d else zeros for c in range(1, seq_count)],
                    axis=1,
                )
                for d in range(1, seq_count)
            ],
            axis=0,
        ).astype(bf16)
        settle(main_in.at[l, others], main_recv.at[l])
        block = main_in[l].reshape(src_rows, main_width)
        image_scores = lax.dot_general(
            spread, block[:, :side], NT, preferred_element_type=f32
        ) * scale
        text_scores = scores[l, PAD:, :]
        top = jnp.maximum(
            jnp.max(text_scores, axis=1, keepdims=True),
            jnp.max(image_scores, axis=1, keepdims=True),
        )
        text_w = jnp.exp(text_scores - top)
        image_w = jnp.exp(image_scores - top)
        total = jnp.sum(text_w, axis=1, keepdims=True) + jnp.sum(
            image_w, axis=1, keepdims=True
        )
        image_sums = jnp.dot(
            image_w.astype(bf16), block[:, side:], preferred_element_type=f32
        )
        for d in range(1, seq_count):
            at = slice((d - 1) * PAD, d * PAD)
            text_sums = jnp.dot(
                text_w[at].astype(bf16), text[l, :, lanes_of(d, kvw)],
                preferred_element_type=f32,
            )
            part_out[l, d, :, :HEAD_DIM] = (
                text_sums + image_sums[at, (d - 1) * HEAD_DIM:d * HEAD_DIM]
            )
            part_out[l, d, :, HEAD_DIM:2 * HEAD_DIM] = jnp.broadcast_to(
                top[at], (PAD, HEAD_DIM)
            )
            part_out[l, d, :, 2 * HEAD_DIM:] = jnp.broadcast_to(total[at], (PAD, HEAD_DIM))
            part_copy(l, d).start()
        moved = jnp.dot(put, block, preferred_element_type=f32).astype(bf16)
        for d in range(1, seq_count):
            cache[l, 0, :, lanes_of(d)] = moved[:, (d - 1) * HEAD_DIM:d * HEAD_DIM]
            cache[l, 0, :, lanes_of(d, kvw)] = moved[
                :, side + (d - 1) * HEAD_DIM:side + d * HEAD_DIM
            ]

    settle(keys_in.at[others], own_recv.at[0])
    own_keys = [keys_in[:, l].reshape(src_rows, HEAD_DIM) for l in range(layers)]
    mine_now = []
    for l in range(layers):
        image_scores = lax.dot_general(
            head_block(l, 0).astype(bf16), own_keys[l], NT, preferred_element_type=f32
        ) * scale
        text_scores = scores[l, :PAD, :]
        top = jnp.maximum(
            jnp.max(text_scores, axis=1, keepdims=True),
            jnp.max(image_scores, axis=1, keepdims=True),
        )
        text_w = jnp.exp(text_scores - top)
        image_w = jnp.exp(image_scores - top)
        total = jnp.sum(text_w, axis=1, keepdims=True) + jnp.sum(
            image_w, axis=1, keepdims=True
        )
        value = jnp.dot(
            text_w.astype(bf16), text[l, :, lanes_of(0, kvw)], preferred_element_type=f32
        )
        weights_out[l * PAD:(l + 1) * PAD, :] = image_w
        mine_now.append(
            (value, jnp.broadcast_to(top, (PAD, HEAD_DIM)), jnp.broadcast_to(total, (PAD, HEAD_DIM)))
        )
    moved = jnp.dot(
        put, jnp.concatenate(own_keys, axis=1), preferred_element_type=f32
    ).astype(bf16)
    for l in range(layers):
        cache[l, 0, :, lanes_of(0)] = moved[:, l * HEAD_DIM:(l + 1) * HEAD_DIM]

    bands = pl.ds(1, seq_count - 1)
    settle(part_in.at[:, bands], part_sem.at[1])
    for l in range(layers):
        cells = [mine_now[l]] + [
            tuple(part_in[l, d, :, i * HEAD_DIM:(i + 1) * HEAD_DIM] for i in range(3))
            for d in range(1, seq_count)
        ]
        top = functools.reduce(jnp.maximum, [c[1] for c in cells])
        factors = [jnp.exp(c[1] - top) for c in cells]
        partial_out[l, :, :HEAD_DIM] = factors[0]
        partial_out[l, :, HEAD_DIM:2 * HEAD_DIM] = sum(
            f * c[0] for f, c in zip(factors, cells)
        )
        partial_out[l, :, 2 * HEAD_DIM:] = sum(f * c[2] for f, c in zip(factors, cells))

    settle(main_out.at[:, others], main_send.at[0])
    settle(place_in.at[others], place_sem.at[0])
    settle(part_out.at[:, bands], part_sem.at[0])
    settle(own_out.at[:, others], own_send.at[0])
    settle(values_in.at[others], own_recv.at[1])


def finish(
    dims, cache, put, values, weights, partial, att_out, cache_out, att, last, sem
):
    _, seq_count, _ = dims
    layers, _, src_rows, full = cache.shape
    kvw = full // 2
    group = HEADS // KV_HEADS
    seq = lax.axis_index("seq")
    f32, bf16 = jnp.float32, jnp.bfloat16

    def lanes_of(d):
        g = lax.rem(seq + d, seq_count)
        return pl.ds(pl.multiple_of(kvw + g * HEAD_DIM, HEAD_DIM), HEAD_DIM)

    for l in range(layers):
        pltpu.make_async_copy(
            cache.at[l, 0, :, pl.ds(0, kvw)], cache_out.at[l, 0, :, pl.ds(0, kvw)], sem.at[0]
        ).start()
        for d in range(1, seq_count):
            pltpu.make_async_copy(
                cache.at[l, 0, :, lanes_of(d)], cache_out.at[l, 0, :, lanes_of(d)], sem.at[0]
            ).start()
    own = [values[:, l].reshape(src_rows, HEAD_DIM) for l in range(layers)]
    both = jnp.concatenate([put[...], weights[...].astype(bf16)], axis=0)
    moved = jnp.dot(both, jnp.concatenate(own, axis=1), preferred_element_type=f32)
    for l in range(layers):
        at = slice(l * HEAD_DIM, (l + 1) * HEAD_DIM)
        last[l] = moved[:src_rows, at].astype(bf16)
        pltpu.make_async_copy(
            last.at[l], cache_out.at[l, 0, :, lanes_of(0)], sem.at[0]
        ).start()
    lines = []
    for l in range(layers):
        value = moved[
            src_rows + l * PAD:src_rows + (l + 1) * PAD, l * HEAD_DIM:(l + 1) * HEAD_DIM
        ]
        factor = partial[l, :, :HEAD_DIM]
        summed = partial[l, :, HEAD_DIM:2 * HEAD_DIM]
        result = (summed + factor * value) / partial[l, :, 2 * HEAD_DIM:]
        lines.append(jnp.concatenate([result[h:h + 1] for h in range(group)], axis=1))
    att[...] = jnp.concatenate(lines, axis=0).astype(bf16)
    att_copy = pltpu.make_async_copy(att, att_out, sem.at[1])
    att_copy.start()
    pltpu.make_async_copy(cache, cache_out, sem.at[0]).wait()
    att_copy.wait()


def body(dims, query, text_cache, text_len, image_rows, patch_map, image_places):
    patch_count, seq_count, req_count = dims
    layers, req_dev, query_width = query.shape
    text_dev, full = text_cache.shape[2:]
    src_rows = image_rows.shape[1]
    groups = patch_count * req_count
    assert req_dev == 1 and seq_count == KV_HEADS and full == 2 * KV_HEADS * HEAD_DIM
    assert patch_count % 2 == 0
    per = src_rows // groups
    main_width = full - 2 * HEAD_DIM
    rows_padded = KV_HEADS * PAD
    bf16, f32, i32 = jnp.bfloat16, jnp.float32, jnp.int32
    dma = pltpu.SemaphoreType.DMA
    vmem = pl.BlockSpec(memory_space=pltpu.VMEM)
    hbm = pl.BlockSpec(memory_space=pltpu.HBM)
    att_shape = jax.ShapeDtypeStruct((layers, query_width // seq_count), bf16)
    cache_shape = jax.ShapeDtypeStruct((layers, 1, src_rows, full), bf16)
    in_hbm = lambda x: pltpu.with_memory_space_constraint(x, pltpu.HBM)
    in_vmem = lambda x: pltpu.with_memory_space_constraint(x, pltpu.VMEM)
    state = pl.pallas_call(
        functools.partial(exchange, dims),
        out_shape=(
            pltpu.VMEM(cache_shape.shape, bf16),
            pltpu.VMEM((src_rows, src_rows), bf16),
            pltpu.VMEM((groups, layers, per, HEAD_DIM), bf16),
            pltpu.VMEM((layers * PAD, src_rows), f32),
            pltpu.VMEM((layers, PAD, 3 * HEAD_DIM), f32),
        ),
        in_specs=[hbm, pl.BlockSpec(memory_space=pl.ANY), hbm, hbm, hbm, hbm],
        out_specs=(vmem,) * 5,
        scratch_shapes=[
            pltpu.VMEM((layers, query_width), bf16),
            pltpu.SMEM((1,), i32),
            pltpu.VMEM((1, src_rows), i32),
            pltpu.VMEM((1, src_rows), i32),
            pltpu.VMEM((layers, src_rows, full), bf16),
            pltpu.VMEM((layers, text_dev, full), bf16),
            pltpu.VMEM((layers, groups, per, main_width), bf16),
            pltpu.VMEM((layers, groups, per, main_width), bf16),
            pltpu.VMEM((2, groups, layers, per, HEAD_DIM), bf16),
            pltpu.VMEM((groups, layers, per, HEAD_DIM), bf16),
            pltpu.VMEM((1, src_rows), i32),
            pltpu.VMEM((groups, 1, src_rows), i32),
            pltpu.VMEM((layers, rows_padded, HEAD_DIM), f32),
            pltpu.VMEM((layers, rows_padded, text_dev), f32),
            pltpu.VMEM((layers, seq_count, PAD, 3 * HEAD_DIM), f32),
            pltpu.VMEM((layers, seq_count, PAD, 3 * HEAD_DIM), f32),
            dma((4,)), dma((3,)), dma((1,)), dma((1,)), dma((layers,)), dma((1,)), dma((2,)),
            dma((2,)), dma((2,)), pltpu.SemaphoreType.REGULAR((4,)),
        ],
        compiler_params=pltpu.CompilerParams(
            collective_id=0, has_side_effects=True, vmem_limit_bytes=32 * 1024 * 1024
        ),
    )(
        in_hbm(query.reshape(layers, query_width)), text_len,
        in_hbm(patch_map.reshape(1, src_rows)), in_hbm(image_places.reshape(1, src_rows)),
        in_hbm(image_rows), in_hbm(text_cache),
    )
    attended, cache = pl.pallas_call(
        functools.partial(finish, dims),
        out_shape=(att_shape, cache_shape),
        in_specs=[vmem] * 5,
        out_specs=(hbm, hbm),
        scratch_shapes=[
            pltpu.VMEM(att_shape.shape, bf16),
            pltpu.VMEM((layers, src_rows, HEAD_DIM), bf16),
            dma((2,)),
        ],
    )(*(in_vmem(x) for x in state))
    return attended.reshape(layers, 1, query_width // seq_count), cache


def solution(mesh):
    dims = tuple(mesh.shape[a] for a in ("patch", "seq", "req"))
    return jax.shard_map(
        functools.partial(body, dims),
        mesh=mesh,
        in_specs=(
            P(None, ("patch", "req"), None),
            P(None, ("patch", "req"), "seq", None),
            P(("patch", "req")),
            P(None, ("patch", "seq", "req"), None),
            P(("patch", "seq", "req")),
            P(("patch", "seq", "req")),
        ),
        out_specs=(P(None, ("patch", "req"), "seq"), P(None, ("patch", "req"), "seq", None)),
        check_vma=False,
    )
```

```python
import functools
import math

import jax
import jax.numpy as jnp
from jax import lax
from jax.experimental import pallas as pl
from jax.experimental.pallas import tpu as pltpu
from jax.sharding import PartitionSpec as P

HEADS = 28
KV_HEADS = 4
HEAD_DIM = 128
PAD = 8
MESH = pl.DeviceIdType.MESH
NT = (((1,), (1,)), ((), ()))


def all_hops(patch_count, req_count):
    half = patch_count // 2
    cores = range(req_count)
    mates = [("mate", 0, c) for c in cores if c]
    near = [("near", i, c) for i in range(1, half) for c in cores]
    far = [[("far", k, c) for c in cores] for k in range(half)]
    return mates, near, far


def exchange(
    dims,
    query_hbm, len_hbm, map_hbm, place_hbm, rows_hbm, text_hbm,
    cache, put_out, values_in, weights_out, partial_out,
    query, length, maps, places, rows, text, main_out, main_in, own_out, keys_in, place_out, place_in,
    heads, scores, part_out, part_in,
    small_sem, load_sem, main_send, main_recv, own_send, own_recv, place_sem, part_sem,
    info,
):
    patch_count, seq_count, req_count = dims
    layers, src_rows, full = rows.shape
    text_dev = text.shape[1]
    kvw = full // 2
    group = HEADS // KV_HEADS
    groups = patch_count * req_count
    per = src_rows // groups
    half = patch_count // 2
    side = (seq_count - 1) * HEAD_DIM
    main_width = 2 * side
    scale = 1.0 / math.sqrt(HEAD_DIM)
    patch, seq, req = (lax.axis_index(a) for a in ("patch", "seq", "req"))
    me = patch * req_count + req
    mates, near, far = all_hops(patch_count, req_count)
    beside = near if half == 2 else []
    late = [hop for hop in near if hop not in beside]
    ahead = min(2, layers)
    f32, bf16 = jnp.float32, jnp.bfloat16
    upper = patch // half
    inner = jnp.logical_or(patch == half - 1, patch == half)

    def partner(hop):
        kind, i, c = hop
        if kind == "mate":
            return patch, lax.rem(req + c, req_count)
        r = req_count - 1 - c if kind == "near" or i == half - 1 else c
        if kind == "near":
            return upper * half + lax.rem(lax.rem(patch, half) + i, half), r
        return (1 - upper) * (patch_count - 1 - i) + upper * i, r

    others = pl.ds(0, groups - 1)
    own_in = (keys_in, values_in)
    halves = (pl.ds(0, kvw), pl.ds(kvw, kvw))
    first_rows = [
        pltpu.make_async_copy(rows_hbm.at[0, :, at], rows.at[0, :, at], load_sem.at[i])
        for i, at in enumerate(halves)
    ]
    second_rows = pltpu.make_async_copy(rows_hbm.at[1], rows.at[1], load_sem.at[2])
    rest = pl.ds(2, layers - 2)
    rest_rows = pltpu.make_async_copy(rows_hbm.at[rest], rows.at[rest], load_sem.at[3])
    text_copy = pltpu.make_async_copy(text_hbm.at[:, 0], text, load_sem.at[0])

    def settle(ref, sem):
        pltpu.make_async_copy(ref, ref, sem).wait()

    small = [
        pltpu.make_async_copy(map_hbm, maps, small_sem.at[0]),
        pltpu.make_async_copy(place_hbm, places, small_sem.at[0]),
        pltpu.make_async_copy(query_hbm, query, small_sem.at[0]),
        pltpu.make_async_copy(len_hbm, length, small_sem.at[0]),
    ]
    small[0].start()
    for copy in first_rows:
        copy.start()
    barrier = pltpu.get_barrier_semaphore()

    def tell(sem, p, s, r):
        pl.semaphore_signal(sem, inc=1, device_id=(p, s, r), device_id_type=MESH)

    above, below = patch < patch_count - 1, patch > 0

    @pl.when(jnp.logical_and(below, patch <= half))
    def _():
        for c in range(req_count):
            tell(barrier, patch - 1, seq, lax.rem(req + c, req_count))

    @pl.when(above)
    def _():
        for c in range(req_count):
            tell(barrier, patch + 1, seq, lax.rem(req + c, req_count))

    for c in range(1, req_count):
        tell(barrier, patch, seq, lax.rem(req + c, req_count))

    @pl.when(patch == 0)
    def _():
        for d in range(1, seq_count):
            tell(barrier, patch, lax.rem(seq + d, seq_count), req)

    has_below = 1 - (patch_count - 1 - patch) // (patch_count - 1)
    arrivals = (
        req_count - 1 + req_count * (has_below + 1 - upper) + (seq_count - 1) * (1 - has_below)
    )
    answers = jnp.logical_and(patch == patch_count - 1, patch > half)

    @pl.when(answers)
    def _():
        pl.semaphore_wait(barrier, arrivals)
        tell(info.at[0], patch - 1, seq, req)


    def lanes_of(d, base=0):
        g = lax.rem(seq + d, seq_count)
        return pl.ds(pl.multiple_of(base + g * HEAD_DIM, HEAD_DIM), HEAD_DIM)

    owner = lax.broadcasted_iota(jnp.int32, (groups, src_rows), 0)
    row_i = lax.broadcasted_iota(jnp.int32, (src_rows, src_rows), 0)
    col_i = lax.broadcasted_iota(jnp.int32, (src_rows, src_rows), 1)
    before = (row_i < col_i).astype(f32).astype(bf16)
    small[0].wait()
    small[1].start()
    mine = maps[...] == owner
    rank = jnp.dot(mine.astype(f32).astype(bf16), before, preferred_element_type=f32)
    slot = jnp.sum(
        jnp.where(mine, rank + (owner * per).astype(f32), 0.0), axis=0, keepdims=True
    )
    pick = (row_i == slot.astype(jnp.int32)).astype(f32).astype(bf16)

    def place_copy(hop):
        p, r = partner(hop)
        return pltpu.make_async_remote_copy(
            src_ref=place_out, dst_ref=place_in.at[me],
            send_sem=place_sem.at[0], recv_sem=place_sem.at[1],
            device_id=(p, seq, r), device_id_type=MESH,
        )

    def main_copy(l, hop, at=pl.ds(0, main_width)):
        p, r = partner(hop)
        return pltpu.make_async_remote_copy(
            src_ref=main_out.at[l, p * req_count + r, :, at], dst_ref=main_in.at[l, me, :, at],
            send_sem=main_send.at[0], recv_sem=main_recv.at[l],
            device_id=(p, seq, r), device_id_type=MESH,
        )

    def own_copy(i, hop):
        p, r = partner(hop)
        return pltpu.make_async_remote_copy(
            src_ref=own_out.at[i, p * req_count + r], dst_ref=own_in[i].at[me],
            send_sem=own_send.at[0], recv_sem=own_recv.at[i],
            device_id=(p, seq, r), device_id_type=MESH,
        )

    def part_copy(l, d):
        s = lax.rem(seq + d, seq_count)
        return pltpu.make_async_remote_copy(
            src_ref=part_out.at[l, d], dst_ref=part_in.at[l, d],
            send_sem=part_sem.at[0], recv_sem=part_sem.at[1],
            device_id=(patch, s, req), device_id_type=MESH,
        )

    def sort(l, base):
        turned = jnp.concatenate(
            [rows[l, :, lanes_of(d, base)] for d in range(1, seq_count)], axis=1
        )
        moved = jnp.dot(pick, turned, preferred_element_type=f32).astype(bf16)
        at = slice(0, side) if base == 0 else slice(side, main_width)
        main_out[l, :, :, at] = moved.reshape(groups, per, side)

    def send_first(l, at):
        for hop in mates:
            main_copy(l, hop, at).start()

        @pl.when(patch != half)
        def _():
            for hop in beside:
                main_copy(l, hop, at).start()

        if l < ahead:

            @pl.when(inner)
            def _():
                for hop in far[-1]:
                    main_copy(l, hop, at).start()

    for l in range(layers):
        if l == 0:
            first_rows[0].wait()
            second_rows.start()
            rest_rows.start()
            sort(l, 0)

            @pl.when(jnp.logical_not(answers))
            def _():
                pl.semaphore_wait(barrier, arrivals)

            send_first(l, pl.ds(0, side))
            first_rows[1].wait()
            sort(l, kvw)
            send_first(l, pl.ds(side, side))

            @pl.when(jnp.logical_and(patch == 1, above))
            def _():
                tell(info.at[1], patch + 1, seq, req)

        else:
            if l == 1:
                second_rows.wait()
            if l == 2:
                rest_rows.wait()
            sort(l, 0)
            sort(l, kvw)
            send_first(l, pl.ds(0, main_width))
        if l == 0:
            small[1].wait()
            small[2].start()
            local = (places[...] - seq * src_rows).astype(f32).astype(bf16)
            place_sorted = lax.dot_general(
                jnp.broadcast_to(local, (PAD, src_rows)), pick, NT,
                preferred_element_type=f32,
            )
            place_out[...] = place_sorted[0:1].astype(jnp.int32)
            place_in[me] = place_sorted[0:1].astype(jnp.int32)
            for hop in mates:
                place_copy(hop).start()

            @pl.when(patch != half)
            def _():
                for hop in beside:
                    place_copy(hop).start()

    for l in range(layers):
        turned = jnp.concatenate([rows[l, :, lanes_of(0)], rows[l, :, lanes_of(0, kvw)]], axis=1)
        moved = jnp.dot(pick, turned, preferred_element_type=f32).astype(bf16)
        own_out[0, :, l] = moved[:, :HEAD_DIM].reshape(groups, per, HEAD_DIM)
        own_out[1, :, l] = moved[:, HEAD_DIM:].reshape(groups, per, HEAD_DIM)
    def own_near():
        for i in range(2):
            for hop in beside:
                own_copy(i, hop).start()

    for i in range(2):
        for hop in mates:
            own_copy(i, hop).start()
    pl.when(patch != half)(own_near)
    listens = jnp.logical_or(
        patch < patch_count - 2, jnp.logical_and(patch >= half, above)
    )

    @pl.when(listens)
    def _():
        pl.semaphore_wait(info.at[0], 1)

    @pl.when(jnp.logical_and(listens, below))
    def _():
        tell(info.at[0], patch - 1, seq, req)

    @pl.when(patch > 1)
    def _():
        pl.semaphore_wait(info.at[1], 1)

    @pl.when(jnp.logical_and(patch > 1, above))
    def _():
        tell(info.at[1], patch + 1, seq, req)

    @pl.when(patch == 0)
    def _():
        for d in range(1, seq_count):
            tell(info.at[2], patch, lax.rem(seq + d, seq_count), req)

    @pl.when(patch == half)
    def _():
        for hop in beside:
            place_copy(hop).start()
        for l in range(layers):
            for hop in beside:
                main_copy(l, hop).start()
        own_near()

    for hop in late:
        place_copy(hop).start()
        for l in range(layers):
            main_copy(l, hop).start()
        for i in range(2):
            own_copy(i, hop).start()
    for wave in far:
        for hop in wave:
            place_copy(hop).start()
    for l in range(layers):
        for wave in far[:-1]:
            for hop in wave:
                main_copy(l, hop).start()

    @pl.when(jnp.logical_not(inner))
    def _():
        for l in range(ahead):
            for hop in far[-1]:
                main_copy(l, hop).start()

    for l in range(ahead, layers):
        for hop in far[-1]:
            main_copy(l, hop).start()
    for wave in far:
        for i in range(2):
            for hop in wave:
                own_copy(i, hop).start()
    text_copy.start()
    for l in range(layers):
        main_in[l, me] = main_out[l, me]
    for i in range(2):
        own_in[i][me] = own_out[i, me]

    small[2].wait()
    small[3].start()
    lines = query[...].astype(f32)
    for l in range(layers):
        for g in range(KV_HEADS):
            heads[l, g * PAD:(g + 1) * PAD, :] = jnp.concatenate(
                [
                    lines[l:l + 1, (g * group + h) * HEAD_DIM:(g * group + h + 1) * HEAD_DIM]
                    for h in range(group)
                ] + [jnp.zeros((PAD - group, HEAD_DIM), f32)],
                axis=0,
            )

    def head_block(l, d):
        g = lax.rem(seq + d, seq_count)
        return heads[l, pl.ds(pl.multiple_of(g * PAD, PAD), PAD), :]

    small[3].wait()
    positions = seq * text_dev + lax.broadcasted_iota(
        jnp.int32, (KV_HEADS * PAD, text_dev), 1
    )
    used = positions < length[0]
    lane_group = lax.broadcasted_iota(jnp.int32, (PAD, kvw), 1) // HEAD_DIM
    for l in range(layers):
        spread = jnp.concatenate(
            [
                jnp.where(
                    lane_group == lax.rem(seq + d, seq_count),
                    jnp.concatenate([head_block(l, d)] * KV_HEADS, axis=1),
                    0.0,
                )
                for d in range(seq_count)
            ],
            axis=0,
        ).astype(bf16)
        if l == 0:
            text_copy.wait()
        raw = lax.dot_general(
            spread, text[l, :, :kvw], NT, preferred_element_type=f32
        ) * scale
        scores[l] = jnp.where(used, raw, -jnp.inf)

    @pl.when(patch == 0)
    def _():
        pl.semaphore_wait(info.at[2], seq_count - 1)
        for p in range(1, patch_count):
            tell(info.at[2], p, seq, req)

    @pl.when(below)
    def _():
        pl.semaphore_wait(info.at[2], 1)

    settle(place_in.at[others], place_sem.at[1])
    wanted = (row_i == me * per + lax.rem(col_i, per)).astype(f32).astype(bf16)
    lanes = jnp.dot(
        place_in[...].reshape(groups, src_rows).astype(f32).astype(bf16), wanted,
        preferred_element_type=f32,
    )
    source = lax.broadcasted_iota(jnp.int32, (groups, src_rows), 1) // per
    place = jnp.sum(jnp.where(source == owner, lanes, 0.0), axis=0, keepdims=True)
    put = (row_i == place.astype(jnp.int32)).astype(f32).astype(bf16)
    put_out[...] = put

    zeros = jnp.zeros((PAD, HEAD_DIM), f32)
    for l in range(layers):
        spread = jnp.concatenate(
            [
                jnp.concatenate(
                    [head_block(l, d) if c == d else zeros for c in range(1, seq_count)],
                    axis=1,
                )
                for d in range(1, seq_count)
            ],
            axis=0,
        ).astype(bf16)
        settle(main_in.at[l, others], main_recv.at[l])
        block = main_in[l].reshape(src_rows, main_width)
        image_scores = lax.dot_general(
            spread, block[:, :side], NT, preferred_element_type=f32
        ) * scale
        both = jnp.concatenate([scores[l, PAD:, :], image_scores], axis=1)
        top = jnp.max(both, axis=1, keepdims=True)
        weights = jnp.exp(both - top)
        total = jnp.sum(weights, axis=1, keepdims=True)
        weights = weights.astype(bf16)
        image_sums = jnp.dot(
            weights[:, text_dev:], block[:, side:], preferred_element_type=f32
        )
        for d in range(1, seq_count):
            at = slice((d - 1) * PAD, d * PAD)
            text_sums = jnp.dot(
                weights[at, :text_dev], text[l, :, lanes_of(d, kvw)],
                preferred_element_type=f32,
            )
            part_out[l, d, :, :HEAD_DIM] = (
                text_sums + image_sums[at, (d - 1) * HEAD_DIM:d * HEAD_DIM]
            )
            part_out[l, d, :, HEAD_DIM:2 * HEAD_DIM] = jnp.broadcast_to(
                top[at], (PAD, HEAD_DIM)
            )
            part_out[l, d, :, 2 * HEAD_DIM:] = jnp.broadcast_to(total[at], (PAD, HEAD_DIM))
            part_copy(l, d).start()
        moved = jnp.dot(put, block, preferred_element_type=f32).astype(bf16)
        for d in range(1, seq_count):
            cache[l, 0, :, lanes_of(d)] = moved[:, (d - 1) * HEAD_DIM:d * HEAD_DIM]
            cache[l, 0, :, lanes_of(d, kvw)] = moved[
                :, side + (d - 1) * HEAD_DIM:side + d * HEAD_DIM
            ]

    settle(keys_in.at[others], own_recv.at[0])
    own_keys = [keys_in[:, l].reshape(src_rows, HEAD_DIM) for l in range(layers)]
    own_scores = jnp.concatenate(
        [
            jnp.concatenate(
                [
                    scores[l, :PAD, :],
                    lax.dot_general(
                        head_block(l, 0).astype(bf16), own_keys[l], NT,
                        preferred_element_type=f32,
                    ) * scale,
                ],
                axis=1,
            )
            for l in range(layers)
        ],
        axis=0,
    )
    own_top = jnp.max(own_scores, axis=1, keepdims=True)
    own_w = jnp.exp(own_scores - own_top)
    own_total = jnp.sum(own_w, axis=1, keepdims=True)
    rounded = own_w.astype(bf16)
    weights_out[...] = rounded[:, text_dev:]
    mine_now = []
    for l in range(layers):
        at = slice(l * PAD, (l + 1) * PAD)
        value = jnp.dot(
            rounded[at, :text_dev], text[l, :, lanes_of(0, kvw)], preferred_element_type=f32
        )
        mine_now.append((
            value,
            jnp.broadcast_to(own_top[at], (PAD, HEAD_DIM)),
            jnp.broadcast_to(own_total[at], (PAD, HEAD_DIM)),
        ))
    moved = jnp.dot(
        put, jnp.concatenate(own_keys, axis=1), preferred_element_type=f32
    ).astype(bf16)
    for l in range(layers):
        cache[l, 0, :, lanes_of(0)] = moved[:, l * HEAD_DIM:(l + 1) * HEAD_DIM]

    bands = pl.ds(1, seq_count - 1)
    settle(part_in.at[:, bands], part_sem.at[1])
    for l in range(layers):
        cells = [mine_now[l]] + [
            tuple(part_in[l, d, :, i * HEAD_DIM:(i + 1) * HEAD_DIM] for i in range(3))
            for d in range(1, seq_count)
        ]
        top = functools.reduce(jnp.maximum, [c[1] for c in cells])
        factors = [jnp.exp(c[1] - top) for c in cells]
        partial_out[l, :, :HEAD_DIM] = factors[0]
        partial_out[l, :, HEAD_DIM:2 * HEAD_DIM] = sum(
            f * c[0] for f, c in zip(factors, cells)
        )
        partial_out[l, :, 2 * HEAD_DIM:] = sum(f * c[2] for f, c in zip(factors, cells))

    settle(main_out.at[:, others], main_send.at[0])
    settle(place_in.at[others], place_sem.at[0])
    settle(part_out.at[:, bands], part_sem.at[0])
    settle(own_out.at[:, others], own_send.at[0])
    settle(values_in.at[others], own_recv.at[1])


def finish(
    dims, cache, put, values, weights, partial, att_out, cache_out, att, last, sem
):
    _, seq_count, _ = dims
    layers, _, src_rows, full = cache.shape
    kvw = full // 2
    group = HEADS // KV_HEADS
    seq = lax.axis_index("seq")
    f32, bf16 = jnp.float32, jnp.bfloat16

    def lanes_of(d):
        g = lax.rem(seq + d, seq_count)
        return pl.ds(pl.multiple_of(kvw + g * HEAD_DIM, HEAD_DIM), HEAD_DIM)

    for l in range(layers):
        pltpu.make_async_copy(
            cache.at[l, 0, :, pl.ds(0, kvw)], cache_out.at[l, 0, :, pl.ds(0, kvw)], sem.at[0]
        ).start()
        for d in range(1, seq_count):
            pltpu.make_async_copy(
                cache.at[l, 0, :, lanes_of(d)], cache_out.at[l, 0, :, lanes_of(d)], sem.at[0]
            ).start()
    own = [values[:, l].reshape(src_rows, HEAD_DIM) for l in range(layers)]
    both = jnp.concatenate([put[...], weights[...]], axis=0)
    moved = jnp.dot(both, jnp.concatenate(own, axis=1), preferred_element_type=f32)
    for l in range(layers):
        at = slice(l * HEAD_DIM, (l + 1) * HEAD_DIM)
        last[l] = moved[:src_rows, at].astype(bf16)
        pltpu.make_async_copy(
            last.at[l], cache_out.at[l, 0, :, lanes_of(0)], sem.at[0]
        ).start()
    lines = []
    for l in range(layers):
        value = moved[
            src_rows + l * PAD:src_rows + (l + 1) * PAD, l * HEAD_DIM:(l + 1) * HEAD_DIM
        ]
        factor = partial[l, :, :HEAD_DIM]
        summed = partial[l, :, HEAD_DIM:2 * HEAD_DIM]
        result = (summed + factor * value) / partial[l, :, 2 * HEAD_DIM:]
        lines.append(jnp.concatenate([result[h:h + 1] for h in range(group)], axis=1))
    att[...] = jnp.concatenate(lines, axis=0).astype(bf16)
    att_copy = pltpu.make_async_copy(att, att_out, sem.at[1])
    att_copy.start()
    pltpu.make_async_copy(cache, cache_out, sem.at[0]).wait()
    att_copy.wait()


def body(dims, query, text_cache, text_len, image_rows, patch_map, image_places):
    patch_count, seq_count, req_count = dims
    layers, req_dev, query_width = query.shape
    text_dev, full = text_cache.shape[2:]
    src_rows = image_rows.shape[1]
    groups = patch_count * req_count
    assert req_dev == 1 and seq_count == KV_HEADS and full == 2 * KV_HEADS * HEAD_DIM
    assert patch_count % 2 == 0 and layers > 2
    per = src_rows // groups
    main_width = full - 2 * HEAD_DIM
    rows_padded = KV_HEADS * PAD
    bf16, f32, i32 = jnp.bfloat16, jnp.float32, jnp.int32
    dma = pltpu.SemaphoreType.DMA
    vmem = pl.BlockSpec(memory_space=pltpu.VMEM)
    hbm = pl.BlockSpec(memory_space=pltpu.HBM)
    att_shape = jax.ShapeDtypeStruct((layers, query_width // seq_count), bf16)
    cache_shape = jax.ShapeDtypeStruct((layers, 1, src_rows, full), bf16)
    in_hbm = lambda x: pltpu.with_memory_space_constraint(x, pltpu.HBM)
    in_vmem = lambda x: pltpu.with_memory_space_constraint(x, pltpu.VMEM)
    state = pl.pallas_call(
        functools.partial(exchange, dims),
        out_shape=(
            pltpu.VMEM(cache_shape.shape, bf16),
            pltpu.VMEM((src_rows, src_rows), bf16),
            pltpu.VMEM((groups, layers, per, HEAD_DIM), bf16),
            pltpu.VMEM((layers * PAD, src_rows), bf16),
            pltpu.VMEM((layers, PAD, 3 * HEAD_DIM), f32),
        ),
        in_specs=[hbm, pl.BlockSpec(memory_space=pl.ANY), hbm, hbm, hbm, hbm],
        out_specs=(vmem,) * 5,
        scratch_shapes=[
            pltpu.VMEM((layers, query_width), bf16),
            pltpu.SMEM((1,), i32),
            pltpu.VMEM((1, src_rows), i32),
            pltpu.VMEM((1, src_rows), i32),
            pltpu.VMEM((layers, src_rows, full), bf16),
            pltpu.VMEM((layers, text_dev, full), bf16),
            pltpu.VMEM((layers, groups, per, main_width), bf16),
            pltpu.VMEM((layers, groups, per, main_width), bf16),
            pltpu.VMEM((2, groups, layers, per, HEAD_DIM), bf16),
            pltpu.VMEM((groups, layers, per, HEAD_DIM), bf16),
            pltpu.VMEM((1, src_rows), i32),
            pltpu.VMEM((groups, 1, src_rows), i32),
            pltpu.VMEM((layers, rows_padded, HEAD_DIM), f32),
            pltpu.VMEM((layers, rows_padded, text_dev), f32),
            pltpu.VMEM((layers, seq_count, PAD, 3 * HEAD_DIM), f32),
            pltpu.VMEM((layers, seq_count, PAD, 3 * HEAD_DIM), f32),
            dma((1,)), dma((4,)), dma((1,)), dma((layers,)), dma((1,)), dma((2,)),
            dma((2,)), dma((2,)), pltpu.SemaphoreType.REGULAR((3,)),
        ],
        compiler_params=pltpu.CompilerParams(
            collective_id=0, has_side_effects=True, vmem_limit_bytes=32 * 1024 * 1024
        ),
    )(
        in_hbm(query.reshape(layers, query_width)), text_len,
        in_hbm(patch_map.reshape(1, src_rows)), in_hbm(image_places.reshape(1, src_rows)),
        in_hbm(image_rows), in_hbm(text_cache),
    )
    attended, cache = pl.pallas_call(
        functools.partial(finish, dims),
        out_shape=(att_shape, cache_shape),
        in_specs=[vmem] * 5,
        out_specs=(hbm, hbm),
        scratch_shapes=[
            pltpu.VMEM(att_shape.shape, bf16),
            pltpu.VMEM((layers, src_rows, HEAD_DIM), bf16),
            dma((2,)),
        ],
    )(*(in_vmem(x) for x in state))
    return attended.reshape(layers, 1, query_width // seq_count), cache


def solution(mesh):
    dims = tuple(mesh.shape[a] for a in ("patch", "seq", "req"))
    return jax.shard_map(
        functools.partial(body, dims),
        mesh=mesh,
        in_specs=(
            P(None, ("patch", "req"), None),
            P(None, ("patch", "req"), "seq", None),
            P(("patch", "req")),
            P(None, ("patch", "seq", "req"), None),
            P(("patch", "seq", "req")),
            P(("patch", "seq", "req")),
        ),
        out_specs=(P(None, ("patch", "req"), "seq"), P(None, ("patch", "req"), "seq", None)),
        check_vma=False,
    )
```

```python
import functools
import math

import jax
import jax.numpy as jnp
from jax import lax
from jax.experimental import pallas as pl
from jax.experimental.pallas import tpu as pltpu
from jax.sharding import PartitionSpec as P

HEADS = 28
KV_HEADS = 4
HEAD_DIM = 128
PAD = 8
MESH = pl.DeviceIdType.MESH
NT = (((1,), (1,)), ((), ()))


def all_hops(patch_count, req_count):
    half = patch_count // 2
    cores = range(req_count)
    mates = [("mate", 0, c) for c in cores if c]
    near = [("near", i, c) for i in range(1, half) for c in cores]
    far = [[("far", k, c) for c in cores] for k in range(half)]
    return mates, near, far


def exchange(
    dims,
    query_hbm, len_hbm, map_hbm, place_hbm, rows_hbm, text_hbm,
    cache, put_out, values_in, weights_out, partial_out,
    query, length, maps, places, rows, text, main_out, main_in, own_out, keys_in, place_out, place_in,
    heads, scores, part_out, part_in, first_out,
    small_sem, load_sem, main_send, main_recv, own_send, own_recv, place_sem, part_sem,
    info,
):
    patch_count, seq_count, req_count = dims
    layers, src_rows, full = rows.shape
    text_dev = text.shape[1]
    kvw = full // 2
    group = HEADS // KV_HEADS
    groups = patch_count * req_count
    per = src_rows // groups
    half = patch_count // 2
    side = (seq_count - 1) * HEAD_DIM
    main_width = 2 * side
    scale = 1.0 / math.sqrt(HEAD_DIM)
    patch, seq, req = (lax.axis_index(a) for a in ("patch", "seq", "req"))
    me = patch * req_count + req
    mates, near, far = all_hops(patch_count, req_count)
    beside = near if half == 2 else []
    late = [hop for hop in near if hop not in beside]
    ahead = min(2, layers)
    f32, bf16 = jnp.float32, jnp.bfloat16
    upper = patch // half
    inner = jnp.logical_or(patch == half - 1, patch == half)

    def partner(hop):
        kind, i, c = hop
        if kind == "mate":
            return patch, lax.rem(req + c, req_count)
        r = req_count - 1 - c if kind == "near" or i == half - 1 else c
        if kind == "near":
            return upper * half + lax.rem(lax.rem(patch, half) + i, half), r
        return (1 - upper) * (patch_count - 1 - i) + upper * i, r

    others = pl.ds(0, groups - 1)
    own_in = (keys_in, values_in)
    second_rows = pltpu.make_async_copy(rows_hbm.at[1], rows.at[1], load_sem.at[0])
    rest = pl.ds(2, layers - 2)
    rest_rows = pltpu.make_async_copy(rows_hbm.at[rest], rows.at[rest], load_sem.at[1])
    text_copy = pltpu.make_async_copy(text_hbm.at[:, 0], text, load_sem.at[2])

    def settle(ref, sem):
        pltpu.make_async_copy(ref, ref, sem).wait()

    small = [
        pltpu.make_async_copy(map_hbm, maps, small_sem.at[0]),
        pltpu.make_async_copy(place_hbm, places, small_sem.at[0]),
        pltpu.make_async_copy(query_hbm, query, small_sem.at[0]),
        pltpu.make_async_copy(len_hbm, length, small_sem.at[0]),
    ]
    def lanes_of(d, base=0):
        g = lax.rem(seq + d, seq_count)
        return pl.ds(pl.multiple_of(base + g * HEAD_DIM, HEAD_DIM), HEAD_DIM)

    def load(i, at):
        pltpu.make_async_copy(rows_hbm.at[0, :, at], rows.at[0, :, at], load_sem.at[i]).start()

    small[0].start()
    load(0, lanes_of(1))
    for d in range(2, seq_count):
        load(1, lanes_of(d))
    barrier = pltpu.get_barrier_semaphore()

    def tell(sem, p, s, r):
        pl.semaphore_signal(sem, inc=1, device_id=(p, s, r), device_id_type=MESH)

    above, below = patch < patch_count - 1, patch > 0

    @pl.when(jnp.logical_and(below, patch <= half))
    def _():
        for c in range(req_count):
            tell(barrier, patch - 1, seq, lax.rem(req + c, req_count))

    @pl.when(above)
    def _():
        for c in range(req_count):
            tell(barrier, patch + 1, seq, lax.rem(req + c, req_count))

    for c in range(1, req_count):
        tell(barrier, patch, seq, lax.rem(req + c, req_count))

    @pl.when(patch == 0)
    def _():
        for d in range(1, seq_count):
            tell(barrier, patch, lax.rem(seq + d, seq_count), req)

    for d in range(1, seq_count):
        load(2, lanes_of(d, kvw))
    has_below = 1 - (patch_count - 1 - patch) // (patch_count - 1)
    arrivals = (
        req_count - 1 + req_count * (has_below + 1 - upper) + (seq_count - 1) * (1 - has_below)
    )
    answers = jnp.logical_and(patch == patch_count - 1, patch > half)

    @pl.when(answers)
    def _():
        pl.semaphore_wait(barrier, arrivals)
        tell(info.at[0], patch - 1, seq, req)


    owner = lax.broadcasted_iota(jnp.int32, (groups, src_rows), 0)
    row_i = lax.broadcasted_iota(jnp.int32, (src_rows, src_rows), 0)
    col_i = lax.broadcasted_iota(jnp.int32, (src_rows, src_rows), 1)
    before = (row_i < col_i).astype(f32).astype(bf16)
    small[0].wait()
    load(3, lanes_of(0))
    load(3, lanes_of(0, kvw))
    small[1].start()
    mine = maps[...] == owner
    rank = jnp.dot(mine.astype(f32).astype(bf16), before, preferred_element_type=f32)
    slot = jnp.sum(
        jnp.where(mine, rank + (owner * per).astype(f32), 0.0), axis=0, keepdims=True
    )
    slot = slot.astype(jnp.int32)
    p_first, _ = partner(far[-1][0])
    row_first = lax.broadcasted_iota(jnp.int32, (req_count * per, src_rows), 0)
    pick_first = (
        row_first + p_first * (req_count * per) == slot
    ).astype(f32).astype(bf16)

    def place_copy(hop):
        p, r = partner(hop)
        return pltpu.make_async_remote_copy(
            src_ref=place_out, dst_ref=place_in.at[me],
            send_sem=place_sem.at[0], recv_sem=place_sem.at[1],
            device_id=(p, seq, r), device_id_type=MESH,
        )

    def main_copy(l, hop, at=pl.ds(0, main_width)):
        p, r = partner(hop)
        return pltpu.make_async_remote_copy(
            src_ref=main_out.at[l, p * req_count + r, :, at], dst_ref=main_in.at[l, me, :, at],
            send_sem=main_send.at[0], recv_sem=main_recv.at[l],
            device_id=(p, seq, r), device_id_type=MESH,
        )

    def first_copy(hop):
        p, r = partner(hop)
        return pltpu.make_async_remote_copy(
            src_ref=first_out.at[r], dst_ref=main_in.at[0, me, :, pl.ds(0, HEAD_DIM)],
            send_sem=main_send.at[0], recv_sem=main_recv.at[0],
            device_id=(p, seq, r), device_id_type=MESH,
        )

    def own_copy(i, hop):
        p, r = partner(hop)
        return pltpu.make_async_remote_copy(
            src_ref=own_out.at[i, p * req_count + r], dst_ref=own_in[i].at[me],
            send_sem=own_send.at[0], recv_sem=own_recv.at[i],
            device_id=(p, seq, r), device_id_type=MESH,
        )

    def part_copy(l, d):
        s = lax.rem(seq + d, seq_count)
        return pltpu.make_async_remote_copy(
            src_ref=part_out.at[l, d], dst_ref=part_in.at[l, d],
            send_sem=part_sem.at[0], recv_sem=part_sem.at[1],
            device_id=(patch, s, req), device_id_type=MESH,
        )

    def sort(l, base):
        turned = jnp.concatenate(
            [rows[l, :, lanes_of(d, base)] for d in range(1, seq_count)], axis=1
        )
        moved = jnp.dot(pick, turned, preferred_element_type=f32).astype(bf16)
        at = slice(0, side) if base == 0 else slice(side, main_width)
        main_out[l, :, :, at] = moved.reshape(groups, per, side)

    def send_first(l, at, across):
        for hop in mates:
            main_copy(l, hop, at).start()

        @pl.when(patch != half)
        def _():
            for hop in beside:
                main_copy(l, hop, at).start()

        if l < ahead:

            @pl.when(inner)
            def _():
                for hop in far[-1]:
                    main_copy(l, hop, across).start()

    def settle_rows(i, width):
        settle(rows.at[0, :, pl.ds(0, width)], load_sem.at[i])

    settle_rows(0, HEAD_DIM)
    second_rows.start()
    moved = jnp.dot(pick_first, rows[0, :, lanes_of(1)], preferred_element_type=f32)
    first_out[...] = moved.astype(bf16).reshape(req_count, per, HEAD_DIM)

    @pl.when(jnp.logical_not(answers))
    def _():
        pl.semaphore_wait(barrier, arrivals)

    @pl.when(inner)
    def _():
        for hop in far[-1]:
            first_copy(hop).start()

    pick = (row_i == slot).astype(f32).astype(bf16)
    for l in range(layers):
        if l == 0:
            settle_rows(1, side - HEAD_DIM)
            rest_rows.start()
            sort(l, 0)
            send_first(l, pl.ds(0, side), pl.ds(HEAD_DIM, side - HEAD_DIM))
            settle_rows(2, side)
            sort(l, kvw)
            send_first(l, pl.ds(side, side), pl.ds(side, side))

            @pl.when(jnp.logical_and(patch == 1, above))
            def _():
                tell(info.at[1], patch + 1, seq, req)

        else:
            if l == 1:
                second_rows.wait()
            if l == 2:
                rest_rows.wait()
            sort(l, 0)
            sort(l, kvw)
            send_first(l, pl.ds(0, main_width), pl.ds(0, main_width))
        if l == 0:
            small[1].wait()
            small[2].start()
            local = (places[...] - seq * src_rows).astype(f32).astype(bf16)
            place_sorted = lax.dot_general(
                jnp.broadcast_to(local, (PAD, src_rows)), pick, NT,
                preferred_element_type=f32,
            )
            place_out[...] = place_sorted[0:1].astype(jnp.int32)
            place_in[me] = place_sorted[0:1].astype(jnp.int32)
            for hop in mates:
                place_copy(hop).start()

            @pl.when(patch != half)
            def _():
                for hop in beside:
                    place_copy(hop).start()

    settle_rows(3, 2 * HEAD_DIM)
    for l in range(layers):
        turned = jnp.concatenate([rows[l, :, lanes_of(0)], rows[l, :, lanes_of(0, kvw)]], axis=1)
        moved = jnp.dot(pick, turned, preferred_element_type=f32).astype(bf16)
        own_out[0, :, l] = moved[:, :HEAD_DIM].reshape(groups, per, HEAD_DIM)
        own_out[1, :, l] = moved[:, HEAD_DIM:].reshape(groups, per, HEAD_DIM)
    def own_near():
        for i in range(2):
            for hop in beside:
                own_copy(i, hop).start()

    for i in range(2):
        for hop in mates:
            own_copy(i, hop).start()
    pl.when(patch != half)(own_near)
    listens = jnp.logical_or(
        patch < patch_count - 2, jnp.logical_and(patch >= half, above)
    )

    @pl.when(listens)
    def _():
        pl.semaphore_wait(info.at[0], 1)

    @pl.when(jnp.logical_and(listens, below))
    def _():
        tell(info.at[0], patch - 1, seq, req)

    @pl.when(patch > 1)
    def _():
        pl.semaphore_wait(info.at[1], 1)

    @pl.when(jnp.logical_and(patch > 1, above))
    def _():
        tell(info.at[1], patch + 1, seq, req)

    @pl.when(patch == 0)
    def _():
        for d in range(1, seq_count):
            tell(info.at[2], patch, lax.rem(seq + d, seq_count), req)

    @pl.when(patch == half)
    def _():
        for hop in beside:
            place_copy(hop).start()
        for l in range(layers):
            for hop in beside:
                main_copy(l, hop).start()
        own_near()

    for hop in late:
        place_copy(hop).start()
        for l in range(layers):
            main_copy(l, hop).start()
        for i in range(2):
            own_copy(i, hop).start()
    for wave in far:
        for hop in wave:
            place_copy(hop).start()
    for l in range(layers):
        for wave in far[:-1]:
            for hop in wave:
                main_copy(l, hop).start()

    @pl.when(jnp.logical_not(inner))
    def _():
        for l in range(ahead):
            for hop in far[-1]:
                main_copy(l, hop).start()

    for l in range(ahead, layers):
        for hop in far[-1]:
            main_copy(l, hop).start()
    for wave in far:
        for i in range(2):
            for hop in wave:
                own_copy(i, hop).start()
    text_copy.start()
    for l in range(layers):
        main_in[l, me] = main_out[l, me]
    for i in range(2):
        own_in[i][me] = own_out[i, me]

    small[2].wait()
    small[3].start()
    lines = query[...].astype(f32)
    for l in range(layers):
        for g in range(KV_HEADS):
            heads[l, g * PAD:(g + 1) * PAD, :] = jnp.concatenate(
                [
                    lines[l:l + 1, (g * group + h) * HEAD_DIM:(g * group + h + 1) * HEAD_DIM]
                    for h in range(group)
                ] + [jnp.zeros((PAD - group, HEAD_DIM), f32)],
                axis=0,
            )

    def head_block(l, d):
        g = lax.rem(seq + d, seq_count)
        return heads[l, pl.ds(pl.multiple_of(g * PAD, PAD), PAD), :]

    small[3].wait()
    positions = seq * text_dev + lax.broadcasted_iota(
        jnp.int32, (KV_HEADS * PAD, text_dev), 1
    )
    used = positions < length[0]
    lane_group = lax.broadcasted_iota(jnp.int32, (PAD, kvw), 1) // HEAD_DIM
    for l in range(layers):
        spread = jnp.concatenate(
            [
                jnp.where(
                    lane_group == lax.rem(seq + d, seq_count),
                    jnp.concatenate([head_block(l, d)] * KV_HEADS, axis=1),
                    0.0,
                )
                for d in range(seq_count)
            ],
            axis=0,
        ).astype(bf16)
        if l == 0:
            text_copy.wait()
        raw = lax.dot_general(
            spread, text[l, :, :kvw], NT, preferred_element_type=f32
        ) * scale
        scores[l] = jnp.where(used, raw, -jnp.inf)

    @pl.when(patch == 0)
    def _():
        pl.semaphore_wait(info.at[2], seq_count - 1)
        for p in range(1, patch_count):
            tell(info.at[2], p, seq, req)

    @pl.when(below)
    def _():
        pl.semaphore_wait(info.at[2], 1)

    settle(place_in.at[others], place_sem.at[1])
    wanted = (row_i == me * per + lax.rem(col_i, per)).astype(f32).astype(bf16)
    lanes = jnp.dot(
        place_in[...].reshape(groups, src_rows).astype(f32).astype(bf16), wanted,
        preferred_element_type=f32,
    )
    source = lax.broadcasted_iota(jnp.int32, (groups, src_rows), 1) // per
    place = jnp.sum(jnp.where(source == owner, lanes, 0.0), axis=0, keepdims=True)
    put = (row_i == place.astype(jnp.int32)).astype(f32).astype(bf16)
    put_out[...] = put

    zeros = jnp.zeros((PAD, HEAD_DIM), f32)
    for l in range(layers):
        spread = jnp.concatenate(
            [
                jnp.concatenate(
                    [head_block(l, d) if c == d else zeros for c in range(1, seq_count)],
                    axis=1,
                )
                for d in range(1, seq_count)
            ],
            axis=0,
        ).astype(bf16)
        settle(main_in.at[l, others], main_recv.at[l])
        block = main_in[l].reshape(src_rows, main_width)
        image_scores = lax.dot_general(
            spread, block[:, :side], NT, preferred_element_type=f32
        ) * scale
        both = jnp.concatenate([scores[l, PAD:, :], image_scores], axis=1)
        top = jnp.max(both, axis=1, keepdims=True)
        weights = jnp.exp(both - top)
        total = jnp.sum(weights, axis=1, keepdims=True)
        weights = weights.astype(bf16)
        image_sums = jnp.dot(
            weights[:, text_dev:], block[:, side:], preferred_element_type=f32
        )
        for d in range(1, seq_count):
            at = slice((d - 1) * PAD, d * PAD)
            text_sums = jnp.dot(
                weights[at, :text_dev], text[l, :, lanes_of(d, kvw)],
                preferred_element_type=f32,
            )
            part_out[l, d, :, :HEAD_DIM] = (
                text_sums + image_sums[at, (d - 1) * HEAD_DIM:d * HEAD_DIM]
            )
            part_out[l, d, :, HEAD_DIM:2 * HEAD_DIM] = jnp.broadcast_to(
                top[at], (PAD, HEAD_DIM)
            )
            part_out[l, d, :, 2 * HEAD_DIM:] = jnp.broadcast_to(total[at], (PAD, HEAD_DIM))
            part_copy(l, d).start()
        moved = jnp.dot(put, block, preferred_element_type=f32).astype(bf16)
        for d in range(1, seq_count):
            cache[l, 0, :, lanes_of(d)] = moved[:, (d - 1) * HEAD_DIM:d * HEAD_DIM]
            cache[l, 0, :, lanes_of(d, kvw)] = moved[
                :, side + (d - 1) * HEAD_DIM:side + d * HEAD_DIM
            ]

    settle(keys_in.at[others], own_recv.at[0])
    own_keys = [keys_in[:, l].reshape(src_rows, HEAD_DIM) for l in range(layers)]
    own_scores = jnp.concatenate(
        [
            jnp.concatenate(
                [
                    scores[l, :PAD, :],
                    lax.dot_general(
                        head_block(l, 0).astype(bf16), own_keys[l], NT,
                        preferred_element_type=f32,
                    ) * scale,
                ],
                axis=1,
            )
            for l in range(layers)
        ],
        axis=0,
    )
    own_top = jnp.max(own_scores, axis=1, keepdims=True)
    own_w = jnp.exp(own_scores - own_top)
    own_total = jnp.sum(own_w, axis=1, keepdims=True)
    rounded = own_w.astype(bf16)
    weights_out[...] = rounded[:, text_dev:]
    mine_now = []
    for l in range(layers):
        at = slice(l * PAD, (l + 1) * PAD)
        value = jnp.dot(
            rounded[at, :text_dev], text[l, :, lanes_of(0, kvw)], preferred_element_type=f32
        )
        mine_now.append((
            value,
            jnp.broadcast_to(own_top[at], (PAD, HEAD_DIM)),
            jnp.broadcast_to(own_total[at], (PAD, HEAD_DIM)),
        ))
    moved = jnp.dot(
        put, jnp.concatenate(own_keys, axis=1), preferred_element_type=f32
    ).astype(bf16)
    for l in range(layers):
        cache[l, 0, :, lanes_of(0)] = moved[:, l * HEAD_DIM:(l + 1) * HEAD_DIM]

    bands = pl.ds(1, seq_count - 1)
    settle(part_in.at[:, bands], part_sem.at[1])
    for l in range(layers):
        cells = [mine_now[l]] + [
            tuple(part_in[l, d, :, i * HEAD_DIM:(i + 1) * HEAD_DIM] for i in range(3))
            for d in range(1, seq_count)
        ]
        top = functools.reduce(jnp.maximum, [c[1] for c in cells])
        factors = [jnp.exp(c[1] - top) for c in cells]
        partial_out[l, :, :HEAD_DIM] = factors[0]
        partial_out[l, :, HEAD_DIM:2 * HEAD_DIM] = sum(
            f * c[0] for f, c in zip(factors, cells)
        )
        partial_out[l, :, 2 * HEAD_DIM:] = sum(f * c[2] for f, c in zip(factors, cells))

    settle(main_out.at[:, others], main_send.at[0])
    settle(place_in.at[others], place_sem.at[0])
    settle(part_out.at[:, bands], part_sem.at[0])
    settle(own_out.at[:, others], own_send.at[0])
    settle(values_in.at[others], own_recv.at[1])


def finish(
    dims, cache, put, values, weights, partial, att_out, cache_out, att, last, sem
):
    _, seq_count, _ = dims
    layers, _, src_rows, full = cache.shape
    kvw = full // 2
    group = HEADS // KV_HEADS
    seq = lax.axis_index("seq")
    f32, bf16 = jnp.float32, jnp.bfloat16

    def lanes_of(d):
        g = lax.rem(seq + d, seq_count)
        return pl.ds(pl.multiple_of(kvw + g * HEAD_DIM, HEAD_DIM), HEAD_DIM)

    def write(piece, at):
        pltpu.make_async_copy(piece, cache_out.at[:, 0, :, at], sem.at[0]).start()

    keys = pl.ds(0, kvw)
    write(cache.at[:, 0, :, keys], keys)
    for d in range(1, seq_count):
        write(cache.at[:, 0, :, lanes_of(d)], lanes_of(d))
    own = [values[:, l].reshape(src_rows, HEAD_DIM) for l in range(layers)]
    both = jnp.concatenate([put[...], weights[...]], axis=0)
    moved = jnp.dot(both, jnp.concatenate(own, axis=1), preferred_element_type=f32)
    for l in range(layers):
        at = slice(l * HEAD_DIM, (l + 1) * HEAD_DIM)
        last[l] = moved[:src_rows, at].astype(bf16)
    write(last, lanes_of(0))
    lines = []
    for l in range(layers):
        value = moved[
            src_rows + l * PAD:src_rows + (l + 1) * PAD, l * HEAD_DIM:(l + 1) * HEAD_DIM
        ]
        factor = partial[l, :, :HEAD_DIM]
        summed = partial[l, :, HEAD_DIM:2 * HEAD_DIM]
        result = (summed + factor * value) / partial[l, :, 2 * HEAD_DIM:]
        lines.append(jnp.concatenate([result[h:h + 1] for h in range(group)], axis=1))
    att[...] = jnp.concatenate(lines, axis=0).astype(bf16)
    att_copy = pltpu.make_async_copy(att, att_out, sem.at[1])
    att_copy.start()
    pltpu.make_async_copy(cache, cache_out, sem.at[0]).wait()
    att_copy.wait()


def body(dims, query, text_cache, text_len, image_rows, patch_map, image_places):
    patch_count, seq_count, req_count = dims
    layers, req_dev, query_width = query.shape
    text_dev, full = text_cache.shape[2:]
    src_rows = image_rows.shape[1]
    groups = patch_count * req_count
    assert req_dev == 1 and seq_count == KV_HEADS and full == 2 * KV_HEADS * HEAD_DIM
    assert patch_count % 2 == 0 and layers > 2
    per = src_rows // groups
    main_width = full - 2 * HEAD_DIM
    rows_padded = KV_HEADS * PAD
    bf16, f32, i32 = jnp.bfloat16, jnp.float32, jnp.int32
    dma = pltpu.SemaphoreType.DMA
    vmem = pl.BlockSpec(memory_space=pltpu.VMEM)
    hbm = pl.BlockSpec(memory_space=pltpu.HBM)
    att_shape = jax.ShapeDtypeStruct((layers, query_width // seq_count), bf16)
    cache_shape = jax.ShapeDtypeStruct((layers, 1, src_rows, full), bf16)
    in_hbm = lambda x: pltpu.with_memory_space_constraint(x, pltpu.HBM)
    in_vmem = lambda x: pltpu.with_memory_space_constraint(x, pltpu.VMEM)
    state = pl.pallas_call(
        functools.partial(exchange, dims),
        out_shape=(
            pltpu.VMEM(cache_shape.shape, bf16),
            pltpu.VMEM((src_rows, src_rows), bf16),
            pltpu.VMEM((groups, layers, per, HEAD_DIM), bf16),
            pltpu.VMEM((layers * PAD, src_rows), bf16),
            pltpu.VMEM((layers, PAD, 3 * HEAD_DIM), f32),
        ),
        in_specs=[hbm, pl.BlockSpec(memory_space=pl.ANY), hbm, hbm, hbm, hbm],
        out_specs=(vmem,) * 5,
        scratch_shapes=[
            pltpu.VMEM((layers, query_width), bf16),
            pltpu.SMEM((1,), i32),
            pltpu.VMEM((1, src_rows), i32),
            pltpu.VMEM((1, src_rows), i32),
            pltpu.VMEM((layers, src_rows, full), bf16),
            pltpu.VMEM((layers, text_dev, full), bf16),
            pltpu.VMEM((layers, groups, per, main_width), bf16),
            pltpu.VMEM((layers, groups, per, main_width), bf16),
            pltpu.VMEM((2, groups, layers, per, HEAD_DIM), bf16),
            pltpu.VMEM((groups, layers, per, HEAD_DIM), bf16),
            pltpu.VMEM((1, src_rows), i32),
            pltpu.VMEM((groups, 1, src_rows), i32),
            pltpu.VMEM((layers, rows_padded, HEAD_DIM), f32),
            pltpu.VMEM((layers, rows_padded, text_dev), f32),
            pltpu.VMEM((layers, seq_count, PAD, 3 * HEAD_DIM), f32),
            pltpu.VMEM((layers, seq_count, PAD, 3 * HEAD_DIM), f32),
            pltpu.VMEM((req_count, per, HEAD_DIM), bf16),
            dma((1,)), dma((4,)), dma((1,)), dma((layers,)), dma((1,)), dma((2,)),
            dma((2,)), dma((2,)), pltpu.SemaphoreType.REGULAR((3,)),
        ],
        compiler_params=pltpu.CompilerParams(
            collective_id=0, has_side_effects=True, vmem_limit_bytes=32 * 1024 * 1024
        ),
    )(
        in_hbm(query.reshape(layers, query_width)), text_len,
        in_hbm(patch_map.reshape(1, src_rows)), in_hbm(image_places.reshape(1, src_rows)),
        in_hbm(image_rows), in_hbm(text_cache),
    )
    attended, cache = pl.pallas_call(
        functools.partial(finish, dims),
        out_shape=(att_shape, cache_shape),
        in_specs=[vmem] * 5,
        out_specs=(hbm, hbm),
        scratch_shapes=[
            pltpu.VMEM(att_shape.shape, bf16),
            pltpu.VMEM((layers, src_rows, HEAD_DIM), bf16),
            dma((2,)),
        ],
    )(*(in_vmem(x) for x in state))
    return attended.reshape(layers, 1, query_width // seq_count), cache


def solution(mesh):
    dims = tuple(mesh.shape[a] for a in ("patch", "seq", "req"))
    return jax.shard_map(
        functools.partial(body, dims),
        mesh=mesh,
        in_specs=(
            P(None, ("patch", "req"), None),
            P(None, ("patch", "req"), "seq", None),
            P(("patch", "req")),
            P(None, ("patch", "seq", "req"), None),
            P(("patch", "seq", "req")),
            P(("patch", "seq", "req")),
        ),
        out_specs=(P(None, ("patch", "req"), "seq"), P(None, ("patch", "req"), "seq", None)),
        check_vma=False,
    )
```

```python
import functools
import math

import jax
import jax.numpy as jnp
from jax import lax
from jax.experimental import pallas as pl
from jax.experimental.pallas import tpu as pltpu
from jax.sharding import PartitionSpec as P

HEADS = 28
KV_HEADS = 4
HEAD_DIM = 128
PAD = 8
MESH = pl.DeviceIdType.MESH
NT = (((1,), (1,)), ((), ()))


def all_hops(patch_count, req_count):
    half = patch_count // 2
    cores = range(req_count)
    mates = [("mate", 0, c) for c in cores if c]
    near = [("near", i, c) for i in range(1, half) for c in cores]
    far = [[("far", k, c) for c in cores] for k in range(half)]
    return mates, near, far


def exchange(
    dims,
    query_hbm, len_hbm, map_hbm, place_hbm, rows_hbm, text_hbm,
    cache, put_out, values_in, weights_out, partial_out,
    query, length, maps, places, rows, text, main_out, main_in, own_out, keys_in, place_out, place_in,
    heads, scores, part_out, part_in, first_out,
    small_sem, load_sem, send_sem, main_recv, own_recv, late_recv,
    info,
):
    patch_count, seq_count, req_count = dims
    layers, src_rows, full = rows.shape
    text_dev = text.shape[1]
    kvw = full // 2
    group = HEADS // KV_HEADS
    groups = patch_count * req_count
    per = src_rows // groups
    half = patch_count // 2
    side = (seq_count - 1) * HEAD_DIM
    main_width = 2 * side
    scale = 1.0 / math.sqrt(HEAD_DIM)
    patch, seq, req = (lax.axis_index(a) for a in ("patch", "seq", "req"))
    me = patch * req_count + req
    mates, near, far = all_hops(patch_count, req_count)
    beside = near if half == 2 else []
    late = [hop for hop in near if hop not in beside]
    ahead = min(2, layers)
    f32, bf16 = jnp.float32, jnp.bfloat16
    upper = patch // half
    inner = jnp.logical_or(patch == half - 1, patch == half)

    def partner(hop):
        kind, i, c = hop
        if kind == "mate":
            return patch, lax.rem(req + c, req_count)
        r = req_count - 1 - c if kind == "near" or i == half - 1 else c
        if kind == "near":
            return upper * half + lax.rem(lax.rem(patch, half) + i, half), r
        return (1 - upper) * (patch_count - 1 - i) + upper * i, r

    others = pl.ds(0, groups - 1)
    own_in = (keys_in, values_in)
    second_rows = pltpu.make_async_copy(rows_hbm.at[1], rows.at[1], load_sem.at[0])
    rest = pl.ds(2, layers - 2)
    rest_rows = pltpu.make_async_copy(rows_hbm.at[rest], rows.at[rest], load_sem.at[1])
    text_copy = pltpu.make_async_copy(text_hbm.at[:, 0], text, load_sem.at[2])

    def settle(ref, sem):
        pltpu.make_async_copy(ref, ref, sem).wait()

    small = [
        pltpu.make_async_copy(map_hbm, maps, small_sem.at[0]),
        pltpu.make_async_copy(place_hbm, places, small_sem.at[0]),
        pltpu.make_async_copy(query_hbm, query, small_sem.at[0]),
        pltpu.make_async_copy(len_hbm, length, small_sem.at[0]),
    ]
    def lanes_of(d, base=0):
        g = lax.rem(seq + d, seq_count)
        return pl.ds(pl.multiple_of(base + g * HEAD_DIM, HEAD_DIM), HEAD_DIM)

    def load(i, at):
        pltpu.make_async_copy(rows_hbm.at[0, :, at], rows.at[0, :, at], load_sem.at[i]).start()

    small[0].start()
    load(0, lanes_of(1))
    barrier = pltpu.get_barrier_semaphore()

    def tell(sem, p, s, r):
        pl.semaphore_signal(sem, inc=1, device_id=(p, s, r), device_id_type=MESH)

    above, below = patch < patch_count - 1, patch > 0

    @pl.when(jnp.logical_and(below, patch <= half))
    def _():
        for c in range(req_count):
            tell(barrier, patch - 1, seq, lax.rem(req + c, req_count))

    @pl.when(above)
    def _():
        for c in range(req_count):
            tell(barrier, patch + 1, seq, lax.rem(req + c, req_count))

    for c in range(1, req_count):
        tell(barrier, patch, seq, lax.rem(req + c, req_count))

    @pl.when(patch == 0)
    def _():
        for d in range(1, seq_count):
            tell(barrier, patch, lax.rem(seq + d, seq_count), req)

    for d in range(2, seq_count):
        load(1, lanes_of(d))
    for d in range(1, seq_count):
        load(2, lanes_of(d, kvw))
    has_below = 1 - (patch_count - 1 - patch) // (patch_count - 1)
    arrivals = (
        req_count - 1 + req_count * (has_below + 1 - upper) + (seq_count - 1) * (1 - has_below)
    )
    answers = jnp.logical_and(patch == patch_count - 1, patch > half)

    @pl.when(answers)
    def _():
        pl.semaphore_wait(barrier, arrivals)
        tell(info.at[0], patch - 1, seq, req)


    owner = lax.broadcasted_iota(jnp.int32, (groups, src_rows), 0)
    source = lax.broadcasted_iota(jnp.int32, (groups, src_rows), 1) // per
    row_i = lax.broadcasted_iota(jnp.int32, (src_rows, src_rows), 0)
    col_i = lax.broadcasted_iota(jnp.int32, (src_rows, src_rows), 1)
    before = (row_i < col_i).astype(f32).astype(bf16)
    small[0].wait()
    small[1].start()
    mine = maps[...] == owner
    rank = jnp.dot(mine.astype(f32).astype(bf16), before, preferred_element_type=f32)
    slot = jnp.sum(
        jnp.where(mine, rank + (owner * per).astype(f32), 0.0), axis=0, keepdims=True
    )
    slot = slot.astype(jnp.int32)
    p_first, _ = partner(far[-1][0])
    row_first = lax.broadcasted_iota(jnp.int32, (req_count * per, src_rows), 0)
    pick_first = (
        row_first + p_first * (req_count * per) == slot
    ).astype(f32).astype(bf16)

    def place_copy(hop):
        p, r = partner(hop)
        return pltpu.make_async_remote_copy(
            src_ref=place_out.at[p * req_count + r], dst_ref=place_in.at[me],
            send_sem=send_sem.at[1], recv_sem=late_recv.at[0],
            device_id=(p, seq, r), device_id_type=MESH,
        )

    def main_copy(l, hop, at=pl.ds(0, main_width)):
        p, r = partner(hop)
        return pltpu.make_async_remote_copy(
            src_ref=main_out.at[l, p * req_count + r, :, at], dst_ref=main_in.at[l, me, :, at],
            send_sem=send_sem.at[0], recv_sem=main_recv.at[l],
            device_id=(p, seq, r), device_id_type=MESH,
        )

    def first_copy(hop):
        p, r = partner(hop)
        return pltpu.make_async_remote_copy(
            src_ref=first_out.at[r], dst_ref=main_in.at[0, me, :, pl.ds(0, HEAD_DIM)],
            send_sem=send_sem.at[0], recv_sem=main_recv.at[0],
            device_id=(p, seq, r), device_id_type=MESH,
        )

    def own_copy(i, hop):
        p, r = partner(hop)
        return pltpu.make_async_remote_copy(
            src_ref=own_out.at[i, p * req_count + r], dst_ref=own_in[i].at[me],
            send_sem=send_sem.at[2], recv_sem=own_recv.at[i],
            device_id=(p, seq, r), device_id_type=MESH,
        )

    def part_copy(l, d):
        s = lax.rem(seq + d, seq_count)
        return pltpu.make_async_remote_copy(
            src_ref=part_out.at[l, d], dst_ref=part_in.at[l, d],
            send_sem=send_sem.at[1], recv_sem=late_recv.at[1],
            device_id=(patch, s, req), device_id_type=MESH,
        )

    def sort(l, base):
        turned = jnp.concatenate(
            [rows[l, :, lanes_of(d, base)] for d in range(1, seq_count)], axis=1
        )
        moved = jnp.dot(pick, turned, preferred_element_type=f32).astype(bf16)
        at = slice(0, side) if base == 0 else slice(side, main_width)
        main_out[l, :, :, at] = moved.reshape(groups, per, side)

    def send_first(l, at, across):
        for hop in mates:
            main_copy(l, hop, at).start()

        @pl.when(patch != half)
        def _():
            for hop in beside:
                main_copy(l, hop, at).start()

        if l < ahead:

            @pl.when(inner)
            def _():
                for hop in far[-1]:
                    main_copy(l, hop, across).start()

    def settle_rows(i, width):
        settle(rows.at[0, :, pl.ds(0, width)], load_sem.at[i])

    settle_rows(0, HEAD_DIM)
    second_rows.start()
    moved = jnp.dot(pick_first, rows[0, :, lanes_of(1)], preferred_element_type=f32)
    first_out[...] = moved.astype(bf16).reshape(req_count, per, HEAD_DIM)

    @pl.when(jnp.logical_not(answers))
    def _():
        pl.semaphore_wait(barrier, arrivals)

    @pl.when(inner)
    def _():
        for hop in far[-1]:
            first_copy(hop).start()

    pick = (row_i == slot).astype(f32).astype(bf16)
    for l in range(layers):
        if l == 0:
            settle_rows(1, side - HEAD_DIM)
            rest_rows.start()
            sort(l, 0)
            send_first(l, pl.ds(0, side), pl.ds(HEAD_DIM, side - HEAD_DIM))
            settle_rows(2, side)
            load(2, lanes_of(0))
            load(2, lanes_of(0, kvw))
            sort(l, kvw)
            send_first(l, pl.ds(side, side), pl.ds(side, side))

            @pl.when(jnp.logical_and(patch == 1, above))
            def _():
                tell(info.at[1], patch + 1, seq, req)

        else:
            if l == 1:
                second_rows.wait()
            if l == 2:
                rest_rows.wait()
            sort(l, 0)
            sort(l, kvw)
            send_first(l, pl.ds(0, main_width), pl.ds(0, main_width))
        if l == 0:
            small[1].wait()
            small[2].start()
            local = (places[...] - seq * src_rows).astype(f32).astype(bf16)
            place_sorted = lax.dot_general(
                jnp.broadcast_to(local, (PAD, src_rows)), pick, NT,
                preferred_element_type=f32,
            )
            apart = jnp.where(source == owner, place_sorted[0:1], 0.0).astype(bf16)
            lane = lax.broadcasted_iota(jnp.int32, (src_rows, HEAD_DIM), 1)
            entry = lax.broadcasted_iota(jnp.int32, (src_rows, HEAD_DIM), 0)
            gather = (lax.rem(entry, per) == lane).astype(f32).astype(bf16)
            placed = jnp.dot(apart, gather, preferred_element_type=f32).astype(jnp.int32)
            place_out[...] = placed.reshape(groups, 1, HEAD_DIM)
            place_in[me] = place_out[me]
            for hop in mates:
                place_copy(hop).start()

            @pl.when(patch != half)
            def _():
                for hop in beside:
                    place_copy(hop).start()

    settle_rows(2, 2 * HEAD_DIM)
    for l in range(layers):
        turned = jnp.concatenate([rows[l, :, lanes_of(0)], rows[l, :, lanes_of(0, kvw)]], axis=1)
        moved = jnp.dot(pick, turned, preferred_element_type=f32).astype(bf16)
        own_out[0, :, l] = moved[:, :HEAD_DIM].reshape(groups, per, HEAD_DIM)
        own_out[1, :, l] = moved[:, HEAD_DIM:].reshape(groups, per, HEAD_DIM)
    def own_near():
        for i in range(2):
            for hop in beside:
                own_copy(i, hop).start()

    for i in range(2):
        for hop in mates:
            own_copy(i, hop).start()
    pl.when(patch != half)(own_near)
    listens = jnp.logical_or(
        patch < patch_count - 2, jnp.logical_and(patch >= half, above)
    )

    @pl.when(listens)
    def _():
        pl.semaphore_wait(info.at[0], 1)

    @pl.when(jnp.logical_and(listens, below))
    def _():
        tell(info.at[0], patch - 1, seq, req)

    @pl.when(patch > 1)
    def _():
        pl.semaphore_wait(info.at[1], 1)

    @pl.when(jnp.logical_and(patch > 1, above))
    def _():
        tell(info.at[1], patch + 1, seq, req)

    @pl.when(patch == 0)
    def _():
        for d in range(1, seq_count):
            tell(info.at[2], patch, lax.rem(seq + d, seq_count), req)

    @pl.when(patch == half)
    def _():
        for hop in beside:
            place_copy(hop).start()
        for l in range(layers):
            for hop in beside:
                main_copy(l, hop).start()
        own_near()

    for hop in late:
        place_copy(hop).start()
        for l in range(layers):
            main_copy(l, hop).start()
        for i in range(2):
            own_copy(i, hop).start()
    for wave in far:
        for hop in wave:
            place_copy(hop).start()
    for l in range(layers):
        for wave in far[:-1]:
            for hop in wave:
                main_copy(l, hop).start()

    @pl.when(jnp.logical_not(inner))
    def _():
        for l in range(ahead):
            for hop in far[-1]:
                main_copy(l, hop).start()

    for l in range(ahead, layers):
        for hop in far[-1]:
            main_copy(l, hop).start()
    for wave in far:
        for i in range(2):
            for hop in wave:
                own_copy(i, hop).start()
    text_copy.start()
    for l in range(layers):
        main_in[l, me] = main_out[l, me]
    for i in range(2):
        own_in[i][me] = own_out[i, me]

    small[2].wait()
    small[3].start()
    lines = query[...].astype(f32)
    for l in range(layers):
        for g in range(KV_HEADS):
            heads[l, g * PAD:(g + 1) * PAD, :] = jnp.concatenate(
                [
                    lines[l:l + 1, (g * group + h) * HEAD_DIM:(g * group + h + 1) * HEAD_DIM]
                    for h in range(group)
                ] + [jnp.zeros((PAD - group, HEAD_DIM), f32)],
                axis=0,
            )

    def head_block(l, d):
        g = lax.rem(seq + d, seq_count)
        return heads[l, pl.ds(pl.multiple_of(g * PAD, PAD), PAD), :]

    small[3].wait()
    positions = seq * text_dev + lax.broadcasted_iota(
        jnp.int32, (KV_HEADS * PAD, text_dev), 1
    )
    used = positions < length[0]
    lane_group = lax.broadcasted_iota(jnp.int32, (PAD, kvw), 1) // HEAD_DIM
    for l in range(layers):
        spread = jnp.concatenate(
            [
                jnp.where(
                    lane_group == lax.rem(seq + d, seq_count),
                    jnp.concatenate([head_block(l, d)] * KV_HEADS, axis=1),
                    0.0,
                )
                for d in range(seq_count)
            ],
            axis=0,
        ).astype(bf16)
        if l == 0:
            text_copy.wait()
        raw = lax.dot_general(
            spread, text[l, :, :kvw], NT, preferred_element_type=f32
        ) * scale
        scores[l] = jnp.where(used, raw, -jnp.inf)

    @pl.when(patch == 0)
    def _():
        pl.semaphore_wait(info.at[2], seq_count - 1)
        for p in range(1, patch_count):
            tell(info.at[2], p, seq, req)

    @pl.when(below)
    def _():
        pl.semaphore_wait(info.at[2], 1)

    settle(place_in.at[others], late_recv.at[0])
    slot_i = lax.broadcasted_iota(jnp.int32, (HEAD_DIM, src_rows), 0)
    place_i = lax.broadcasted_iota(jnp.int32, (HEAD_DIM, src_rows), 1)
    wanted = (slot_i == lax.rem(place_i, per)).astype(f32).astype(bf16)
    lanes = jnp.dot(
        place_in[...].reshape(groups, HEAD_DIM).astype(f32).astype(bf16), wanted,
        preferred_element_type=f32,
    )
    place = jnp.sum(jnp.where(source == owner, lanes, 0.0), axis=0, keepdims=True)
    put = (row_i == place.astype(jnp.int32)).astype(f32).astype(bf16)
    put_out[...] = put

    zeros = jnp.zeros((PAD, HEAD_DIM), f32)
    for l in range(layers):
        spread = jnp.concatenate(
            [
                jnp.concatenate(
                    [head_block(l, d) if c == d else zeros for c in range(1, seq_count)],
                    axis=1,
                )
                for d in range(1, seq_count)
            ],
            axis=0,
        ).astype(bf16)
        settle(main_in.at[l, others], main_recv.at[l])
        if l == 0:
            settle(place_in.at[others], send_sem.at[1])
        block = main_in[l].reshape(src_rows, main_width)
        image_scores = lax.dot_general(
            spread, block[:, :side], NT, preferred_element_type=f32
        ) * scale
        both = jnp.concatenate([scores[l, PAD:, :], image_scores], axis=1)
        top = jnp.max(both, axis=1, keepdims=True)
        weights = jnp.exp(both - top)
        total = jnp.sum(weights, axis=1, keepdims=True)
        weights = weights.astype(bf16)
        image_sums = jnp.dot(
            weights[:, text_dev:], block[:, side:], preferred_element_type=f32
        )
        for d in range(1, seq_count):
            at = slice((d - 1) * PAD, d * PAD)
            text_sums = jnp.dot(
                weights[at, :text_dev], text[l, :, lanes_of(d, kvw)],
                preferred_element_type=f32,
            )
            part_out[l, d, :, :HEAD_DIM] = (
                text_sums + image_sums[at, (d - 1) * HEAD_DIM:d * HEAD_DIM]
            )
            part_out[l, d, :, HEAD_DIM:2 * HEAD_DIM] = jnp.broadcast_to(
                top[at], (PAD, HEAD_DIM)
            )
            part_out[l, d, :, 2 * HEAD_DIM:] = jnp.broadcast_to(total[at], (PAD, HEAD_DIM))
            part_copy(l, d).start()
        moved = jnp.dot(put, block, preferred_element_type=f32).astype(bf16)
        for d in range(1, seq_count):
            cache[l, 0, :, lanes_of(d)] = moved[:, (d - 1) * HEAD_DIM:d * HEAD_DIM]
            cache[l, 0, :, lanes_of(d, kvw)] = moved[
                :, side + (d - 1) * HEAD_DIM:side + d * HEAD_DIM
            ]

    settle(keys_in.at[others], own_recv.at[0])
    own_keys = [keys_in[:, l].reshape(src_rows, HEAD_DIM) for l in range(layers)]
    own_scores = jnp.concatenate(
        [
            jnp.concatenate(
                [
                    scores[l, :PAD, :],
                    lax.dot_general(
                        head_block(l, 0).astype(bf16), own_keys[l], NT,
                        preferred_element_type=f32,
                    ) * scale,
                ],
                axis=1,
            )
            for l in range(layers)
        ],
        axis=0,
    )
    own_top = jnp.max(own_scores, axis=1, keepdims=True)
    own_w = jnp.exp(own_scores - own_top)
    own_total = jnp.sum(own_w, axis=1, keepdims=True)
    rounded = own_w.astype(bf16)
    weights_out[...] = rounded[:, text_dev:]
    mine_now = []
    for l in range(layers):
        at = slice(l * PAD, (l + 1) * PAD)
        value = jnp.dot(
            rounded[at, :text_dev], text[l, :, lanes_of(0, kvw)], preferred_element_type=f32
        )
        mine_now.append((
            value,
            jnp.broadcast_to(own_top[at], (PAD, HEAD_DIM)),
            jnp.broadcast_to(own_total[at], (PAD, HEAD_DIM)),
        ))
    moved = jnp.dot(
        put, jnp.concatenate(own_keys, axis=1), preferred_element_type=f32
    ).astype(bf16)
    for l in range(layers):
        cache[l, 0, :, lanes_of(0)] = moved[:, l * HEAD_DIM:(l + 1) * HEAD_DIM]

    bands = pl.ds(1, seq_count - 1)
    settle(part_in.at[:, bands], late_recv.at[1])
    for l in range(layers):
        cells = [mine_now[l]] + [
            tuple(part_in[l, d, :, i * HEAD_DIM:(i + 1) * HEAD_DIM] for i in range(3))
            for d in range(1, seq_count)
        ]
        top = functools.reduce(jnp.maximum, [c[1] for c in cells])
        factors = [jnp.exp(c[1] - top) for c in cells]
        partial_out[l, :, :HEAD_DIM] = factors[0]
        partial_out[l, :, HEAD_DIM:2 * HEAD_DIM] = sum(
            f * c[0] for f, c in zip(factors, cells)
        )
        partial_out[l, :, 2 * HEAD_DIM:] = sum(f * c[2] for f, c in zip(factors, cells))

    settle(part_out.at[:, bands], send_sem.at[1])
    settle(main_out.at[:, others], send_sem.at[0])
    settle(own_out.at[:, others], send_sem.at[2])
    settle(values_in.at[others], own_recv.at[1])


def finish(
    dims, cache, put, values, weights, partial, att_out, cache_out, att, last, sem
):
    _, seq_count, _ = dims
    layers, _, src_rows, full = cache.shape
    kvw = full // 2
    group = HEADS // KV_HEADS
    seq = lax.axis_index("seq")
    f32, bf16 = jnp.float32, jnp.bfloat16

    def lanes_of(d):
        g = lax.rem(seq + d, seq_count)
        return pl.ds(pl.multiple_of(kvw + g * HEAD_DIM, HEAD_DIM), HEAD_DIM)

    def write(piece, at):
        pltpu.make_async_copy(piece, cache_out.at[:, 0, :, at], sem.at[0]).start()

    keys = pl.ds(0, kvw)
    write(cache.at[:, 0, :, keys], keys)
    for d in range(1, seq_count):
        write(cache.at[:, 0, :, lanes_of(d)], lanes_of(d))
    own = [values[:, l].reshape(src_rows, HEAD_DIM) for l in range(layers)]
    both = jnp.concatenate([put[...], weights[...]], axis=0)
    moved = jnp.dot(both, jnp.concatenate(own, axis=1), preferred_element_type=f32)
    for l in range(layers):
        at = slice(l * HEAD_DIM, (l + 1) * HEAD_DIM)
        last[l] = moved[:src_rows, at].astype(bf16)
    write(last, lanes_of(0))
    lines = []
    for l in range(layers):
        value = moved[
            src_rows + l * PAD:src_rows + (l + 1) * PAD, l * HEAD_DIM:(l + 1) * HEAD_DIM
        ]
        factor = partial[l, :, :HEAD_DIM]
        summed = partial[l, :, HEAD_DIM:2 * HEAD_DIM]
        result = (summed + factor * value) / partial[l, :, 2 * HEAD_DIM:]
        lines.append(jnp.concatenate([result[h:h + 1] for h in range(group)], axis=1))
    att[...] = jnp.concatenate(lines, axis=0).astype(bf16)
    att_copy = pltpu.make_async_copy(att, att_out, sem.at[1])
    att_copy.start()
    pltpu.make_async_copy(cache, cache_out, sem.at[0]).wait()
    att_copy.wait()


def body(dims, query, text_cache, text_len, image_rows, patch_map, image_places):
    patch_count, seq_count, req_count = dims
    layers, req_dev, query_width = query.shape
    text_dev, full = text_cache.shape[2:]
    src_rows = image_rows.shape[1]
    groups = patch_count * req_count
    assert req_dev == 1 and seq_count == KV_HEADS and full == 2 * KV_HEADS * HEAD_DIM
    per = src_rows // groups
    assert patch_count % 2 == 0 and layers > 2 and per <= HEAD_DIM
    main_width = full - 2 * HEAD_DIM
    rows_padded = KV_HEADS * PAD
    bf16, f32, i32 = jnp.bfloat16, jnp.float32, jnp.int32
    dma = pltpu.SemaphoreType.DMA
    vmem = pl.BlockSpec(memory_space=pltpu.VMEM)
    hbm = pl.BlockSpec(memory_space=pltpu.HBM)
    att_shape = jax.ShapeDtypeStruct((layers, query_width // seq_count), bf16)
    cache_shape = jax.ShapeDtypeStruct((layers, 1, src_rows, full), bf16)
    in_hbm = lambda x: pltpu.with_memory_space_constraint(x, pltpu.HBM)
    in_vmem = lambda x: pltpu.with_memory_space_constraint(x, pltpu.VMEM)
    state = pl.pallas_call(
        functools.partial(exchange, dims),
        out_shape=(
            pltpu.VMEM(cache_shape.shape, bf16),
            pltpu.VMEM((src_rows, src_rows), bf16),
            pltpu.VMEM((groups, layers, per, HEAD_DIM), bf16),
            pltpu.VMEM((layers * PAD, src_rows), bf16),
            pltpu.VMEM((layers, PAD, 3 * HEAD_DIM), f32),
        ),
        in_specs=[hbm, pl.BlockSpec(memory_space=pl.ANY), hbm, hbm, hbm, hbm],
        out_specs=(vmem,) * 5,
        scratch_shapes=[
            pltpu.VMEM((layers, query_width), bf16),
            pltpu.SMEM((1,), i32),
            pltpu.VMEM((1, src_rows), i32),
            pltpu.VMEM((1, src_rows), i32),
            pltpu.VMEM((layers, src_rows, full), bf16),
            pltpu.VMEM((layers, text_dev, full), bf16),
            pltpu.VMEM((layers, groups, per, main_width), bf16),
            pltpu.VMEM((layers, groups, per, main_width), bf16),
            pltpu.VMEM((2, groups, layers, per, HEAD_DIM), bf16),
            pltpu.VMEM((groups, layers, per, HEAD_DIM), bf16),
            pltpu.VMEM((groups, 1, HEAD_DIM), i32),
            pltpu.VMEM((groups, 1, HEAD_DIM), i32),
            pltpu.VMEM((layers, rows_padded, HEAD_DIM), f32),
            pltpu.VMEM((layers, rows_padded, text_dev), f32),
            pltpu.VMEM((layers, seq_count, PAD, 3 * HEAD_DIM), f32),
            pltpu.VMEM((layers, seq_count, PAD, 3 * HEAD_DIM), f32),
            pltpu.VMEM((req_count, per, HEAD_DIM), bf16),
            dma((1,)), dma((3,)), dma((3,)), dma((layers,)), dma((2,)), dma((2,)), pltpu.SemaphoreType.REGULAR((3,)),
        ],
        compiler_params=pltpu.CompilerParams(
            collective_id=0, has_side_effects=True, vmem_limit_bytes=32 * 1024 * 1024
        ),
    )(
        in_hbm(query.reshape(layers, query_width)), text_len,
        in_hbm(patch_map.reshape(1, src_rows)), in_hbm(image_places.reshape(1, src_rows)),
        in_hbm(image_rows), in_hbm(text_cache),
    )
    attended, cache = pl.pallas_call(
        functools.partial(finish, dims),
        out_shape=(att_shape, cache_shape),
        in_specs=[vmem] * 5,
        out_specs=(hbm, hbm),
        scratch_shapes=[
            pltpu.VMEM(att_shape.shape, bf16),
            pltpu.VMEM((layers, src_rows, HEAD_DIM), bf16),
            dma((2,)),
        ],
    )(*(in_vmem(x) for x in state))
    return attended.reshape(layers, 1, query_width // seq_count), cache


def solution(mesh):
    dims = tuple(mesh.shape[a] for a in ("patch", "seq", "req"))
    return jax.shard_map(
        functools.partial(body, dims),
        mesh=mesh,
        in_specs=(
            P(None, ("patch", "req"), None),
            P(None, ("patch", "req"), "seq", None),
            P(("patch", "req")),
            P(None, ("patch", "seq", "req"), None),
            P(("patch", "seq", "req")),
            P(("patch", "seq", "req")),
        ),
        out_specs=(P(None, ("patch", "req"), "seq"), P(None, ("patch", "req"), "seq", None)),
        check_vma=False,
    )
```

```python
import functools
import math

import jax
import jax.numpy as jnp
from jax import lax
from jax.experimental import pallas as pl
from jax.experimental.pallas import tpu as pltpu
from jax.sharding import PartitionSpec as P

HEADS = 28
KV_HEADS = 4
HEAD_DIM = 128
PAD = 8
MESH = pl.DeviceIdType.MESH
NT = (((1,), (1,)), ((), ()))


def all_hops(patch_count, req_count):
    half = patch_count // 2
    cores = range(req_count)
    mates = [("mate", 0, c) for c in cores if c]
    near = [("near", i, c) for i in range(1, half) for c in cores]
    far = [[("far", k, c) for c in cores] for k in range(half)]
    return mates, near, far


def exchange(
    dims,
    query_hbm, len_hbm, map_hbm, place_hbm, rows_hbm, text_hbm,
    cache, put_out, values_in, weights_out, partial_out,
    query, length, maps, places, rows, text, main_out, main_in, own_out, keys_in, place_out, place_in,
    heads, scores, part_out, part_in, first_out,
    small_sem, load_sem, send_sem, main_recv, own_recv, late_recv,
    info,
):
    patch_count, seq_count, req_count = dims
    layers, src_rows, full = rows.shape
    text_dev = text.shape[1]
    kvw = full // 2
    group = HEADS // KV_HEADS
    groups = patch_count * req_count
    per = src_rows // groups
    half = patch_count // 2
    side = (seq_count - 1) * HEAD_DIM
    main_width = 2 * side
    scale = 1.0 / math.sqrt(HEAD_DIM)
    patch, seq, req = (lax.axis_index(a) for a in ("patch", "seq", "req"))
    me = patch * req_count + req
    mates, near, far = all_hops(patch_count, req_count)
    beside = near if half == 2 else []
    late = [hop for hop in near if hop not in beside]
    ahead = min(2, layers)
    f32, bf16 = jnp.float32, jnp.bfloat16
    upper = patch // half
    inner = jnp.logical_or(patch == half - 1, patch == half)

    def partner(hop):
        kind, i, c = hop
        if kind == "mate":
            return patch, lax.rem(req + c, req_count)
        r = req_count - 1 - c if kind == "near" or i == half - 1 else c
        if kind == "near":
            return upper * half + lax.rem(lax.rem(patch, half) + i, half), r
        return (1 - upper) * (patch_count - 1 - i) + upper * i, r

    others = pl.ds(0, groups - 1)
    own_in = (keys_in, values_in)
    second_rows = pltpu.make_async_copy(rows_hbm.at[1], rows.at[1], load_sem.at[0])
    rest = pl.ds(2, layers - 2)
    rest_rows = pltpu.make_async_copy(rows_hbm.at[rest], rows.at[rest], load_sem.at[1])
    text_copy = pltpu.make_async_copy(text_hbm.at[:, 0], text, load_sem.at[2])

    def settle(ref, sem):
        pltpu.make_async_copy(ref, ref, sem).wait()

    small = [
        pltpu.make_async_copy(map_hbm, maps, small_sem.at[0]),
        pltpu.make_async_copy(place_hbm, places, small_sem.at[0]),
        pltpu.make_async_copy(query_hbm, query, small_sem.at[0]),
        pltpu.make_async_copy(len_hbm, length, small_sem.at[0]),
    ]
    def lanes_of(d, base=0):
        g = lax.rem(seq + d, seq_count)
        return pl.ds(pl.multiple_of(base + g * HEAD_DIM, HEAD_DIM), HEAD_DIM)

    def load(i, at):
        pltpu.make_async_copy(rows_hbm.at[0, :, at], rows.at[0, :, at], load_sem.at[i]).start()

    small[0].start()
    load(0, lanes_of(1))
    barrier = pltpu.get_barrier_semaphore()

    def tell(sem, p, s, r):
        pl.semaphore_signal(sem, inc=1, device_id=(p, s, r), device_id_type=MESH)

    above, below = patch < patch_count - 1, patch > 0

    @pl.when(jnp.logical_and(below, patch <= half))
    def _():
        for c in range(req_count):
            tell(barrier, patch - 1, seq, lax.rem(req + c, req_count))

    @pl.when(above)
    def _():
        for c in range(req_count):
            tell(barrier, patch + 1, seq, lax.rem(req + c, req_count))

    for c in range(1, req_count):
        tell(barrier, patch, seq, lax.rem(req + c, req_count))

    @pl.when(patch == 0)
    def _():
        for d in range(1, seq_count):
            tell(barrier, patch, lax.rem(seq + d, seq_count), req)

    for d in range(2, seq_count):
        load(1, lanes_of(d))
    for d in range(1, seq_count):
        load(2, lanes_of(d, kvw))
    has_below = 1 - (patch_count - 1 - patch) // (patch_count - 1)
    arrivals = (
        req_count - 1 + req_count * (has_below + 1 - upper) + (seq_count - 1) * (1 - has_below)
    )
    answers = jnp.logical_and(patch == patch_count - 1, patch > half)

    @pl.when(answers)
    def _():
        pl.semaphore_wait(barrier, arrivals)
        tell(info.at[0], patch - 1, seq, req)


    owner = lax.broadcasted_iota(jnp.int32, (groups, src_rows), 0)
    source = lax.broadcasted_iota(jnp.int32, (groups, src_rows), 1) // per
    row_i = lax.broadcasted_iota(jnp.int32, (src_rows, src_rows), 0)
    col_i = lax.broadcasted_iota(jnp.int32, (src_rows, src_rows), 1)
    before = (row_i < col_i).astype(f32).astype(bf16)
    small[0].wait()
    small[1].start()
    mine = maps[...] == owner
    rank = jnp.dot(mine.astype(f32).astype(bf16), before, preferred_element_type=f32)
    slot = jnp.sum(
        jnp.where(mine, rank + (owner * per).astype(f32), 0.0), axis=0, keepdims=True
    )
    slot = slot.astype(jnp.int32)
    p_first, _ = partner(far[-1][0])
    row_first = lax.broadcasted_iota(jnp.int32, (req_count * per, src_rows), 0)
    pick_first = (
        row_first + p_first * (req_count * per) == slot
    ).astype(f32).astype(bf16)

    def place_copy(hop):
        p, r = partner(hop)
        return pltpu.make_async_remote_copy(
            src_ref=place_out.at[p * req_count + r], dst_ref=place_in.at[me],
            send_sem=send_sem.at[1], recv_sem=late_recv.at[0],
            device_id=(p, seq, r), device_id_type=MESH,
        )

    def main_copy(l, hop, at=pl.ds(0, main_width)):
        p, r = partner(hop)
        return pltpu.make_async_remote_copy(
            src_ref=main_out.at[l, p * req_count + r, :, at], dst_ref=main_in.at[l, me, :, at],
            send_sem=send_sem.at[0], recv_sem=main_recv.at[l],
            device_id=(p, seq, r), device_id_type=MESH,
        )

    def first_copy(hop):
        p, r = partner(hop)
        return pltpu.make_async_remote_copy(
            src_ref=first_out.at[r], dst_ref=main_in.at[0, me, :, pl.ds(0, HEAD_DIM)],
            send_sem=send_sem.at[0], recv_sem=main_recv.at[0],
            device_id=(p, seq, r), device_id_type=MESH,
        )

    def own_copy(i, hop):
        p, r = partner(hop)
        return pltpu.make_async_remote_copy(
            src_ref=own_out.at[i, p * req_count + r], dst_ref=own_in[i].at[me],
            send_sem=send_sem.at[2], recv_sem=own_recv.at[i],
            device_id=(p, seq, r), device_id_type=MESH,
        )

    def part_copy(l, d):
        s = lax.rem(seq + d, seq_count)
        return pltpu.make_async_remote_copy(
            src_ref=part_out.at[l, d], dst_ref=part_in.at[l, d],
            send_sem=send_sem.at[1], recv_sem=late_recv.at[1],
            device_id=(patch, s, req), device_id_type=MESH,
        )

    def sort(l, base):
        turned = jnp.concatenate(
            [rows[l, :, lanes_of(d, base)] for d in range(1, seq_count)], axis=1
        )
        moved = jnp.dot(pick, turned, preferred_element_type=f32).astype(bf16)
        at = slice(0, side) if base == 0 else slice(side, main_width)
        main_out[l, :, :, at] = moved.reshape(groups, per, side)

    def send_first(l, at, across):
        for hop in mates:
            main_copy(l, hop, at).start()

        @pl.when(patch != half)
        def _():
            for hop in beside:
                main_copy(l, hop, at).start()

        if l < ahead:

            @pl.when(inner)
            def _():
                for hop in far[-1]:
                    main_copy(l, hop, across).start()

    def settle_rows(i, width):
        settle(rows.at[0, :, pl.ds(0, width)], load_sem.at[i])

    settle_rows(0, HEAD_DIM)
    second_rows.start()
    moved = jnp.dot(pick_first, rows[0, :, lanes_of(1)], preferred_element_type=f32)
    first_out[...] = moved.astype(bf16).reshape(req_count, per, HEAD_DIM)

    @pl.when(jnp.logical_not(answers))
    def _():
        pl.semaphore_wait(barrier, arrivals)

    @pl.when(inner)
    def _():
        for hop in far[-1]:
            first_copy(hop).start()

    pick = (row_i == slot).astype(f32).astype(bf16)
    for l in range(layers):
        if l == 0:
            settle_rows(1, side - HEAD_DIM)
            rest_rows.start()
            sort(l, 0)
            send_first(l, pl.ds(0, side), pl.ds(HEAD_DIM, side - HEAD_DIM))
            settle_rows(2, side)
            load(2, lanes_of(0))
            load(2, lanes_of(0, kvw))
            sort(l, kvw)
            send_first(l, pl.ds(side, side), pl.ds(side, side))

            @pl.when(jnp.logical_and(patch == 1, above))
            def _():
                tell(info.at[1], patch + 1, seq, req)

        else:
            if l == 1:
                second_rows.wait()
            if l == 2:
                rest_rows.wait()
            sort(l, 0)
            sort(l, kvw)
            send_first(l, pl.ds(0, main_width), pl.ds(0, main_width))
        if l == 0:
            small[1].wait()
            small[2].start()
            local = (places[...] - seq * src_rows).astype(f32).astype(bf16)
            place_sorted = lax.dot_general(
                jnp.broadcast_to(local, (PAD, src_rows)), pick, NT,
                preferred_element_type=f32,
            )
            apart = jnp.where(source == owner, place_sorted[0:1], 0.0).astype(bf16)
            lane = lax.broadcasted_iota(jnp.int32, (src_rows, HEAD_DIM), 1)
            entry = lax.broadcasted_iota(jnp.int32, (src_rows, HEAD_DIM), 0)
            gather = (lax.rem(entry, per) == lane).astype(f32).astype(bf16)
            placed = jnp.dot(apart, gather, preferred_element_type=f32).astype(jnp.int32)
            place_out[...] = placed.reshape(groups, 1, HEAD_DIM)
            place_in[me] = place_out[me]
            for hop in mates:
                place_copy(hop).start()

            @pl.when(patch != half)
            def _():
                for hop in beside:
                    place_copy(hop).start()

    settle_rows(2, 2 * HEAD_DIM)
    for l in range(layers):
        turned = jnp.concatenate([rows[l, :, lanes_of(0)], rows[l, :, lanes_of(0, kvw)]], axis=1)
        moved = jnp.dot(pick, turned, preferred_element_type=f32).astype(bf16)
        own_out[0, :, l] = moved[:, :HEAD_DIM].reshape(groups, per, HEAD_DIM)
        own_out[1, :, l] = moved[:, HEAD_DIM:].reshape(groups, per, HEAD_DIM)
    def own_near():
        for i in range(2):
            for hop in beside:
                own_copy(i, hop).start()

    for i in range(2):
        for hop in mates:
            own_copy(i, hop).start()
    pl.when(patch != half)(own_near)
    listens = jnp.logical_or(
        patch < patch_count - 2, jnp.logical_and(patch >= half, above)
    )

    @pl.when(listens)
    def _():
        pl.semaphore_wait(info.at[0], 1)

    @pl.when(jnp.logical_and(listens, below))
    def _():
        tell(info.at[0], patch - 1, seq, req)

    @pl.when(patch > 1)
    def _():
        pl.semaphore_wait(info.at[1], 1)

    @pl.when(jnp.logical_and(patch > 1, above))
    def _():
        tell(info.at[1], patch + 1, seq, req)

    @pl.when(patch == 0)
    def _():
        for d in range(1, seq_count):
            tell(info.at[2], patch, lax.rem(seq + d, seq_count), req)

    @pl.when(patch == half)
    def _():
        for hop in beside:
            place_copy(hop).start()
        for l in range(layers):
            for hop in beside:
                main_copy(l, hop).start()
        own_near()

    for hop in late:
        place_copy(hop).start()
        for l in range(layers):
            main_copy(l, hop).start()
        for i in range(2):
            own_copy(i, hop).start()
    for wave in far:
        for hop in wave:
            place_copy(hop).start()
    for l in range(layers):
        for wave in far[:-1]:
            for hop in wave:
                main_copy(l, hop).start()

    @pl.when(jnp.logical_not(inner))
    def _():
        for l in range(ahead):
            for hop in far[-1]:
                main_copy(l, hop).start()

    for l in range(ahead, layers):
        for hop in far[-1]:
            main_copy(l, hop).start()
    for wave in far:
        for i in range(2):
            for hop in wave:
                own_copy(i, hop).start()
    text_copy.start()
    for l in range(layers):
        main_in[l, me] = main_out[l, me]
    for i in range(2):
        own_in[i][me] = own_out[i, me]

    small[2].wait()
    small[3].start()
    lines = query[...].astype(f32)
    for l in range(layers):
        for g in range(KV_HEADS):
            heads[l, g * PAD:(g + 1) * PAD, :] = jnp.concatenate(
                [
                    lines[l:l + 1, (g * group + h) * HEAD_DIM:(g * group + h + 1) * HEAD_DIM]
                    for h in range(group)
                ] + [jnp.zeros((PAD - group, HEAD_DIM), f32)],
                axis=0,
            )

    def head_block(l, d):
        g = lax.rem(seq + d, seq_count)
        return heads[l, pl.ds(pl.multiple_of(g * PAD, PAD), PAD), :]

    small[3].wait()
    positions = seq * text_dev + lax.broadcasted_iota(
        jnp.int32, (KV_HEADS * PAD, text_dev), 1
    )
    used = positions < length[0]
    lane_group = lax.broadcasted_iota(jnp.int32, (PAD, kvw), 1) // HEAD_DIM
    for l in range(layers):
        spread = jnp.concatenate(
            [
                jnp.where(
                    lane_group == lax.rem(seq + d, seq_count),
                    jnp.concatenate([head_block(l, d)] * KV_HEADS, axis=1),
                    0.0,
                )
                for d in range(seq_count)
            ],
            axis=0,
        ).astype(bf16)
        if l == 0:
            text_copy.wait()
        raw = lax.dot_general(
            spread, text[l, :, :kvw], NT, preferred_element_type=f32
        ) * scale
        scores[l] = jnp.where(used, raw, -jnp.inf)

    @pl.when(patch == 0)
    def _():
        pl.semaphore_wait(info.at[2], seq_count - 1)
        for p in range(1, patch_count):
            tell(info.at[2], p, seq, req)

    @pl.when(below)
    def _():
        pl.semaphore_wait(info.at[2], 1)

    settle(place_in.at[others], late_recv.at[0])
    slot_i = lax.broadcasted_iota(jnp.int32, (HEAD_DIM, src_rows), 0)
    place_i = lax.broadcasted_iota(jnp.int32, (HEAD_DIM, src_rows), 1)
    wanted = (slot_i == lax.rem(place_i, per)).astype(f32).astype(bf16)
    lanes = jnp.dot(
        place_in[...].reshape(groups, HEAD_DIM).astype(f32).astype(bf16), wanted,
        preferred_element_type=f32,
    )
    place = jnp.sum(jnp.where(source == owner, lanes, 0.0), axis=0, keepdims=True)
    put = (row_i == place.astype(jnp.int32)).astype(f32).astype(bf16)
    put_out[...] = put

    zeros = jnp.zeros((PAD, HEAD_DIM), f32)
    for l in range(layers):
        spread = jnp.concatenate(
            [
                jnp.concatenate(
                    [head_block(l, d) if c == d else zeros for c in range(1, seq_count)],
                    axis=1,
                )
                for d in range(1, seq_count)
            ],
            axis=0,
        ).astype(bf16)
        settle(main_in.at[l, others], main_recv.at[l])
        if l == 0:
            settle(place_in.at[others], send_sem.at[1])
        block = main_in[l].reshape(src_rows, main_width)
        image_scores = lax.dot_general(
            spread, block[:, :side], NT, preferred_element_type=f32
        ) * scale
        both = jnp.concatenate([scores[l, PAD:, :], image_scores], axis=1)
        top = jnp.max(both, axis=1, keepdims=True)
        weights = jnp.exp(both - top)
        total = jnp.sum(weights, axis=1, keepdims=True)
        weights = weights.astype(bf16)
        image_sums = jnp.dot(
            weights[:, text_dev:], block[:, side:], preferred_element_type=f32
        )
        for d in range(1, seq_count):
            at = slice((d - 1) * PAD, d * PAD)
            text_sums = jnp.dot(
                weights[at, :text_dev], text[l, :, lanes_of(d, kvw)],
                preferred_element_type=f32,
            )
            part_out[l, d, :, :HEAD_DIM] = (
                text_sums + image_sums[at, (d - 1) * HEAD_DIM:d * HEAD_DIM]
            )
            part_out[l, d, :, HEAD_DIM:2 * HEAD_DIM] = jnp.broadcast_to(
                top[at], (PAD, HEAD_DIM)
            )
            part_out[l, d, :, 2 * HEAD_DIM:] = jnp.broadcast_to(total[at], (PAD, HEAD_DIM))
            part_copy(l, d).start()
        moved = jnp.dot(put, block, preferred_element_type=f32).astype(bf16)
        for d in range(1, seq_count):
            cache[l, 0, :, lanes_of(d)] = moved[:, (d - 1) * HEAD_DIM:d * HEAD_DIM]
            cache[l, 0, :, lanes_of(d, kvw)] = moved[
                :, side + (d - 1) * HEAD_DIM:side + d * HEAD_DIM
            ]

    settle(keys_in.at[others], own_recv.at[0])
    own_keys = [keys_in[:, l].reshape(src_rows, HEAD_DIM) for l in range(layers)]
    own_scores = jnp.concatenate(
        [
            jnp.concatenate(
                [
                    scores[l, :PAD, :],
                    lax.dot_general(
                        head_block(l, 0).astype(bf16), own_keys[l], NT,
                        preferred_element_type=f32,
                    ) * scale,
                ],
                axis=1,
            )
            for l in range(layers)
        ],
        axis=0,
    )
    own_top = jnp.max(own_scores, axis=1, keepdims=True)
    own_w = jnp.exp(own_scores - own_top)
    own_total = jnp.sum(own_w, axis=1, keepdims=True)
    rounded = own_w.astype(bf16)
    weights_out[...] = rounded[:, text_dev:]
    mine_now = []
    for l in range(layers):
        at = slice(l * PAD, (l + 1) * PAD)
        value = jnp.dot(
            rounded[at, :text_dev], text[l, :, lanes_of(0, kvw)], preferred_element_type=f32
        )
        mine_now.append((
            value,
            jnp.broadcast_to(own_top[at], (PAD, HEAD_DIM)),
            jnp.broadcast_to(own_total[at], (PAD, HEAD_DIM)),
        ))
    moved = jnp.dot(
        put, jnp.concatenate(own_keys, axis=1), preferred_element_type=f32
    ).astype(bf16)
    for l in range(layers):
        cache[l, 0, :, lanes_of(0)] = moved[:, l * HEAD_DIM:(l + 1) * HEAD_DIM]

    bands = pl.ds(1, seq_count - 1)
    settle(part_in.at[:, bands], late_recv.at[1])
    for l in range(layers):
        cells = [mine_now[l]] + [
            tuple(part_in[l, d, :, i * HEAD_DIM:(i + 1) * HEAD_DIM] for i in range(3))
            for d in range(1, seq_count)
        ]
        top = functools.reduce(jnp.maximum, [c[1] for c in cells])
        factors = [jnp.exp(c[1] - top) for c in cells]
        partial_out[l, :, :HEAD_DIM] = factors[0]
        partial_out[l, :, HEAD_DIM:2 * HEAD_DIM] = sum(
            f * c[0] for f, c in zip(factors, cells)
        )
        partial_out[l, :, 2 * HEAD_DIM:] = sum(f * c[2] for f, c in zip(factors, cells))

    settle(part_out.at[:, bands], send_sem.at[1])
    settle(main_out.at[:, others], send_sem.at[0])
    settle(own_out.at[:, others], send_sem.at[2])
    settle(values_in.at[others], own_recv.at[1])


def finish(
    dims, cache, put, values, weights, partial, att_out, cache_out, att, last, sem
):
    _, seq_count, _ = dims
    layers, _, src_rows, full = cache.shape
    kvw = full // 2
    group = HEADS // KV_HEADS
    seq = lax.axis_index("seq")
    f32, bf16 = jnp.float32, jnp.bfloat16

    def lanes_of(d):
        g = lax.rem(seq + d, seq_count)
        return pl.ds(pl.multiple_of(kvw + g * HEAD_DIM, HEAD_DIM), HEAD_DIM)

    def write(l, piece, at):
        pltpu.make_async_copy(piece, cache_out.at[l, 0, :, at], sem.at[0]).start()

    for l in range(layers):
        for g in range(seq_count):
            keys = pl.ds(g * HEAD_DIM, HEAD_DIM)
            write(l, cache.at[l, 0, :, keys], keys)
        for d in range(1, seq_count):
            write(l, cache.at[l, 0, :, lanes_of(d)], lanes_of(d))
    own = [values[:, l].reshape(src_rows, HEAD_DIM) for l in range(layers)]
    both = jnp.concatenate([put[...], weights[...]], axis=0)
    moved = jnp.dot(both, jnp.concatenate(own, axis=1), preferred_element_type=f32)
    for l in range(layers):
        at = slice(l * HEAD_DIM, (l + 1) * HEAD_DIM)
        last[l] = moved[:src_rows, at].astype(bf16)
        write(l, last.at[l], lanes_of(0))
    lines = []
    for l in range(layers):
        value = moved[
            src_rows + l * PAD:src_rows + (l + 1) * PAD, l * HEAD_DIM:(l + 1) * HEAD_DIM
        ]
        factor = partial[l, :, :HEAD_DIM]
        summed = partial[l, :, HEAD_DIM:2 * HEAD_DIM]
        result = (summed + factor * value) / partial[l, :, 2 * HEAD_DIM:]
        lines.append(jnp.concatenate([result[h:h + 1] for h in range(group)], axis=1))
    att[...] = jnp.concatenate(lines, axis=0).astype(bf16)
    att_copy = pltpu.make_async_copy(att, att_out, sem.at[1])
    att_copy.start()
    pltpu.make_async_copy(cache, cache_out, sem.at[0]).wait()
    att_copy.wait()


def body(dims, query, text_cache, text_len, image_rows, patch_map, image_places):
    patch_count, seq_count, req_count = dims
    layers, req_dev, query_width = query.shape
    text_dev, full = text_cache.shape[2:]
    src_rows = image_rows.shape[1]
    groups = patch_count * req_count
    assert req_dev == 1 and seq_count == KV_HEADS and full == 2 * KV_HEADS * HEAD_DIM
    per = src_rows // groups
    assert patch_count % 2 == 0 and layers > 2 and per <= HEAD_DIM
    main_width = full - 2 * HEAD_DIM
    rows_padded = KV_HEADS * PAD
    bf16, f32, i32 = jnp.bfloat16, jnp.float32, jnp.int32
    dma = pltpu.SemaphoreType.DMA
    vmem = pl.BlockSpec(memory_space=pltpu.VMEM)
    hbm = pl.BlockSpec(memory_space=pltpu.HBM)
    att_shape = jax.ShapeDtypeStruct((layers, query_width // seq_count), bf16)
    cache_shape = jax.ShapeDtypeStruct((layers, 1, src_rows, full), bf16)
    in_hbm = lambda x: pltpu.with_memory_space_constraint(x, pltpu.HBM)
    in_vmem = lambda x: pltpu.with_memory_space_constraint(x, pltpu.VMEM)
    state = pl.pallas_call(
        functools.partial(exchange, dims),
        out_shape=(
            pltpu.VMEM(cache_shape.shape, bf16),
            pltpu.VMEM((src_rows, src_rows), bf16),
            pltpu.VMEM((groups, layers, per, HEAD_DIM), bf16),
            pltpu.VMEM((layers * PAD, src_rows), bf16),
            pltpu.VMEM((layers, PAD, 3 * HEAD_DIM), f32),
        ),
        in_specs=[hbm, pl.BlockSpec(memory_space=pl.ANY), hbm, hbm, hbm, hbm],
        out_specs=(vmem,) * 5,
        scratch_shapes=[
            pltpu.VMEM((layers, query_width), bf16),
            pltpu.SMEM((1,), i32),
            pltpu.VMEM((1, src_rows), i32),
            pltpu.VMEM((1, src_rows), i32),
            pltpu.VMEM((layers, src_rows, full), bf16),
            pltpu.VMEM((layers, text_dev, full), bf16),
            pltpu.VMEM((layers, groups, per, main_width), bf16),
            pltpu.VMEM((layers, groups, per, main_width), bf16),
            pltpu.VMEM((2, groups, layers, per, HEAD_DIM), bf16),
            pltpu.VMEM((groups, layers, per, HEAD_DIM), bf16),
            pltpu.VMEM((groups, 1, HEAD_DIM), i32),
            pltpu.VMEM((groups, 1, HEAD_DIM), i32),
            pltpu.VMEM((layers, rows_padded, HEAD_DIM), f32),
            pltpu.VMEM((layers, rows_padded, text_dev), f32),
            pltpu.VMEM((layers, seq_count, PAD, 3 * HEAD_DIM), f32),
            pltpu.VMEM((layers, seq_count, PAD, 3 * HEAD_DIM), f32),
            pltpu.VMEM((req_count, per, HEAD_DIM), bf16),
            dma((1,)), dma((3,)), dma((3,)), dma((layers,)), dma((2,)), dma((2,)), pltpu.SemaphoreType.REGULAR((3,)),
        ],
        compiler_params=pltpu.CompilerParams(
            collective_id=0, has_side_effects=True, vmem_limit_bytes=32 * 1024 * 1024
        ),
    )(
        in_hbm(query.reshape(layers, query_width)), text_len,
        in_hbm(patch_map.reshape(1, src_rows)), in_hbm(image_places.reshape(1, src_rows)),
        in_hbm(image_rows), in_hbm(text_cache),
    )
    attended, cache = pl.pallas_call(
        functools.partial(finish, dims),
        out_shape=(att_shape, cache_shape),
        in_specs=[vmem] * 5,
        out_specs=(hbm, hbm),
        scratch_shapes=[
            pltpu.VMEM(att_shape.shape, bf16),
            pltpu.VMEM((layers, src_rows, HEAD_DIM), bf16),
            dma((2,)),
        ],
    )(*(in_vmem(x) for x in state))
    return attended.reshape(layers, 1, query_width // seq_count), cache


def solution(mesh):
    dims = tuple(mesh.shape[a] for a in ("patch", "seq", "req"))
    return jax.shard_map(
        functools.partial(body, dims),
        mesh=mesh,
        in_specs=(
            P(None, ("patch", "req"), None),
            P(None, ("patch", "req"), "seq", None),
            P(("patch", "req")),
            P(None, ("patch", "seq", "req"), None),
            P(("patch", "seq", "req")),
            P(("patch", "seq", "req")),
        ),
        out_specs=(P(None, ("patch", "req"), "seq"), P(None, ("patch", "req"), "seq", None)),
        check_vma=False,
    )
```
